256 devices in a mesh: gx: 4 (over x), gy: 8 (over y, core), gz: 8 (over z).
Axes of the slice: x: 4, y: 4, z: 8, core: 2. Of those that a mesh axis runs over, the one named last changes fastest.
Arguments:
- right_side: float32 [8, 32, 256, 1024], P(None, 'gx', 'gy', 'gz'), may hold values from -12 to 12
- shift: float32 [32, 256, 1024], P('gx', 'gy', 'gz'), may hold values from 0.02 to 2
Outputs:
- solution_block: float32 [8, 32, 256, 1024], P(None, 'gx', 'gy', 'gz')
- residual_norms: float32 [8], replicated
The draws below stay inside these ranges and needn't reach their ends.
All inputs are finite; a program needn't handle non-finite values.
Results may differ from the reference program's by a relative error of at most 0.0003.
Values sent between devices are 32-bit elements; how exact they have to be, the bound alone decides.
A program may use at most 128 MiB of HBM per device.

```python
import math
import jax
import jax.numpy as jnp
from jax import lax

S = 8
ITERS = 2
NX = 32
NY = 256
NZ = 1024


def draw_right_side(key, part):
    first = jax.random.fold_in(key, 11)
    ramp_x = jnp.arange(NX, dtype=jnp.float32)[:, None, None] / NX
    ramp_y = jnp.arange(NY, dtype=jnp.float32)[None, :, None] / NY
    ramp_z = jnp.arange(NZ, dtype=jnp.float32)[None, None, :] / NZ
    ramp = 1.0 + (ramp_x + ramp_y + ramp_z) * 2.0 / 3.0
    values = jax.random.normal(first, (S, NX, NY, NZ), jnp.float32) * ramp[None]
    return jnp.clip(values, -12.0, 12.0)


def level_of(key, dims, cuts, low, top_value):
    gain, own = 1.0, jax.random.fold_in(key, 6)
    for dim, parts in cuts:
        heights = jnp.exp(jax.random.uniform(jax.random.fold_in(own, dim), (parts,), jnp.float32, low / len(cuts), top_value / len(cuts)))
        gain = gain * jnp.repeat(heights, dims[dim] // parts).reshape([-1 if axis == dim else 1 for axis in range(len(dims))])
    return gain


def setup_inputs(seed: int = 0) -> dict:
    key_of = jax.random.split(jax.random.key(seed), 3)
    right_side = draw_right_side(jax.random.fold_in(key_of[2], 71), 0)
    shift = jnp.clip(jnp.exp(math.log(2.0) - 4.6051702 * jax.random.uniform(key_of[1], (NX, NY, NZ), jnp.float32) ** level_of(key_of[1], (NX, NY, NZ), ((0, 4), (1, 8), (2, 8)), -0.2, 0.2)), 0.02, 2.0)
    return dict(right_side=right_side, shift=shift)


def operate(fields, shift):
    padded = jnp.pad(fields, ((0, 0), (1, 1), (1, 1), (1, 1)))
    beside = padded[:, 2:, 1:-1, 1:-1] + padded[:, :-2, 1:-1, 1:-1]
    beside = beside + padded[:, 1:-1, 2:, 1:-1] + padded[:, 1:-1, :-2, 1:-1]
    beside = beside + padded[:, 1:-1, 1:-1, 2:] + padded[:, 1:-1, 1:-1, :-2]
    return (6.0 + shift)[None] * fields - beside

def lower_inverse(lower):
    count = lower.shape[0]
    return jax.scipy.linalg.solve_triangular(lower, jnp.eye(count, dtype=lower.dtype), lower=True)

def small_dot(left, right):
    return jnp.dot(left, right, precision=lax.Precision.HIGHEST)

def reference(right_side, shift):
    width = right_side.shape[0]
    shape = right_side.shape
    rows = right_side.reshape(width, -1)
    gram = small_dot(rows, rows.T)
    lower = jnp.linalg.cholesky(gram)
    start_coeff = lower.T
    basis = [small_dot(lower_inverse(lower), rows)]
    hessen = jnp.zeros(((ITERS + 1) * width, ITERS * width), jnp.float32)
    for step in range(ITERS):
        image = operate(basis[step].reshape(shape), shift).reshape(width, -1)
        stacked = jnp.concatenate(basis, axis=0)
        products = small_dot(jnp.concatenate([stacked, image], axis=0), image.T)
        coeffs = products[:-width]
        gram = products[-width:] - small_dot(coeffs.T, coeffs)
        lower = jnp.linalg.cholesky(gram)
        hessen = hessen.at[:(step + 1) * width, step * width:(step + 1) * width].set(coeffs)
        hessen = hessen.at[(step + 1) * width:(step + 2) * width, step * width:(step + 1) * width].set(lower.T)
        if step + 1 < ITERS:
            projected = image - small_dot(coeffs.T, stacked)
            basis.append(small_dot(lower_inverse(lower), projected))
    target = jnp.zeros(((ITERS + 1) * width, width), jnp.float32).at[:width].set(start_coeff)
    normal = small_dot(hessen.T, hessen)
    factor = jnp.linalg.cholesky(normal)
    coeff_y = jax.scipy.linalg.cho_solve((factor, True), small_dot(hessen.T, target))
    solution = small_dot(coeff_y.T, jnp.concatenate(basis, axis=0)).reshape(shape)
    leftover = target - small_dot(hessen, coeff_y)
    norms = jnp.sqrt(lax.optimization_barrier(jnp.sum(leftover * leftover, axis=0)))
    return (solution, norms)
```

```python
import functools

import jax
import jax.numpy as jnp
from jax import lax
from jax.experimental import pallas as pl
from jax.experimental.pallas import tpu as pltpu
from jax.sharding import PartitionSpec as P

MESH = pl.DeviceIdType.MESH
F, NX, NY, NZ = 8, 8, 32, 128
TOP = 8
ROWS = slice(TOP, TOP + NY)
GROUPS = 4
WIDE = F // GROUPS
TILE = (8, 128)


def exchange_kernel(gx, gy, gz, b_hbm, s_hbm, gram_ref, ab_hbm,
                    buf_p, buf_q, buf_r, diag, side, pack_s, pack_r, part_z, part_p,
                    load_sem, xs_sem, xr_sem, ys_sem, yr_sem, zs_sem, zr_sem,
                    g_send, g_recv, out_sem):
    ix, iy, iz = lax.axis_index("gx"), lax.axis_index("gy"), lax.axis_index("gz")
    plane = gx * gy
    here = ix * gy + iy

    def in_plane(k):
        other = lax.rem(here + k, plane)
        return (lax.div(other, gy), lax.rem(other, gy), iz)

    def in_line(k):
        return (ix, iy, lax.rem(iz + k, gz))

    barrier = pltpu.get_barrier_semaphore()
    for k in range(1, gz):
        pl.semaphore_signal(barrier, inc=1, device_id=in_line(k), device_id_type=MESH)
    for k in range(1, plane):
        pl.semaphore_signal(barrier, inc=1, device_id=in_plane(k), device_id_type=MESH)

    loads = [
        pltpu.make_async_copy(b_hbm.at[:, 0], buf_p.at[:, 1, ROWS], load_sem.at[0]),
        pltpu.make_async_copy(b_hbm.at[:, NX - 1], buf_p.at[:, NX, ROWS], load_sem.at[1]),
        pltpu.make_async_copy(b_hbm.at[:, 1:NX - 1], buf_p.at[:, 2:NX, ROWS], load_sem.at[2]),
        pltpu.make_async_copy(s_hbm, diag, load_sem.at[3]),
    ]
    for load in loads:
        load.start()

    zero_x = jnp.zeros((F, NY, NZ), jnp.float32)
    zero_y = jnp.zeros((F, NX, 1, NZ), jnp.float32)
    zero_z = jnp.zeros((2 * F, NZ), jnp.float32)
    for turn, buf in enumerate((buf_p, buf_q)):
        @pl.when(ix == 0)
        def _():
            buf[:, 0, ROWS] = zero_x

        @pl.when(ix == gx - 1)
        def _():
            buf[:, NX + 1, ROWS] = zero_x

        @pl.when(iy == 0)
        def _():
            buf[:, 1:NX + 1, TOP - 1:TOP] = zero_y

        @pl.when(iy == gy - 1)
        def _():
            buf[:, 1:NX + 1, TOP + NY:TOP + NY + 1] = zero_y

        @pl.when(iz == 0)
        def _():
            pack_r[turn, 0] = zero_z

        @pl.when(iz == gz - 1)
        def _():
            pack_r[turn, 1] = zero_z

    bufs = (buf_p, buf_q)
    has = {
        "x": (ix > 0, ix < gx - 1),
        "y": (iy > 0, iy < gy - 1),
        "z": (iz > 0, iz < gz - 1),
    }

    def x_copy(turn, way, group):
        fields = slice(group * WIDE, (group + 1) * WIDE)
        buf = bufs[turn]
        return pltpu.make_async_remote_copy(
            src_ref=buf.at[fields, NX if way else 1, ROWS],
            dst_ref=buf.at[fields, 0 if way else NX + 1, ROWS],
            send_sem=xs_sem.at[turn, way, group],
            recv_sem=xr_sem.at[turn, way, group],
            device_id=(ix + 1 if way else ix - 1, iy, iz),
            device_id_type=MESH,
        )

    def y_copy(turn, way):
        buf = bufs[turn]
        src, dst = (TOP + NY - 1, TOP - 1) if way else (TOP, TOP + NY)
        return pltpu.make_async_remote_copy(
            src_ref=buf.at[:, 1:NX + 1, src:src + 1],
            dst_ref=buf.at[:, 1:NX + 1, dst:dst + 1],
            send_sem=ys_sem.at[turn, way],
            recv_sem=yr_sem.at[turn, way],
            device_id=(ix, iy + 1 if way else iy - 1, iz),
            device_id_type=MESH,
        )

    def z_copy(turn, way):
        return pltpu.make_async_remote_copy(
            src_ref=pack_s.at[turn, way],
            dst_ref=pack_r.at[turn, 0 if way else 1],
            send_sem=zs_sem.at[turn, way],
            recv_sem=zr_sem.at[turn, way],
            device_id=(ix, iy, iz + 1 if way else iz - 1),
            device_id_type=MESH,
        )

    def start(axis, way, copy):
        @pl.when(has[axis][way])
        def _():
            copy.start()

    def arrive(axis, way, copy):
        @pl.when(has[axis][1 - way])
        def _():
            copy.wait_recv()

    def sent(axis, way, copy):
        @pl.when(has[axis][way])
        def _():
            copy.wait_send()

    def pack_z(turn):
        buf = bufs[turn]
        for t in range(2 * F):
            f, half = t // 2, t % 2
            tile = buf[f, 1 + 4 * half:5 + 4 * half, ROWS].reshape(NZ, NZ).T
            pack_s[turn, 0, t:t + 1] = tile[0:1]
            pack_s[turn, 1, t:t + 1] = tile[NZ - 1:NZ]

    def unpack_z(turn):
        for t in range(2 * F):
            f, half = t // 2, t % 2
            low = jnp.broadcast_to(pack_r[turn, 0, t:t + 1], (NZ // 2, NZ))
            high = jnp.broadcast_to(pack_r[turn, 1, t:t + 1], (NZ // 2, NZ))
            tile = jnp.concatenate([low, high], axis=0).T
            side[f, 4 * half:4 * half + 4] = tile.reshape(4, NY, NZ)

    lane = lax.broadcasted_iota(jnp.int32, (NY, NZ), 1)
    first, last = lane == 0, lane == NZ - 1

    def apply(src, f, x):
        c = src[f, x, ROWS]
        edge = side[f, x - 1]
        beside = src[f, x + 1, ROWS] + src[f, x - 1, ROWS]
        beside = beside + src[f, x, TOP + 1:TOP + NY + 1] + src[f, x, TOP - 1:TOP + NY - 1]
        up = jnp.where(last, edge, pltpu.roll(c, NZ - 1, 1))
        down = jnp.where(first, edge, pltpu.roll(c, 1, 1))
        beside = beside + up + down
        return (6.0 + diag[x - 1]) * c - beside

    def at_p(x, rows):
        return buf_p[:, x, rows]

    def at_q(x, rows):
        return buf_q[:, x, rows]

    def at_r(x, rows):
        return buf_r[:, x, rows]

    def moment(left, right, low, high, sums):
        def step(x, sums):
            for t in range(NY // 8):
                rows = slice(TOP + 8 * t, TOP + 8 * t + 8)
                u = left(x, rows)
                v = u if right is left else right(x, rows)
                sums = tuple(sums[i] + u[i:i + 1] * v[i:] for i in range(F))
            return sums

        return lax.fori_loop(low, high, step, sums)

    none = tuple(jnp.zeros((F - i,) + TILE, jnp.float32) for i in range(F))

    sub = lax.broadcasted_iota(jnp.int32, TILE, 0)
    cell = lax.broadcasted_iota(jnp.int32, TILE, 1)

    def fold(parts):
        width = 1
        while len(parts) > 1:
            odd = (sub & width) != 0
            merged = []
            for i in range(0, len(parts), 2):
                a, b = parts[i], parts[i + 1]
                kept = jnp.where(odd, b, a)
                moved = jnp.where(odd, a, b)
                moved = jnp.where(odd, pltpu.roll(moved, width, 0), pltpu.roll(moved, 8 - width, 0))
                merged.append(kept + moved)
            parts = merged
            width *= 2
        return parts[0]

    def gather(order, sums, total):
        for c in range(F):
            row = fold([sums[min(i, c)][max(i, c) - min(i, c)] for i in range(F)])
            total = jnp.where(cell == order * F + c, jnp.sum(row, axis=1, keepdims=True), total)
        return total

    loads[0].wait()
    loads[1].wait()
    pl.semaphore_wait(barrier, gz - 1 + plane - 1)
    for group in range(GROUPS):
        for way in range(2):
            start("x", way, x_copy(0, way, group))
    loads[2].wait()
    for way in range(2):
        start("y", way, y_copy(0, way))
    pack_z(0)
    for way in range(2):
        start("z", way, z_copy(0, way))
    loads[3].wait()
    total = gather(0, moment(at_p, at_p, 1, NX + 1, none), jnp.zeros(TILE, jnp.float32))
    for way in range(2):
        arrive("y", way, y_copy(0, way))
        arrive("z", way, z_copy(0, way))
    unpack_z(0)

    def inner(src, dst, shift):
        def step(f, _):
            for x in range(2, NX):
                dst[f, x, ROWS] = apply(src, f, x)
            return 0

        lax.fori_loop(0, F, step, 0)

    inner(buf_p, buf_q, 0)

    def outer(src, dst, turn):
        for group in range(GROUPS):
            for way in range(2):
                arrive("x", way, x_copy(turn, way, group))
            for f in range(group * WIDE, (group + 1) * WIDE):
                for x in (1, NX):
                    dst[f, x, ROWS] = apply(src, f, x)
            if turn == 0:
                for way in range(2):
                    start("x", way, x_copy(1, way, group))

    outer(buf_p, buf_q, 0)

    for way in range(2):
        start("y", way, y_copy(1, way))
    pack_z(1)
    for way in range(2):
        start("z", way, z_copy(1, way))
    out_copy = pltpu.make_async_copy(buf_q.at[:, 1:NX + 1, ROWS], ab_hbm, out_sem.at[0])
    out_copy.start()
    total = gather(1, moment(at_p, at_q, 1, NX + 1, none), total)
    total = gather(2, moment(at_q, at_q, 1, NX + 1, none), total)
    for way in range(2):
        arrive("y", way, y_copy(1, way))
        arrive("z", way, z_copy(1, way))
    unpack_z(1)
    inner(buf_q, buf_r, 0)
    third = moment(at_q, at_r, 2, NX, none)
    fourth = moment(at_r, at_r, 2, NX, none)
    outer(buf_q, buf_r, 1)
    for x in (1, NX):
        third = moment(at_q, at_r, x, x + 1, third)
        fourth = moment(at_r, at_r, x, x + 1, fourth)
    total = gather(3, third, total)
    total = gather(4, fourth, total)

    def line_copy(k):
        return pltpu.make_async_remote_copy(
            src_ref=part_z.at[iz], dst_ref=part_z.at[iz],
            send_sem=g_send.at[0], recv_sem=g_recv.at[0],
            device_id=in_line(k), device_id_type=MESH)

    def plane_copy(k):
        return pltpu.make_async_remote_copy(
            src_ref=part_p.at[here], dst_ref=part_p.at[here],
            send_sem=g_send.at[1], recv_sem=g_recv.at[1],
            device_id=in_plane(k), device_id_type=MESH)

    part_z[iz] = total
    for k in range(1, gz):
        line_copy(k).start()
    every = pltpu.make_async_remote_copy(
        src_ref=part_z.at[0:gz - 1], dst_ref=part_z.at[0:gz - 1],
        send_sem=g_send.at[0], recv_sem=g_recv.at[0],
        device_id=in_line(1), device_id_type=MESH)
    every.wait_recv()
    total = part_z[0]
    for k in range(1, gz):
        total = total + part_z[k]
    part_p[here] = total
    for k in range(1, plane):
        plane_copy(k).start()
    most = pltpu.make_async_remote_copy(
        src_ref=part_p.at[0:plane - 1], dst_ref=part_p.at[0:plane - 1],
        send_sem=g_send.at[1], recv_sem=g_recv.at[1],
        device_id=in_plane(1), device_id_type=MESH)
    most.wait_recv()
    total = part_p[0]
    for k in range(1, plane):
        total = total + part_p[k]
    gram_ref[...] = total

    every.wait_send()
    most.wait_send()
    for turn in range(2):
        for way in range(2):
            for group in range(GROUPS):
                sent("x", way, x_copy(turn, way, group))
            sent("y", way, y_copy(turn, way))
            sent("z", way, z_copy(turn, way))
    out_copy.wait()


def combine_kernel(gram_ref, b_hbm, ab_hbm, x_hbm, norm_ref, buf_b, buf_a, buf_x, coeff, load_sem, out_sem):
    load_b = pltpu.make_async_copy(b_hbm, buf_b, load_sem.at[0])
    load_a = pltpu.make_async_copy(ab_hbm, buf_a, load_sem.at[1])
    load_b.start()
    load_a.start()

    gram = gram_ref[...]
    sub = lax.broadcasted_iota(jnp.int32, TILE, 0)
    cell = lax.broadcasted_iota(jnp.int32, TILE, 1)

    def column(order, c):
        k = order * F + c
        return jnp.broadcast_to(gram[:, k:k + 1], TILE)

    def spread(value, row):
        return jnp.broadcast_to(value[row:row + 1], TILE)

    moments = [[column(order, c) for c in range(F)] for order in range(5)]
    columns = [[moments[2][c], moments[3][c]] for c in range(F)]
    columns += [[moments[3][c], moments[4][c]] for c in range(F)]
    rights = [[moments[1][c], moments[2][c]] for c in range(F)]
    for k in range(2 * F):
        half, row = k // F, k % F
        pivot = columns[k]
        inverse = 1.0 / spread(pivot[half], row)
        mine = sub == row
        for other in columns[k + 1:] + rights:
            r = spread(other[half], row) * inverse
            for h in range(2):
                value = other[h] - pivot[h] * r
                other[h] = jnp.where(mine, r, value) if h == half else value
    norms = jnp.zeros((1, 128), jnp.float32)
    for c in range(F):
        for h in range(2):
            coeff[c, h] = rights[c][h]
        fit = moments[1][c] * rights[c][0] + moments[2][c] * rights[c][1]
        left = jnp.where(sub == c, moments[0][c], 0.0) - fit
        norms = jnp.where(cell[0:1] == c, jnp.sum(left, axis=0, keepdims=True), norms)
    norm_ref[...] = jnp.sqrt(jnp.maximum(norms, 0.0))[:, :F]

    load_b.wait()
    load_a.wait()
    pair = 2
    outs = []
    for c0 in range(0, F, pair):
        weights = [[[spread(coeff[c, h], i) for i in range(F)] for h in range(2)] for c in range(c0, c0 + pair)]

        def step(x, _):
            for t in range(NY // 8):
                rows = slice(8 * t, 8 * t + 8)
                fields = [buf_b[:, x, rows], buf_a[:, x, rows]]
                for c in range(pair):
                    sums = [None, None]
                    for h in range(2):
                        for i in range(F):
                            term = weights[c][h][i] * fields[h][i]
                            sums[h] = term if sums[h] is None else sums[h] + term
                    buf_x[c0 + c, x, rows] = sums[0] + sums[1]
            return 0

        lax.fori_loop(0, NX, step, 0)
        out = pltpu.make_async_copy(buf_x.at[c0:c0 + pair], x_hbm.at[c0:c0 + pair], out_sem.at[c0 // pair])
        out.start()
        outs.append(out)
    for out in outs:
        out.wait()


def solution(mesh):
    gx, gy, gz = mesh.shape["gx"], mesh.shape["gy"], mesh.shape["gz"]
    f32 = jnp.float32
    dma = pltpu.SemaphoreType.DMA
    anywhere = pl.BlockSpec(memory_space=pl.ANY)
    vmem = pl.BlockSpec(memory_space=pltpu.VMEM)
    block = (F, NX, NY, NZ)
    padded = (F, NX + 2, NY + 16, NZ)

    def body(right_side, shift):
        gram, images = pl.pallas_call(
            functools.partial(exchange_kernel, gx, gy, gz),
            out_shape=(jax.ShapeDtypeStruct(TILE, f32), jax.ShapeDtypeStruct(block, f32)),
            in_specs=[anywhere, anywhere],
            out_specs=(vmem, anywhere),
            scratch_shapes=[
                pltpu.VMEM(padded, f32),
                pltpu.VMEM(padded, f32),
                pltpu.VMEM(padded, f32),
                pltpu.VMEM((NX, NY, NZ), f32),
                pltpu.VMEM(block, f32),
                pltpu.VMEM((2, 2, 2 * F, NZ), f32),
                pltpu.VMEM((2, 2, 2 * F, NZ), f32),
                pltpu.VMEM((gz,) + TILE, f32),
                pltpu.VMEM((gx * gy,) + TILE, f32),
                dma((4,)),
                dma((2, 2, GROUPS)),
                dma((2, 2, GROUPS)),
                dma((2, 2)),
                dma((2, 2)),
                dma((2, 2)),
                dma((2, 2)),
                dma((2,)),
                dma((2,)),
                dma((1,)),
            ],
            compiler_params=pltpu.CompilerParams(
                collective_id=0, has_side_effects=True, vmem_limit_bytes=24 << 20
            ),
        )(right_side, shift)
        solved, norms = pl.pallas_call(
            combine_kernel,
            out_shape=(jax.ShapeDtypeStruct(block, f32), jax.ShapeDtypeStruct((1, F), f32)),
            in_specs=[vmem, anywhere, anywhere],
            out_specs=(anywhere, vmem),
            scratch_shapes=[
                pltpu.VMEM(block, f32),
                pltpu.VMEM(block, f32),
                pltpu.VMEM(block, f32),
                pltpu.VMEM((F, 2) + TILE, f32),
                dma((2,)),
                dma((F // 2,)),
            ],
            compiler_params=pltpu.CompilerParams(vmem_limit_bytes=16 << 20),
        )(gram, right_side, images)
        return solved, norms.reshape(F)

    return jax.shard_map(
        body,
        mesh=mesh,
        in_specs=(P(None, "gx", "gy", "gz"), P("gx", "gy", "gz")),
        out_specs=(P(None, "gx", "gy", "gz"), P()),
        check_vma=False,
    )
```

```python
import functools

import jax
import jax.numpy as jnp
from jax import lax
from jax.experimental import pallas as pl
from jax.experimental.pallas import tpu as pltpu
from jax.sharding import PartitionSpec as P

MESH = pl.DeviceIdType.MESH
F, NX, NY, NZ = 8, 8, 32, 128
TOP = 8
ROWS = slice(TOP, TOP + NY)
GROUPS = 4
WIDE = F // GROUPS
INNER, FACE = 12, 4
TILE = (8, 128)


def exchange_kernel(gx, gy, gz, b_hbm, s_hbm, gram_ref, buf_p, buf_q,
                    buf_r, diag, side, inner_s, inner_r, face_s, face_r, part_z, part_p,
                    load_sem, xs_sem, xr_sem, ys_sem, yr_sem, zs_sem, zr_sem, g_send, g_recv):
    ix, iy, iz = lax.axis_index("gx"), lax.axis_index("gy"), lax.axis_index("gz")

    loads = [
        pltpu.make_async_copy(b_hbm.at[:, 0], buf_p.at[:, 1, ROWS], load_sem.at[0]),
        pltpu.make_async_copy(b_hbm.at[:, NX - 1], buf_p.at[:, NX, ROWS], load_sem.at[1]),
        pltpu.make_async_copy(b_hbm.at[:, 1:NX - 1], buf_p.at[:, 2:NX, ROWS], load_sem.at[2]),
        pltpu.make_async_copy(s_hbm, diag, load_sem.at[3]),
    ]
    for load in loads:
        load.start()

    chips_y = gy // 2
    core = lax.rem(iy, 2)
    row = iy - core
    xs = [ix] + [lax.rem(ix + k, gx) for k in range(1, gx)]
    ys = [iy] + [lax.rem(iy + 2 * k, gy) for k in range(1, chips_y)]
    zs = [iz] + [lax.rem(iz + k, gz) for k in range(1, gz)]
    across = row + 1 - core
    beyond = lax.rem(iy + gy - 1 + 2 * core, gy)
    line = [(ix, y, zs[k]) for k in dict.fromkeys((1, gz - 1) + tuple(range(2, gz - 1))) for y in (iy, across)]
    line = [(ix, across, iz)] + line
    plane = [(xs[a], ys[b], iz) for a in range(gx) for b in range(chips_y) if a or b]
    near = [(xs[k], iy, iz) for k in dict.fromkeys((1, gx - 1))] + [(ix, beyond, iz)]
    rest = [(xs[a], ys[b], iz) for a in range(gx) for b in range(chips_y) if (a or b) and not (b == 0 and a in (1, gx - 1))]
    greeted = near + line + rest

    barrier = pltpu.get_barrier_semaphore()
    for device in greeted:
        pl.semaphore_signal(barrier, inc=1, device_id=device, device_id_type=MESH)

    zero_x = jnp.zeros((F, NY, NZ), jnp.float32)
    zero_y = jnp.zeros((F, NX, 1, NZ), jnp.float32)
    for turn, buf in enumerate((buf_p, buf_q)):
        @pl.when(ix == 0)
        def _():
            buf[:, 0, ROWS] = zero_x

        @pl.when(ix == gx - 1)
        def _():
            buf[:, NX + 1, ROWS] = zero_x

        @pl.when(iy == 0)
        def _():
            buf[:, 1:NX + 1, TOP - 1:TOP] = zero_y

        @pl.when(iy == gy - 1)
        def _():
            buf[:, 1:NX + 1, TOP + NY:TOP + NY + 1] = zero_y

        for way, edge in enumerate((0, gz - 1)):
            @pl.when(iz == edge)
            def _():
                inner_r[turn, way] = jnp.zeros((INNER, NZ), jnp.float32)
                face_r[turn, way] = jnp.zeros((FACE, NZ), jnp.float32)

    bufs = (buf_p, buf_q)
    has = {
        "x": (ix > 0, ix < gx - 1),
        "y": (iy > 0, iy < gy - 1),
        "z": (iz > 0, iz < gz - 1),
    }

    def x_copy(turn, way, group):
        fields = slice(group * WIDE, (group + 1) * WIDE)
        buf = bufs[turn]
        return pltpu.make_async_remote_copy(
            src_ref=buf.at[fields, NX if way else 1, ROWS],
            dst_ref=buf.at[fields, 0 if way else NX + 1, ROWS],
            send_sem=xs_sem.at[turn, way, group],
            recv_sem=xr_sem.at[turn, way, group],
            device_id=(ix + 1 if way else ix - 1, iy, iz),
            device_id_type=MESH,
        )

    planes = (slice(2, NX), slice(1, 2), slice(NX, NX + 1))

    def y_copy(turn, way, part):
        buf = bufs[turn]
        src, dst = (TOP + NY - 1, TOP - 1) if way else (TOP, TOP + NY)
        return pltpu.make_async_remote_copy(
            src_ref=buf.at[:, planes[part], src:src + 1],
            dst_ref=buf.at[:, planes[part], dst:dst + 1],
            send_sem=ys_sem.at[turn, way, part],
            recv_sem=yr_sem.at[turn, way, part],
            device_id=(ix, iy + 1 if way else iy - 1, iz),
            device_id_type=MESH,
        )

    def z_copy(turn, way, part):
        source, target = ((inner_s, inner_r), (face_s, face_r))[part]
        return pltpu.make_async_remote_copy(
            src_ref=source.at[turn, way],
            dst_ref=target.at[turn, 0 if way else 1],
            send_sem=zs_sem.at[turn, way, part],
            recv_sem=zr_sem.at[turn, way, part],
            device_id=(ix, iy, iz + 1 if way else iz - 1),
            device_id_type=MESH,
        )

    def start(axis, way, copies):
        @pl.when(has[axis][way])
        def _():
            for copy in copies:
                copy.start()

    def arrive(axis, way, copies):
        @pl.when(has[axis][1 - way])
        def _():
            for copy in copies:
                copy.wait_recv()

    def sent(axis, way, copies):
        @pl.when(has[axis][way])
        def _():
            for copy in copies:
                copy.wait_send()

    tiles = ([], [])
    for f in range(0, F, 2):
        tiles[0].append([(f, 2, 6)])
        tiles[0].append([(f, 6, 8), (f + 1, 2, 4)])
        tiles[0].append([(f + 1, 4, 8)])
        tiles[1].append([(f, 1, 2), (f, 8, 9), (f + 1, 1, 2), (f + 1, 8, 9)])

    def pack_z(turn, part):
        buf, target = bufs[turn], (inner_s, face_s)[part]
        for t, pieces in enumerate(tiles[part]):
            tile = jnp.concatenate([buf[f, a:b, ROWS] for f, a, b in pieces], axis=0)
            tile = tile.reshape(NZ, NZ).T
            target[turn, 0, t:t + 1] = tile[0:1]
            target[turn, 1, t:t + 1] = tile[NZ - 1:NZ]

    def unpack_z(turn, part):
        source = (inner_r, face_r)[part]
        for t, pieces in enumerate(tiles[part]):
            low = jnp.broadcast_to(source[turn, 0, t:t + 1], (NZ // 2, NZ))
            high = jnp.broadcast_to(source[turn, 1, t:t + 1], (NZ // 2, NZ))
            tile = jnp.concatenate([low, high], axis=0).T.reshape(4, NY, NZ)
            at = 0
            for f, a, b in pieces:
                side[f, a - 1:b - 1] = tile[at:at + b - a]
                at += b - a

    lane = lax.broadcasted_iota(jnp.int32, (NY, NZ), 1)
    first, last = lane == 0, lane == NZ - 1

    def apply(src, dst, f, x):
        c = src[f, x, ROWS]
        edge = side[f, x - 1]
        beside = src[f, x + 1, ROWS] + src[f, x - 1, ROWS]
        beside = beside + src[f, x, TOP + 1:TOP + NY + 1] + src[f, x, TOP - 1:TOP + NY - 1]
        up = jnp.where(last, edge, pltpu.roll(c, NZ - 1, 1))
        down = jnp.where(first, edge, pltpu.roll(c, 1, 1))
        beside = beside + up + down
        dst[f, x, ROWS] = (6.0 + diag[x - 1]) * c - beside

    def moment(left, right, low, high, sums):
        def step(x, sums):
            for t in range(NY // 8):
                rows = slice(TOP + 8 * t, TOP + 8 * t + 8)
                u = left[:, x, rows]
                v = u if right is left else right[:, x, rows]
                sums = tuple(sums[i] + u[i:i + 1] * v[i:] for i in range(F))
            return sums

        return lax.fori_loop(low, high, step, sums)

    def faces(left, right, sums):
        def step(k, sums):
            x = 1 + (NX - 1) * k
            for t in range(NY // 8):
                rows = slice(TOP + 8 * t, TOP + 8 * t + 8)
                u = left[:, x, rows]
                v = u if right is left else right[:, x, rows]
                sums = tuple(sums[i] + u[i:i + 1] * v[i:] for i in range(F))
            return sums

        return lax.fori_loop(0, 2, step, sums)

    none = tuple(jnp.zeros((F - i,) + TILE, jnp.float32) for i in range(F))

    sub = lax.broadcasted_iota(jnp.int32, TILE, 0)
    cell = lax.broadcasted_iota(jnp.int32, TILE, 1)

    def fold(parts):
        width = 1
        while len(parts) > 1:
            odd = (sub & width) != 0
            merged = []
            for i in range(0, len(parts), 2):
                a, b = parts[i], parts[i + 1]
                kept = jnp.where(odd, b, a)
                moved = jnp.where(odd, a, b)
                moved = jnp.where(odd, pltpu.roll(moved, width, 0), pltpu.roll(moved, 8 - width, 0))
                merged.append(kept + moved)
            parts = merged
            width *= 2
        return parts[0]

    def gather(order, sums, total):
        for c in range(F):
            line = fold([sums[min(i, c)][max(i, c) - min(i, c)] for i in range(F)])
            total = jnp.where(cell == order * F + c, jnp.sum(line, axis=1, keepdims=True), total)
        return total

    def inner(src, dst):
        def step(f, _):
            for x in range(2, NX):
                apply(src, dst, f, x)
            return 0

        lax.fori_loop(0, F, step, 0)

    def outer(src, dst, turn, group):
        for way in range(2):
            arrive("x", way, [x_copy(turn, way, group)])
        for f in range(group * WIDE, (group + 1) * WIDE):
            for x in (1, NX):
                apply(src, dst, f, x)
        if turn == 0:
            for way in range(2):
                start("x", way, [x_copy(1, way, group)])

    both = range(2)
    loads[0].wait()
    loads[1].wait()
    pl.semaphore_wait(barrier, len(greeted))
    for way in both:
        start("x", way, [x_copy(0, way, group) for group in range(GROUPS)])
    loads[2].wait()
    for way in both:
        start("y", way, [y_copy(0, way, part) for part in range(3)])
    for part in both:
        pack_z(0, part)
    for way in both:
        start("z", way, [z_copy(0, way, part) for part in both])
    loads[3].wait()
    zeroth = moment(buf_p, buf_p, 1, NX + 1, none)
    total = gather(0, zeroth, jnp.zeros(TILE, jnp.float32))
    for way in both:
        arrive("y", way, [y_copy(0, way, part) for part in range(3)])
        arrive("z", way, [z_copy(0, way, part) for part in both])
    for part in both:
        unpack_z(0, part)

    outer(buf_p, buf_q, 0, 0)
    inner(buf_p, buf_q)
    for way in both:
        start("y", way, [y_copy(1, way, 0)])
    pack_z(1, 0)
    for way in both:
        start("z", way, [z_copy(1, way, 0)])
    for group in range(1, GROUPS):
        outer(buf_p, buf_q, 0, group)
    for way in both:
        start("y", way, [y_copy(1, way, part) for part in (1, 2)])
    pack_z(1, 1)
    for way in both:
        start("z", way, [z_copy(1, way, 1)])
    total = gather(1, moment(buf_p, buf_q, 1, NX + 1, none), total)
    total = gather(2, moment(buf_q, buf_q, 1, NX + 1, none), total)

    for way in both:
        arrive("y", way, [y_copy(1, way, 0)])
        arrive("z", way, [z_copy(1, way, 0)])
    unpack_z(1, 0)
    inner(buf_q, buf_r)
    third = moment(buf_q, buf_r, 2, NX, none)
    fourth = moment(buf_r, buf_r, 2, NX, none)
    for way in both:
        arrive("y", way, [y_copy(1, way, part) for part in (1, 2)])
        arrive("z", way, [z_copy(1, way, 1)])
    unpack_z(1, 1)
    for group in range(GROUPS):
        outer(buf_q, buf_r, 1, group)
    third = faces(buf_q, buf_r, third)
    fourth = faces(buf_r, buf_r, fourth)
    total = gather(3, third, total)
    total = gather(4, fourth, total)

    def spread(stage, parts, mine, devices, total):
        slots = len(devices) + 1
        parts[mine] = total

        def copy(src, dst, device):
            return pltpu.make_async_remote_copy(
                src_ref=src, dst_ref=dst,
                send_sem=g_send.at[stage], recv_sem=g_recv.at[stage],
                device_id=device, device_id_type=MESH)

        for device in devices:
            copy(parts.at[mine], parts.at[mine], device).start()
        every = copy(parts.at[0:slots - 1], parts.at[0:slots - 1], devices[0])
        every.wait_recv()
        sums = [parts[k] for k in range(slots)]
        while len(sums) > 1:
            sums = [sums[k] + sums[k + 1] for k in range(0, len(sums), 2)]
        return sums[0], every

    total, lines_done = spread(0, part_z, 2 * iz + core, line, total)
    total, planes_done = spread(1, part_p, ix * chips_y + lax.div(row, 2), plane, total)
    gram_ref[...] = total

    lines_done.wait_send()
    planes_done.wait_send()
    for turn in both:
        for way in both:
            sent("x", way, [x_copy(turn, way, group) for group in range(GROUPS)])
            sent("y", way, [y_copy(turn, way, part) for part in range(3)])
            sent("z", way, [z_copy(turn, way, part) for part in both])


def combine_kernel(gram_ref, buf_b, buf_a, x_hbm, norm_ref, buf_x, coeff, out_sem):
    gram = gram_ref[...]
    sub = lax.broadcasted_iota(jnp.int32, TILE, 0)
    cell = lax.broadcasted_iota(jnp.int32, TILE, 1)

    def column(order, c):
        k = order * F + c
        return jnp.broadcast_to(gram[:, k:k + 1], TILE)

    def spread(value, row):
        return jnp.broadcast_to(value[row:row + 1], TILE)

    moments = [[column(order, c) for c in range(F)] for order in range(5)]
    columns = [[moments[2][c], moments[3][c]] for c in range(F)]
    columns += [[moments[3][c], moments[4][c]] for c in range(F)]
    rights = [[moments[1][c], moments[2][c]] for c in range(F)]
    for k in range(2 * F):
        half, row = k // F, k % F
        pivot = columns[k]
        inverse = 1.0 / spread(pivot[half], row)
        mine = sub == row
        for other in columns[k + 1:] + rights:
            r = spread(other[half], row) * inverse
            for h in range(2):
                value = other[h] - pivot[h] * r
                other[h] = jnp.where(mine, r, value) if h == half else value
    norms = jnp.zeros((1, 128), jnp.float32)
    for c in range(F):
        for h in range(2):
            coeff[c, h] = rights[c][h]
        fit = moments[1][c] * rights[c][0] + moments[2][c] * rights[c][1]
        left = jnp.where(sub == c, moments[0][c], 0.0) - fit
        norms = jnp.where(cell[0:1] == c, jnp.sum(left, axis=0, keepdims=True), norms)
    norm_ref[...] = jnp.sqrt(jnp.maximum(norms, 0.0))[:, :F]

    pair = 2
    outs = []
    for c0 in range(0, F, pair):
        weights = [[[spread(coeff[c, h], i) for i in range(F)] for h in range(2)] for c in range(c0, c0 + pair)]

        def step(x, _):
            for t in range(NY // 8):
                rows = slice(8 * t, 8 * t + 8)
                held = slice(TOP + 8 * t, TOP + 8 * t + 8)
                fields = [buf_b[:, x + 1, held], buf_a[:, x + 1, held]]
                for c in range(pair):
                    sums = [None, None]
                    for h in range(2):
                        for i in range(F):
                            term = weights[c][h][i] * fields[h][i]
                            sums[h] = term if sums[h] is None else sums[h] + term
                    buf_x[c0 + c, x, rows] = sums[0] + sums[1]
            return 0

        lax.fori_loop(0, NX, step, 0)
        out = pltpu.make_async_copy(buf_x.at[c0:c0 + pair], x_hbm.at[c0:c0 + pair], out_sem.at[c0 // pair])
        out.start()
        outs.append(out)
    for out in outs:
        out.wait()


def solution(mesh):
    gx, gy, gz = mesh.shape["gx"], mesh.shape["gy"], mesh.shape["gz"]
    f32 = jnp.float32
    dma = pltpu.SemaphoreType.DMA
    hbm = pl.BlockSpec(memory_space=pltpu.HBM)
    vmem = pl.BlockSpec(memory_space=pltpu.VMEM)
    block = (F, NX, NY, NZ)
    padded = (F, NX + 2, NY + 16, NZ)

    def body(right_side, shift):
        gram, fields, images = pl.pallas_call(
            functools.partial(exchange_kernel, gx, gy, gz),
            out_shape=(
                jax.ShapeDtypeStruct(TILE, f32),
                jax.ShapeDtypeStruct(padded, f32),
                jax.ShapeDtypeStruct(padded, f32),
            ),
            in_specs=[hbm, hbm],
            out_specs=(vmem, vmem, vmem),
            scratch_shapes=[
                pltpu.VMEM(padded, f32),
                pltpu.VMEM((NX, NY, NZ), f32),
                pltpu.VMEM(block, f32),
                pltpu.VMEM((2, 2, INNER, NZ), f32),
                pltpu.VMEM((2, 2, INNER, NZ), f32),
                pltpu.VMEM((2, 2, FACE, NZ), f32),
                pltpu.VMEM((2, 2, FACE, NZ), f32),
                pltpu.VMEM((2 * gz,) + TILE, f32),
                pltpu.VMEM((gx * gy // 2,) + TILE, f32),
                dma((4,)),
                dma((2, 2, GROUPS)),
                dma((2, 2, GROUPS)),
                dma((2, 2, 3)),
                dma((2, 2, 3)),
                dma((2, 2, 2)),
                dma((2, 2, 2)),
                dma((2,)),
                dma((2,)),
            ],
            compiler_params=pltpu.CompilerParams(
                collective_id=0, has_side_effects=True, vmem_limit_bytes=24 << 20
            ),
        )(*(pltpu.with_memory_space_constraint(a, pltpu.HBM) for a in (right_side, shift)))
        solved, norms = pl.pallas_call(
            combine_kernel,
            out_shape=(jax.ShapeDtypeStruct(block, f32), jax.ShapeDtypeStruct((1, F), f32)),
            in_specs=[vmem, vmem, vmem],
            out_specs=(hbm, vmem),
            scratch_shapes=[
                pltpu.VMEM(block, f32),
                pltpu.VMEM((F, 2) + TILE, f32),
                dma((F // 2,)),
            ],
            compiler_params=pltpu.CompilerParams(vmem_limit_bytes=16 << 20),
        )(gram, fields, images)
        return solved, norms.reshape(F)

    return jax.shard_map(
        body,
        mesh=mesh,
        in_specs=(P(None, "gx", "gy", "gz"), P("gx", "gy", "gz")),
        out_specs=(P(None, "gx", "gy", "gz"), P()),
        check_vma=False,
    )
```

```python
import functools

import jax
import jax.numpy as jnp
from jax import lax
from jax.experimental import pallas as pl
from jax.experimental.pallas import tpu as pltpu
from jax.sharding import PartitionSpec as P

MESH = pl.DeviceIdType.MESH
F, NX, NY, NZ = 8, 8, 32, 128
TOP = 8
ROWS = slice(TOP, TOP + NY)
GROUPS = 4
WIDE = F // GROUPS
INNER, FACE = 12, 4
TILE = (8, 128)


def exchange_kernel(gx, gy, gz, b_hbm, s_hbm, gram_ref, buf_p, buf_q,
                    buf_r, diag, y_halo, inner_s, inner_r, face_s, face_r, part_z, part_p,
                    load_sem, xs_sem, xr_sem, ys_sem, yr_sem, zs_sem, zr_sem, g_send, g_recv):
    ix, iy, iz = lax.axis_index("gx"), lax.axis_index("gy"), lax.axis_index("gz")

    loads = [
        pltpu.make_async_copy(b_hbm.at[:, 0], buf_p.at[:, 1, ROWS], load_sem.at[0]),
        pltpu.make_async_copy(b_hbm.at[:, NX - 1], buf_p.at[:, NX, ROWS], load_sem.at[1]),
        pltpu.make_async_copy(b_hbm.at[:, 1:NX - 1], buf_p.at[:, 2:NX, ROWS], load_sem.at[2]),
        pltpu.make_async_copy(s_hbm, diag, load_sem.at[3]),
    ]
    for load in loads:
        load.start()

    chips_y = gy // 2
    core = lax.rem(iy, 2)
    row = iy - core
    xs = [ix] + [lax.rem(ix + k, gx) for k in range(1, gx)]
    ys = [iy] + [lax.rem(iy + 2 * k, gy) for k in range(1, chips_y)]
    zs = [iz] + [lax.rem(iz + k, gz) for k in range(1, gz)]
    across = row + 1 - core
    beyond = lax.rem(iy + gy - 1 + 2 * core, gy)
    line = [(ix, y, zs[k]) for k in dict.fromkeys((1, gz - 1) + tuple(range(2, gz - 1))) for y in (iy, across)]
    line = [(ix, across, iz)] + line
    plane = [(xs[a], ys[b], iz) for a in range(gx) for b in range(chips_y) if a or b]
    near = [(xs[k], iy, iz) for k in dict.fromkeys((1, gx - 1))] + [(ix, beyond, iz)]
    rest = [(xs[a], ys[b], iz) for a in range(gx) for b in range(chips_y) if (a or b) and not (b == 0 and a in (1, gx - 1))]
    greeted = near + line + rest

    barrier = pltpu.get_barrier_semaphore()
    for device in greeted:
        pl.semaphore_signal(barrier, inc=1, device_id=device, device_id_type=MESH)

    zero_x = jnp.zeros((F, NY, NZ), jnp.float32)
    zero_y = jnp.zeros((F, NX, 1, NZ), jnp.float32)
    for turn, buf in enumerate((buf_p, buf_q)):
        buf[:, 1:NX + 1, TOP - 1:TOP] = zero_y
        buf[:, 1:NX + 1, TOP + NY:TOP + NY + 1] = zero_y
        for way in range(2):
            @pl.when(ix == way * (gx - 1))
            def _():
                buf[:, way * (NX + 1), ROWS] = zero_x

            @pl.when(iy == way * (gy - 1))
            def _():
                y_halo[turn, way] = zero_y

            @pl.when(iz == way * (gz - 1))
            def _():
                inner_r[turn, way] = jnp.zeros((INNER, NZ), jnp.float32)
                face_r[turn, way] = jnp.zeros((FACE, NZ), jnp.float32)

    bufs, both = (buf_p, buf_q), range(2)
    has = {
        "x": (ix > 0, ix < gx - 1),
        "y": (iy > 0, iy < gy - 1),
        "z": (iz > 0, iz < gz - 1),
    }

    def x_copy(turn, way, group):
        fields = slice(group * WIDE, (group + 1) * WIDE)
        buf = bufs[turn]
        return pltpu.make_async_remote_copy(
            src_ref=buf.at[fields, NX if way else 1, ROWS],
            dst_ref=buf.at[fields, 0 if way else NX + 1, ROWS],
            send_sem=xs_sem.at[turn, way, group],
            recv_sem=xr_sem.at[turn, way, group],
            device_id=(ix + 1 if way else ix - 1, iy, iz),
            device_id_type=MESH,
        )

    spans = ((2, NX), (1, 2), (NX, NX + 1))

    def y_copy(turn, way, part):
        buf, (low, high) = bufs[turn], spans[part]
        edge = TOP + NY - 1 if way else TOP
        return pltpu.make_async_remote_copy(
            src_ref=buf.at[:, low:high, edge:edge + 1],
            dst_ref=y_halo.at[turn, 1 - way, :, low - 1:high - 1],
            send_sem=ys_sem.at[turn, way, part],
            recv_sem=yr_sem.at[turn, way, part],
            device_id=(ix, iy + 1 if way else iy - 1, iz),
            device_id_type=MESH,
        )

    def z_copy(turn, way, part):
        source, target = ((inner_s, inner_r), (face_s, face_r))[part]
        return pltpu.make_async_remote_copy(
            src_ref=source.at[turn, way],
            dst_ref=target.at[turn, 0 if way else 1],
            send_sem=zs_sem.at[turn, way, part],
            recv_sem=zr_sem.at[turn, way, part],
            device_id=(ix, iy, iz + 1 if way else iz - 1),
            device_id_type=MESH,
        )

    def start(axis, way, copies):
        @pl.when(has[axis][way])
        def _():
            for copy in copies:
                copy.start()

    def arrive(axis, way, copies):
        @pl.when(has[axis][1 - way])
        def _():
            for copy in copies:
                copy.wait_recv()

    def sent(axis, way, copies):
        @pl.when(has[axis][way])
        def _():
            for copy in copies:
                copy.wait_send()

    tiles = ([], [])
    for f in range(0, F, 2):
        tiles[0].append([(f, 2, 6)])
        tiles[0].append([(f, 6, 8), (f + 1, 2, 4)])
        tiles[0].append([(f + 1, 4, 8)])
        tiles[1].append([(f, 1, 2), (f, 8, 9), (f + 1, 1, 2), (f + 1, 8, 9)])

    def pack_z(turn, part):
        buf, target = bufs[turn], (inner_s, face_s)[part]
        for t, pieces in enumerate(tiles[part]):
            tile = jnp.concatenate([buf[f, a:b, ROWS] for f, a, b in pieces], axis=0)
            tile = tile.reshape(NZ, NZ).T
            target[turn, 0, t:t + 1] = tile[0:1]
            target[turn, 1, t:t + 1] = tile[NZ - 1:NZ]

    lane = lax.broadcasted_iota(jnp.int32, (NY, NZ), 1)
    first, last = lane == 0, lane == NZ - 1
    edges = jnp.logical_or(first, last)

    def apply(src, dst, f, x):
        c = src[f, x, ROWS]
        beside = src[f, x, TOP + 1:TOP + NY + 1] + src[f, x, TOP - 1:TOP + NY - 1]
        for other in (x - 1, x + 1):
            if 1 <= other <= NX:
                beside = beside + src[f, other, ROWS]
        beside = beside + jnp.where(last, 0.0, pltpu.roll(c, NZ - 1, 1))
        beside = beside + jnp.where(first, 0.0, pltpu.roll(c, 1, 1))
        dst[f, x, ROWS] = diag[x - 1] * c - beside

    def inside(src, dst):
        def step(f, _):
            for x in range(1, NX + 1):
                apply(src, dst, f, x)
            return 0

        lax.fori_loop(0, F, step, 0)

    def take_x(src, dst, turn, group):
        for way in both:
            arrive("x", way, [x_copy(turn, way, group)])
        for f in range(group * WIDE, (group + 1) * WIDE):
            dst[f, 1, ROWS] -= src[f, 0, ROWS]
            dst[f, NX, ROWS] -= src[f, NX + 1, ROWS]

    def take_y(dst, turn, parts):
        for way in both:
            arrive("y", way, [y_copy(turn, way, part) for part in parts])
        for part in parts:
            low, high = spans[part]
            for way, edge in enumerate((TOP, TOP + NY - 1)):
                dst[:, low:high, edge:edge + 1] -= y_halo[turn, way, :, low - 1:high - 1]

    def take_z(dst, turn, part):
        for way in both:
            arrive("z", way, [z_copy(turn, way, part)])
        source = (inner_r, face_r)[part]
        for t, pieces in enumerate(tiles[part]):
            low = jnp.broadcast_to(source[turn, 0, t:t + 1], (NZ // 2, NZ))
            high = jnp.broadcast_to(source[turn, 1, t:t + 1], (NZ // 2, NZ))
            tile = jnp.concatenate([low, high], axis=0).T.reshape(4, NY, NZ)
            at = 0
            for f, a, b in pieces:
                dst[f, a:b, ROWS] -= jnp.where(edges, tile[at:at + b - a], 0.0)
                at += b - a

    def moment(left, right, low, high, sums):
        def step(x, sums):
            for t in range(NY // 8):
                rows = slice(TOP + 8 * t, TOP + 8 * t + 8)
                u = left[:, x, rows]
                v = u if right is left else right[:, x, rows]
                sums = tuple(sums[i] + u[i:i + 1] * v[i:] for i in range(F))
            return sums

        return lax.fori_loop(low, high, step, sums)

    def faces(left, right, sums):
        def step(k, sums):
            x = 1 + (NX - 1) * k
            for t in range(NY // 8):
                rows = slice(TOP + 8 * t, TOP + 8 * t + 8)
                u = left[:, x, rows]
                v = u if right is left else right[:, x, rows]
                sums = tuple(sums[i] + u[i:i + 1] * v[i:] for i in range(F))
            return sums

        return lax.fori_loop(0, 2, step, sums)

    none = tuple(jnp.zeros((F - i,) + TILE, jnp.float32) for i in range(F))

    sub = lax.broadcasted_iota(jnp.int32, TILE, 0)
    cell = lax.broadcasted_iota(jnp.int32, TILE, 1)

    def fold(parts):
        width = 1
        while len(parts) > 1:
            odd = (sub & width) != 0
            merged = []
            for i in range(0, len(parts), 2):
                a, b = parts[i], parts[i + 1]
                kept = jnp.where(odd, b, a)
                moved = jnp.where(odd, a, b)
                moved = jnp.where(odd, pltpu.roll(moved, width, 0), pltpu.roll(moved, 8 - width, 0))
                merged.append(kept + moved)
            parts = merged
            width *= 2
        return parts[0]

    def gather(order, sums, total):
        for c in range(F):
            line = fold([sums[min(i, c)][max(i, c) - min(i, c)] for i in range(F)])
            total = jnp.where(cell == order * F + c, jnp.sum(line, axis=1, keepdims=True), total)
        return total

    loads[0].wait()
    loads[1].wait()
    pl.semaphore_wait(barrier, len(greeted))
    for way in both:
        start("x", way, [x_copy(0, way, group) for group in range(GROUPS)])
    loads[2].wait()
    for way in both:
        start("y", way, [y_copy(0, way, part) for part in range(3)])
    for part in both:
        pack_z(0, part)
    for way in both:
        start("z", way, [z_copy(0, way, part) for part in both])
    loads[3].wait()
    diag[...] = 6.0 + diag[...]
    inside(buf_p, buf_q)
    zeroth = moment(buf_p, buf_p, 1, NX + 1, none)
    total = gather(0, zeroth, jnp.zeros(TILE, jnp.float32))
    take_y(buf_q, 0, range(3))
    for part in both:
        take_z(buf_q, 0, part)

    def forward(group):
        take_x(buf_p, buf_q, 0, group)
        for way in both:
            start("x", way, [x_copy(1, way, group)])

    forward(0)
    for way in both:
        start("y", way, [y_copy(1, way, 0)])
    pack_z(1, 0)
    for way in both:
        start("z", way, [z_copy(1, way, 0)])
    forward(1)
    first_sums = moment(buf_p, buf_q, 2, NX, none)
    forward(2)
    second_sums = moment(buf_q, buf_q, 2, NX, none)
    for group in range(3, GROUPS):
        forward(group)
    for way in both:
        start("y", way, [y_copy(1, way, part) for part in (1, 2)])
    pack_z(1, 1)
    for way in both:
        start("z", way, [z_copy(1, way, 1)])

    inside(buf_q, buf_r)
    total = gather(1, faces(buf_p, buf_q, first_sums), total)
    total = gather(2, faces(buf_q, buf_q, second_sums), total)
    take_y(buf_r, 1, (0,))
    take_z(buf_r, 1, 0)
    third = moment(buf_q, buf_r, 2, NX, none)
    fourth = moment(buf_r, buf_r, 2, NX, none)
    take_y(buf_r, 1, (1, 2))
    take_z(buf_r, 1, 1)
    for group in range(GROUPS):
        take_x(buf_q, buf_r, 1, group)
    third = faces(buf_q, buf_r, third)
    fourth = faces(buf_r, buf_r, fourth)
    total = gather(3, third, total)
    total = gather(4, fourth, total)

    def spread(stage, parts, mine, devices, total):
        slots = len(devices) + 1
        parts[mine] = total

        def copy(src, dst, device):
            return pltpu.make_async_remote_copy(
                src_ref=src, dst_ref=dst,
                send_sem=g_send.at[stage], recv_sem=g_recv.at[stage],
                device_id=device, device_id_type=MESH)

        for device in devices:
            copy(parts.at[mine], parts.at[mine], device).start()
        every = copy(parts.at[0:slots - 1], parts.at[0:slots - 1], devices[0])
        every.wait_recv()
        sums = [parts[k] for k in range(slots)]
        while len(sums) > 1:
            sums = [sums[k] + sums[k + 1] for k in range(0, len(sums), 2)]
        return sums[0], every

    total, lines_done = spread(0, part_z, 2 * iz + core, line, total)
    total, planes_done = spread(1, part_p, ix * chips_y + lax.div(row, 2), plane, total)
    gram_ref[...] = total

    lines_done.wait_send()
    planes_done.wait_send()
    for turn in both:
        for way in both:
            sent("x", way, [x_copy(turn, way, group) for group in range(GROUPS)])
            sent("y", way, [y_copy(turn, way, part) for part in range(3)])
            sent("z", way, [z_copy(turn, way, part) for part in both])


def combine_kernel(gram_ref, buf_b, buf_a, x_hbm, norm_ref, buf_x, coeff, out_sem):
    gram = gram_ref[...]
    sub = lax.broadcasted_iota(jnp.int32, TILE, 0)
    cell = lax.broadcasted_iota(jnp.int32, TILE, 1)

    def column(order, c):
        k = order * F + c
        return jnp.broadcast_to(gram[:, k:k + 1], TILE)

    def spread(value, row):
        return jnp.broadcast_to(value[row:row + 1], TILE)

    moments = [[column(order, c) for c in range(F)] for order in range(5)]
    columns = [[moments[2][c], moments[3][c]] for c in range(F)]
    columns += [[moments[3][c], moments[4][c]] for c in range(F)]
    rights = [[moments[1][c], moments[2][c]] for c in range(F)]
    for k in range(2 * F):
        half, row = k // F, k % F
        pivot = columns[k]
        inverse = 1.0 / spread(pivot[half], row)
        mine = sub == row
        for other in columns[k + 1:] + rights:
            r = spread(other[half], row) * inverse
            for h in range(2):
                value = other[h] - pivot[h] * r
                other[h] = jnp.where(mine, r, value) if h == half else value
    norms = jnp.zeros((1, 128), jnp.float32)
    for c in range(F):
        for h in range(2):
            coeff[c, h] = rights[c][h]
        fit = moments[1][c] * rights[c][0] + moments[2][c] * rights[c][1]
        left = jnp.where(sub == c, moments[0][c], 0.0) - fit
        norms = jnp.where(cell[0:1] == c, jnp.sum(left, axis=0, keepdims=True), norms)
    norm_ref[...] = jnp.sqrt(jnp.maximum(norms, 0.0))[:, :F]

    pair = 2
    outs = []
    for c0 in range(0, F, pair):
        weights = [[[spread(coeff[c, h], i) for i in range(F)] for h in range(2)] for c in range(c0, c0 + pair)]

        def step(x, _):
            for t in range(NY // 8):
                rows = slice(8 * t, 8 * t + 8)
                held = slice(TOP + 8 * t, TOP + 8 * t + 8)
                fields = [buf_b[:, x + 1, held], buf_a[:, x + 1, held]]
                for c in range(pair):
                    sums = [None, None]
                    for h in range(2):
                        for i in range(F):
                            term = weights[c][h][i] * fields[h][i]
                            sums[h] = term if sums[h] is None else sums[h] + term
                    buf_x[c0 + c, x, rows] = sums[0] + sums[1]
            return 0

        lax.fori_loop(0, NX, step, 0)
        out = pltpu.make_async_copy(buf_x.at[c0:c0 + pair], x_hbm.at[c0:c0 + pair], out_sem.at[c0 // pair])
        out.start()
        outs.append(out)
    for out in outs:
        out.wait()


def solution(mesh):
    gx, gy, gz = mesh.shape["gx"], mesh.shape["gy"], mesh.shape["gz"]
    f32 = jnp.float32
    dma = pltpu.SemaphoreType.DMA
    hbm = pl.BlockSpec(memory_space=pltpu.HBM)
    vmem = pl.BlockSpec(memory_space=pltpu.VMEM)
    block = (F, NX, NY, NZ)
    padded = (F, NX + 2, NY + 16, NZ)

    def body(right_side, shift):
        gram, fields, images = pl.pallas_call(
            functools.partial(exchange_kernel, gx, gy, gz),
            out_shape=(
                jax.ShapeDtypeStruct(TILE, f32),
                jax.ShapeDtypeStruct(padded, f32),
                jax.ShapeDtypeStruct(padded, f32),
            ),
            in_specs=[hbm, hbm],
            out_specs=(vmem, vmem, vmem),
            scratch_shapes=[
                pltpu.VMEM(padded, f32),
                pltpu.VMEM((NX, NY, NZ), f32),
                pltpu.VMEM((2, 2, F, NX, 1, NZ), f32),
                pltpu.VMEM((2, 2, INNER, NZ), f32),
                pltpu.VMEM((2, 2, INNER, NZ), f32),
                pltpu.VMEM((2, 2, FACE, NZ), f32),
                pltpu.VMEM((2, 2, FACE, NZ), f32),
                pltpu.VMEM((2 * gz,) + TILE, f32),
                pltpu.VMEM((gx * gy // 2,) + TILE, f32),
                dma((4,)),
                dma((2, 2, GROUPS)),
                dma((2, 2, GROUPS)),
                dma((2, 2, 3)),
                dma((2, 2, 3)),
                dma((2, 2, 2)),
                dma((2, 2, 2)),
                dma((2,)),
                dma((2,)),
            ],
            compiler_params=pltpu.CompilerParams(
                collective_id=0, has_side_effects=True, vmem_limit_bytes=24 << 20
            ),
        )(*(pltpu.with_memory_space_constraint(a, pltpu.HBM) for a in (right_side, shift)))
        solved, norms = pl.pallas_call(
            combine_kernel,
            out_shape=(jax.ShapeDtypeStruct(block, f32), jax.ShapeDtypeStruct((1, F), f32)),
            in_specs=[vmem, vmem, vmem],
            out_specs=(hbm, vmem),
            scratch_shapes=[
                pltpu.VMEM(block, f32),
                pltpu.VMEM((F, 2) + TILE, f32),
                dma((F // 2,)),
            ],
            compiler_params=pltpu.CompilerParams(vmem_limit_bytes=16 << 20),
        )(gram, fields, images)
        return solved, norms.reshape(F)

    return jax.shard_map(
        body,
        mesh=mesh,
        in_specs=(P(None, "gx", "gy", "gz"), P("gx", "gy", "gz")),
        out_specs=(P(None, "gx", "gy", "gz"), P()),
        check_vma=False,
    )
```

```python
import functools

import jax
import jax.numpy as jnp
from jax import lax
from jax.experimental import pallas as pl
from jax.experimental.pallas import tpu as pltpu
from jax.sharding import PartitionSpec as P

MESH = pl.DeviceIdType.MESH
F, NX, NY, NZ = 8, 8, 32, 128
TOP = 8
ROWS = slice(TOP, TOP + NY)
GROUPS = 4
WIDE = F // GROUPS
INNER, FACE = 12, 4
TILE = (8, 128)


def exchange_kernel(gx, gy, gz, b_hbm, s_hbm, gram_ref, buf_p, buf_q,
                    buf_r, diag, y_halo, inner_s, inner_r, face_s, face_r, part_z, part_p,
                    load_sem, xs_sem, xr_sem, ys_sem, yr_sem, zs_sem, zr_sem, g_send, g_recv, heard):
    ix, iy, iz = lax.axis_index("gx"), lax.axis_index("gy"), lax.axis_index("gz")

    loads = [
        pltpu.make_async_copy(b_hbm.at[:, 0], buf_p.at[:, 1, ROWS], load_sem.at[0]),
        pltpu.make_async_copy(b_hbm.at[:, NX - 1], buf_p.at[:, NX, ROWS], load_sem.at[1]),
        pltpu.make_async_copy(b_hbm.at[:, 1:NX - 1], buf_p.at[:, 2:NX, ROWS], load_sem.at[2]),
        pltpu.make_async_copy(s_hbm, diag, load_sem.at[3]),
    ]
    for load in loads:
        load.start()

    chips_y = gy // 2
    core = lax.rem(iy, 2)
    row = iy - core
    xs = [ix] + [lax.rem(ix + k, gx) for k in range(1, gx)]
    ys = [iy] + [lax.rem(iy + 2 * k, gy) for k in range(1, chips_y)]
    zs = [iz] + [lax.rem(iz + k, gz) for k in range(1, gz)]
    across = row + 1 - core
    beyond = lax.rem(iy + gy - 1 + 2 * core, gy)
    line = [(ix, y, zs[k]) for k in dict.fromkeys((1, gz - 1) + tuple(range(2, gz - 1))) for y in (iy, across)]
    line = [(ix, across, iz)] + line
    plane = [(xs[a], ys[b], iz) for a in range(gx) for b in range(chips_y) if a or b]
    step_y = [ys[k] for k in dict.fromkeys((1, chips_y - 1))]
    near = [(xs[k], iy, iz) for k in dict.fromkeys((1, gx - 1))] + [(ix, beyond, iz), (ix, across, iz)]
    near += [(ix, iy, zs[k]) for k in dict.fromkeys((1, gz - 1))] + [(ix, y, iz) for y in step_y]
    second = [(xs[2 % gx], iy, iz), (ix, ys[2 % chips_y], iz)] if gx > 2 and chips_y > 2 else []
    second += [(ix, iy, zs[k]) for k in dict.fromkeys((2, gz - 2))] if gz > 3 else []

    barrier = pltpu.get_barrier_semaphore()
    for device in near:
        pl.semaphore_signal(barrier, inc=1, device_id=device, device_id_type=MESH)

    def tell(stage, devices):
        for device in devices:
            pl.semaphore_signal(heard.at[stage], inc=1, device_id=device, device_id_type=MESH)

    zero_x = jnp.zeros((F, NY, NZ), jnp.float32)
    zero_y = jnp.zeros((F, NX, 1, NZ), jnp.float32)
    for turn, buf in enumerate((buf_p, buf_q)):
        buf[:, 1:NX + 1, TOP - 1:TOP] = zero_y
        buf[:, 1:NX + 1, TOP + NY:TOP + NY + 1] = zero_y
        for way in range(2):
            @pl.when(ix == way * (gx - 1))
            def _():
                buf[:, way * (NX + 1), ROWS] = zero_x

            @pl.when(iy == way * (gy - 1))
            def _():
                y_halo[turn, way] = zero_y

            @pl.when(iz == way * (gz - 1))
            def _():
                inner_r[turn, way] = jnp.zeros((INNER, NZ), jnp.float32)
                face_r[turn, way] = jnp.zeros((FACE, NZ), jnp.float32)

    bufs, both = (buf_p, buf_q), range(2)
    has = {
        "x": (ix > 0, ix < gx - 1),
        "y": (iy > 0, iy < gy - 1),
        "z": (iz > 0, iz < gz - 1),
    }

    def x_copy(turn, way, group):
        fields = slice(group * WIDE, (group + 1) * WIDE)
        buf = bufs[turn]
        return pltpu.make_async_remote_copy(
            src_ref=buf.at[fields, NX if way else 1, ROWS],
            dst_ref=buf.at[fields, 0 if way else NX + 1, ROWS],
            send_sem=xs_sem.at[turn, way, group],
            recv_sem=xr_sem.at[turn, way, group],
            device_id=(ix + 1 if way else ix - 1, iy, iz),
            device_id_type=MESH,
        )

    spans = ((2, NX), (1, 2), (NX, NX + 1))

    def y_copy(turn, way, part):
        buf, (low, high) = bufs[turn], spans[part]
        edge = TOP + NY - 1 if way else TOP
        return pltpu.make_async_remote_copy(
            src_ref=buf.at[:, low:high, edge:edge + 1],
            dst_ref=y_halo.at[turn, 1 - way, :, low - 1:high - 1],
            send_sem=ys_sem.at[turn, way, part],
            recv_sem=yr_sem.at[turn, way, part],
            device_id=(ix, iy + 1 if way else iy - 1, iz),
            device_id_type=MESH,
        )

    def z_copy(turn, way, part):
        source, target = ((inner_s, inner_r), (face_s, face_r))[part]
        return pltpu.make_async_remote_copy(
            src_ref=source.at[turn, way],
            dst_ref=target.at[turn, 0 if way else 1],
            send_sem=zs_sem.at[turn, way, part],
            recv_sem=zr_sem.at[turn, way, part],
            device_id=(ix, iy, iz + 1 if way else iz - 1),
            device_id_type=MESH,
        )

    def start(axis, way, copies):
        @pl.when(has[axis][way])
        def _():
            for copy in copies:
                copy.start()

    def arrive(axis, way, copies):
        @pl.when(has[axis][1 - way])
        def _():
            for copy in copies:
                copy.wait_recv()

    def sent(axis, way, copies):
        @pl.when(has[axis][way])
        def _():
            for copy in copies:
                copy.wait_send()

    tiles = ([], [])
    for f in range(0, F, 2):
        tiles[0].append([(f, 2, 6)])
        tiles[0].append([(f, 6, 8), (f + 1, 2, 4)])
        tiles[0].append([(f + 1, 4, 8)])
        tiles[1].append([(f, 1, 2), (f, 8, 9), (f + 1, 1, 2), (f + 1, 8, 9)])

    def pack_z(turn, part):
        buf, target = bufs[turn], (inner_s, face_s)[part]
        for t, pieces in enumerate(tiles[part]):
            tile = jnp.concatenate([buf[f, a:b, ROWS] for f, a, b in pieces], axis=0)
            tile = tile.reshape(NZ, NZ).T
            target[turn, 0, t:t + 1] = tile[0:1]
            target[turn, 1, t:t + 1] = tile[NZ - 1:NZ]

    lane = lax.broadcasted_iota(jnp.int32, (NY, NZ), 1)
    first, last = lane == 0, lane == NZ - 1
    edges = jnp.logical_or(first, last)

    def apply(src, dst, f, x):
        c = src[f, x, ROWS]
        beside = src[f, x, TOP + 1:TOP + NY + 1] + src[f, x, TOP - 1:TOP + NY - 1]
        for other in (x - 1, x + 1):
            if 1 <= other <= NX:
                beside = beside + src[f, other, ROWS]
        beside = beside + jnp.where(last, 0.0, pltpu.roll(c, NZ - 1, 1))
        beside = beside + jnp.where(first, 0.0, pltpu.roll(c, 1, 1))
        dst[f, x, ROWS] = diag[x - 1] * c - beside

    def inside(src, dst):
        def step(f, _):
            for x in range(1, NX + 1):
                apply(src, dst, f, x)
            return 0

        lax.fori_loop(0, F, step, 0)

    def take_x(src, dst, turn, group):
        for way in both:
            arrive("x", way, [x_copy(turn, way, group)])
        for f in range(group * WIDE, (group + 1) * WIDE):
            dst[f, 1, ROWS] -= src[f, 0, ROWS]
            dst[f, NX, ROWS] -= src[f, NX + 1, ROWS]

    def take_y(dst, turn, parts):
        for way in both:
            arrive("y", way, [y_copy(turn, way, part) for part in parts])
        for part in parts:
            low, high = spans[part]
            for way, edge in enumerate((TOP, TOP + NY - 1)):
                dst[:, low:high, edge:edge + 1] -= y_halo[turn, way, :, low - 1:high - 1]

    def take_z(dst, turn, part):
        for way in both:
            arrive("z", way, [z_copy(turn, way, part)])
        source = (inner_r, face_r)[part]
        for t, pieces in enumerate(tiles[part]):
            low = jnp.broadcast_to(source[turn, 0, t:t + 1], (NZ // 2, NZ))
            high = jnp.broadcast_to(source[turn, 1, t:t + 1], (NZ // 2, NZ))
            tile = jnp.concatenate([low, high], axis=0).T.reshape(4, NY, NZ)
            at = 0
            for f, a, b in pieces:
                dst[f, a:b, ROWS] -= jnp.where(edges, tile[at:at + b - a], 0.0)
                at += b - a

    def moment(left, right, low, high, sums):
        def step(x, sums):
            for t in range(NY // 8):
                rows = slice(TOP + 8 * t, TOP + 8 * t + 8)
                u = left[:, x, rows]
                v = u if right is left else right[:, x, rows]
                sums = tuple(sums[i] + u[i:i + 1] * v[i:] for i in range(F))
            return sums

        return lax.fori_loop(low, high, step, sums)

    def faces(left, right, sums):
        def step(k, sums):
            x = 1 + (NX - 1) * k
            for t in range(NY // 8):
                rows = slice(TOP + 8 * t, TOP + 8 * t + 8)
                u = left[:, x, rows]
                v = u if right is left else right[:, x, rows]
                sums = tuple(sums[i] + u[i:i + 1] * v[i:] for i in range(F))
            return sums

        return lax.fori_loop(0, 2, step, sums)

    none = tuple(jnp.zeros((F - i,) + TILE, jnp.float32) for i in range(F))

    sub = lax.broadcasted_iota(jnp.int32, TILE, 0)
    cell = lax.broadcasted_iota(jnp.int32, TILE, 1)

    def fold(parts):
        width = 1
        while len(parts) > 1:
            odd = (sub & width) != 0
            merged = []
            for i in range(0, len(parts), 2):
                a, b = parts[i], parts[i + 1]
                kept = jnp.where(odd, b, a)
                moved = jnp.where(odd, a, b)
                moved = jnp.where(odd, pltpu.roll(moved, width, 0), pltpu.roll(moved, 8 - width, 0))
                merged.append(kept + moved)
            parts = merged
            width *= 2
        return parts[0]

    def gather(order, sums, total):
        for c in range(F):
            line = fold([sums[min(i, c)][max(i, c) - min(i, c)] for i in range(F)])
            total = jnp.where(cell == order * F + c, jnp.sum(line, axis=1, keepdims=True), total)
        return total

    loads[0].wait()
    loads[1].wait()
    pl.semaphore_wait(barrier, len(near))
    for way in both:
        start("x", way, [x_copy(0, way, group) for group in range(GROUPS)])
    tell(0, near)
    loads[2].wait()
    for way in both:
        start("y", way, [y_copy(0, way, part) for part in range(3)])
    for part in both:
        pack_z(0, part)
    for way in both:
        start("z", way, [z_copy(0, way, part) for part in both])
    loads[3].wait()
    diag[...] = 6.0 + diag[...]
    inside(buf_p, buf_q)
    zeroth = moment(buf_p, buf_p, 1, NX + 1, none)
    total = gather(0, zeroth, jnp.zeros(TILE, jnp.float32))
    pl.semaphore_wait(heard.at[0], len(near))
    tell(1, second)
    take_y(buf_q, 0, range(3))
    for part in both:
        take_z(buf_q, 0, part)

    def forward(group):
        take_x(buf_p, buf_q, 0, group)
        for way in both:
            start("x", way, [x_copy(1, way, group)])

    forward(0)
    for way in both:
        start("y", way, [y_copy(1, way, 0)])
    pack_z(1, 0)
    for way in both:
        start("z", way, [z_copy(1, way, 0)])
    forward(1)
    first_sums = moment(buf_p, buf_q, 2, NX, none)
    forward(2)
    second_sums = moment(buf_q, buf_q, 2, NX, none)
    for group in range(3, GROUPS):
        forward(group)
    for way in both:
        start("y", way, [y_copy(1, way, part) for part in (1, 2)])
    pack_z(1, 1)
    for way in both:
        start("z", way, [z_copy(1, way, 1)])

    if second:
        pl.semaphore_wait(heard.at[1], len(second))
    tell(2, [(ix, across, iz)])

    inside(buf_q, buf_r)
    total = gather(1, faces(buf_p, buf_q, first_sums), total)
    total = gather(2, faces(buf_q, buf_q, second_sums), total)
    take_y(buf_r, 1, (0,))
    take_z(buf_r, 1, 0)
    third = moment(buf_q, buf_r, 2, NX, none)
    fourth = moment(buf_r, buf_r, 2, NX, none)
    take_y(buf_r, 1, (1, 2))
    take_z(buf_r, 1, 1)
    for group in range(GROUPS):
        take_x(buf_q, buf_r, 1, group)
    third = faces(buf_q, buf_r, third)
    fourth = faces(buf_r, buf_r, fourth)
    total = gather(3, third, total)
    total = gather(4, fourth, total)

    pl.semaphore_wait(heard.at[2], 1)

    def spread(stage, parts, mine, devices, total):
        slots = len(devices) + 1
        parts[mine] = total

        def copy(src, dst, device):
            return pltpu.make_async_remote_copy(
                src_ref=src, dst_ref=dst,
                send_sem=g_send.at[stage], recv_sem=g_recv.at[stage],
                device_id=device, device_id_type=MESH)

        for device in devices:
            copy(parts.at[mine], parts.at[mine], device).start()
        every = copy(parts.at[0:slots - 1], parts.at[0:slots - 1], devices[0])
        every.wait_recv()
        sums = [parts[k] for k in range(slots)]
        while len(sums) > 1:
            sums = [sums[k] + sums[k + 1] for k in range(0, len(sums), 2)]
        return sums[0], every

    total, lines_done = spread(0, part_z, 2 * iz + core, line, total)
    total, planes_done = spread(1, part_p, ix * chips_y + lax.div(row, 2), plane, total)
    gram_ref[...] = total

    lines_done.wait_send()
    planes_done.wait_send()
    for turn in both:
        for way in both:
            sent("x", way, [x_copy(turn, way, group) for group in range(GROUPS)])
            sent("y", way, [y_copy(turn, way, part) for part in range(3)])
            sent("z", way, [z_copy(turn, way, part) for part in both])


def combine_kernel(gram_ref, buf_b, buf_a, x_hbm, norm_ref, buf_x, coeff, out_sem):
    gram = gram_ref[...]
    sub = lax.broadcasted_iota(jnp.int32, TILE, 0)
    cell = lax.broadcasted_iota(jnp.int32, TILE, 1)

    def column(order, c):
        k = order * F + c
        return jnp.broadcast_to(gram[:, k:k + 1], TILE)

    def spread(value, row):
        return jnp.broadcast_to(value[row:row + 1], TILE)

    moments = [[column(order, c) for c in range(F)] for order in range(5)]
    columns = [[moments[2][c], moments[3][c]] for c in range(F)]
    columns += [[moments[3][c], moments[4][c]] for c in range(F)]
    rights = [[moments[1][c], moments[2][c]] for c in range(F)]
    for k in range(2 * F):
        half, row = k // F, k % F
        pivot = columns[k]
        inverse = 1.0 / spread(pivot[half], row)
        mine = sub == row
        for other in columns[k + 1:] + rights:
            r = spread(other[half], row) * inverse
            for h in range(2):
                value = other[h] - pivot[h] * r
                other[h] = jnp.where(mine, r, value) if h == half else value
    norms = jnp.zeros((1, 128), jnp.float32)
    for c in range(F):
        for h in range(2):
            coeff[c, h] = rights[c][h]
        fit = moments[1][c] * rights[c][0] + moments[2][c] * rights[c][1]
        left = jnp.where(sub == c, moments[0][c], 0.0) - fit
        norms = jnp.where(cell[0:1] == c, jnp.sum(left, axis=0, keepdims=True), norms)
    norm_ref[...] = jnp.sqrt(jnp.maximum(norms, 0.0))[:, :F]

    pair = 2
    outs = []
    for c0 in range(0, F, pair):
        weights = [[[spread(coeff[c, h], i) for i in range(F)] for h in range(2)] for c in range(c0, c0 + pair)]

        def step(x, _):
            for t in range(NY // 8):
                rows = slice(8 * t, 8 * t + 8)
                held = slice(TOP + 8 * t, TOP + 8 * t + 8)
                fields = [buf_b[:, x + 1, held], buf_a[:, x + 1, held]]
                for c in range(pair):
                    sums = [None, None]
                    for h in range(2):
                        for i in range(F):
                            term = weights[c][h][i] * fields[h][i]
                            sums[h] = term if sums[h] is None else sums[h] + term
                    buf_x[c0 + c, x, rows] = sums[0] + sums[1]
            return 0

        lax.fori_loop(0, NX, step, 0)
        out = pltpu.make_async_copy(buf_x.at[c0:c0 + pair], x_hbm.at[c0:c0 + pair], out_sem.at[c0 // pair])
        out.start()
        outs.append(out)
    for out in outs:
        out.wait()


def solution(mesh):
    gx, gy, gz = mesh.shape["gx"], mesh.shape["gy"], mesh.shape["gz"]
    f32 = jnp.float32
    dma = pltpu.SemaphoreType.DMA
    hbm = pl.BlockSpec(memory_space=pltpu.HBM)
    vmem = pl.BlockSpec(memory_space=pltpu.VMEM)
    block = (F, NX, NY, NZ)
    padded = (F, NX + 2, NY + 16, NZ)

    def body(right_side, shift):
        gram, fields, images = pl.pallas_call(
            functools.partial(exchange_kernel, gx, gy, gz),
            out_shape=(
                jax.ShapeDtypeStruct(TILE, f32),
                jax.ShapeDtypeStruct(padded, f32),
                jax.ShapeDtypeStruct(padded, f32),
            ),
            in_specs=[hbm, hbm],
            out_specs=(vmem, vmem, vmem),
            scratch_shapes=[
                pltpu.VMEM(padded, f32),
                pltpu.VMEM((NX, NY, NZ), f32),
                pltpu.VMEM((2, 2, F, NX, 1, NZ), f32),
                pltpu.VMEM((2, 2, INNER, NZ), f32),
                pltpu.VMEM((2, 2, INNER, NZ), f32),
                pltpu.VMEM((2, 2, FACE, NZ), f32),
                pltpu.VMEM((2, 2, FACE, NZ), f32),
                pltpu.VMEM((2 * gz,) + TILE, f32),
                pltpu.VMEM((gx * gy // 2,) + TILE, f32),
                dma((4,)),
                dma((2, 2, GROUPS)),
                dma((2, 2, GROUPS)),
                dma((2, 2, 3)),
                dma((2, 2, 3)),
                dma((2, 2, 2)),
                dma((2, 2, 2)),
                dma((2,)),
                dma((2,)),
                pltpu.SemaphoreType.REGULAR((3,)),
            ],
            compiler_params=pltpu.CompilerParams(
                collective_id=0, has_side_effects=True, vmem_limit_bytes=24 << 20
            ),
        )(*(pltpu.with_memory_space_constraint(a, pltpu.HBM) for a in (right_side, shift)))
        solved, norms = pl.pallas_call(
            combine_kernel,
            out_shape=(jax.ShapeDtypeStruct(block, f32), jax.ShapeDtypeStruct((1, F), f32)),
            in_specs=[vmem, vmem, vmem],
            out_specs=(hbm, vmem),
            scratch_shapes=[
                pltpu.VMEM(block, f32),
                pltpu.VMEM((F, 2) + TILE, f32),
                dma((F // 2,)),
            ],
            compiler_params=pltpu.CompilerParams(vmem_limit_bytes=16 << 20),
        )(gram, fields, images)
        return solved, norms.reshape(F)

    return jax.shard_map(
        body,
        mesh=mesh,
        in_specs=(P(None, "gx", "gy", "gz"), P("gx", "gy", "gz")),
        out_specs=(P(None, "gx", "gy", "gz"), P()),
        check_vma=False,
    )
```

```python
import functools

import jax
import jax.numpy as jnp
from jax import lax
from jax.experimental import pallas as pl
from jax.experimental.pallas import tpu as pltpu
from jax.sharding import PartitionSpec as P

MESH = pl.DeviceIdType.MESH
F, NX, NY, NZ = 8, 8, 32, 128
TOP = 8
ROWS = slice(TOP, TOP + NY)
GROUPS = 4
WIDE = F // GROUPS
INNER, FACE = 12, 4
TILE = (8, 128)


def exchange_kernel(gx, gy, gz, b_hbm, s_hbm, gram_ref, buf_p, buf_q,
                    buf_r, diag, y_halo, inner_s, inner_r, face_s, face_r, part_e, part_l, part_p,
                    load_sem, xs_sem, xr_sem, ys_sem, yr_sem, zs_sem, zr_sem, g_send, g_recv, heard):
    ix, iy, iz = lax.axis_index("gx"), lax.axis_index("gy"), lax.axis_index("gz")

    loads = [
        pltpu.make_async_copy(b_hbm.at[:, 0], buf_p.at[:, 1, ROWS], load_sem.at[0]),
        pltpu.make_async_copy(b_hbm.at[:, NX - 1], buf_p.at[:, NX, ROWS], load_sem.at[1]),
        pltpu.make_async_copy(b_hbm.at[:, 1:NX - 1], buf_p.at[:, 2:NX, ROWS], load_sem.at[2]),
        pltpu.make_async_copy(s_hbm, diag, load_sem.at[3]),
    ]
    for load in loads:
        load.start()

    chips_y = gy // 2
    core = lax.rem(iy, 2)
    row = iy - core
    xs = [ix] + [lax.rem(ix + k, gx) for k in range(1, gx)]
    ys = [iy] + [lax.rem(iy + 2 * k, gy) for k in range(1, chips_y)]
    zs = [iz] + [lax.rem(iz + k, gz) for k in range(1, gz)]
    across = row + 1 - core
    beyond = lax.rem(iy + gy - 1 + 2 * core, gy)
    line = [(ix, y, zs[k]) for k in dict.fromkeys((1, gz - 1) + tuple(range(2, gz - 1))) for y in (iy, across)]
    line = [(ix, across, iz)] + line
    plane = [(xs[a], ys[b], iz) for a in range(gx) for b in range(chips_y) if a or b]
    step_y = [ys[k] for k in dict.fromkeys((1, chips_y - 1)) if k % chips_y]
    near = [(xs[k], iy, iz) for k in dict.fromkeys((1, gx - 1))] + [(ix, beyond, iz), (ix, across, iz)]
    near += [(ix, iy, zs[k]) for k in dict.fromkeys((1, gz - 1))] + [(ix, y, iz) for y in step_y]
    second = [(xs[2 % gx], iy, iz), (ix, ys[2 % chips_y], iz)] if gx > 2 and chips_y > 2 else []
    second += [(ix, iy, zs[k]) for k in dict.fromkeys((2, gz - 2))] if gz > 3 else []

    barrier = pltpu.get_barrier_semaphore()
    for device in near:
        pl.semaphore_signal(barrier, inc=1, device_id=device, device_id_type=MESH)

    def tell(stage, devices):
        for device in devices:
            pl.semaphore_signal(heard.at[stage], inc=1, device_id=device, device_id_type=MESH)

    zero_x = jnp.zeros((F, NY, NZ), jnp.float32)
    zero_y = jnp.zeros((F, NX, 1, NZ), jnp.float32)
    for turn, buf in enumerate((buf_p, buf_q)):
        buf[:, 1:NX + 1, TOP - 1:TOP] = zero_y
        buf[:, 1:NX + 1, TOP + NY:TOP + NY + 1] = zero_y
        for way in range(2):
            @pl.when(ix == way * (gx - 1))
            def _():
                buf[:, way * (NX + 1), ROWS] = zero_x

            @pl.when(iy == way * (gy - 1))
            def _():
                y_halo[turn, way] = zero_y

            @pl.when(iz == way * (gz - 1))
            def _():
                inner_r[turn, way] = jnp.zeros((INNER, NZ), jnp.float32)
                face_r[turn, way] = jnp.zeros((FACE, NZ), jnp.float32)

    bufs, both = (buf_p, buf_q), range(2)
    has = {
        "x": (ix > 0, ix < gx - 1),
        "y": (iy > 0, iy < gy - 1),
        "z": (iz > 0, iz < gz - 1),
    }

    def x_copy(turn, way, group):
        fields = slice(group * WIDE, (group + 1) * WIDE)
        buf = bufs[turn]
        return pltpu.make_async_remote_copy(
            src_ref=buf.at[fields, NX if way else 1, ROWS],
            dst_ref=buf.at[fields, 0 if way else NX + 1, ROWS],
            send_sem=xs_sem.at[turn, way, group],
            recv_sem=xr_sem.at[turn, way, group],
            device_id=(ix + 1 if way else ix - 1, iy, iz),
            device_id_type=MESH,
        )

    spans = ((2, NX), (1, 2), (NX, NX + 1))

    def y_copy(turn, way, part):
        buf, (low, high) = bufs[turn], spans[part]
        edge = TOP + NY - 1 if way else TOP
        return pltpu.make_async_remote_copy(
            src_ref=buf.at[:, low:high, edge:edge + 1],
            dst_ref=y_halo.at[turn, 1 - way, :, low - 1:high - 1],
            send_sem=ys_sem.at[turn, way, part],
            recv_sem=yr_sem.at[turn, way, part],
            device_id=(ix, iy + 1 if way else iy - 1, iz),
            device_id_type=MESH,
        )

    def z_copy(turn, way, part):
        source, target = ((inner_s, inner_r), (face_s, face_r))[part]
        return pltpu.make_async_remote_copy(
            src_ref=source.at[turn, way],
            dst_ref=target.at[turn, 0 if way else 1],
            send_sem=zs_sem.at[turn, way, part],
            recv_sem=zr_sem.at[turn, way, part],
            device_id=(ix, iy, iz + 1 if way else iz - 1),
            device_id_type=MESH,
        )

    def start(axis, way, copies):
        @pl.when(has[axis][way])
        def _():
            for copy in copies:
                copy.start()

    def arrive(axis, way, copies):
        @pl.when(has[axis][1 - way])
        def _():
            for copy in copies:
                copy.wait_recv()

    def sent(axis, way, copies):
        @pl.when(has[axis][way])
        def _():
            for copy in copies:
                copy.wait_send()

    tiles = ([], [])
    for f in range(0, F, 2):
        tiles[0].append([(f, 2, 6)])
        tiles[0].append([(f, 6, 8), (f + 1, 2, 4)])
        tiles[0].append([(f + 1, 4, 8)])
        tiles[1].append([(f, 1, 2), (f, 8, 9), (f + 1, 1, 2), (f + 1, 8, 9)])

    def pack_z(turn, part):
        buf, target = bufs[turn], (inner_s, face_s)[part]
        for t, pieces in enumerate(tiles[part]):
            tile = jnp.concatenate([buf[f, a:b, ROWS] for f, a, b in pieces], axis=0)
            tile = tile.reshape(NZ, NZ).T
            target[turn, 0, t:t + 1] = tile[0:1]
            target[turn, 1, t:t + 1] = tile[NZ - 1:NZ]

    lane = lax.broadcasted_iota(jnp.int32, (NY, NZ), 1)
    first, last = lane == 0, lane == NZ - 1
    edges = jnp.logical_or(first, last)

    def apply(src, dst, f, x):
        c = src[f, x, ROWS]
        beside = src[f, x, TOP + 1:TOP + NY + 1] + src[f, x, TOP - 1:TOP + NY - 1]
        for other in (x - 1, x + 1):
            if 1 <= other <= NX:
                beside = beside + src[f, other, ROWS]
        beside = beside + jnp.where(last, 0.0, pltpu.roll(c, NZ - 1, 1))
        beside = beside + jnp.where(first, 0.0, pltpu.roll(c, 1, 1))
        dst[f, x, ROWS] = diag[x - 1] * c - beside

    def inside(src, dst):
        def step(f, _):
            for x in range(1, NX + 1):
                apply(src, dst, f, x)
            return 0

        lax.fori_loop(0, F, step, 0)

    def take_x(src, dst, turn, group):
        for way in both:
            arrive("x", way, [x_copy(turn, way, group)])
        for f in range(group * WIDE, (group + 1) * WIDE):
            dst[f, 1, ROWS] -= src[f, 0, ROWS]
            dst[f, NX, ROWS] -= src[f, NX + 1, ROWS]

    def take_y(dst, turn, parts):
        for way in both:
            arrive("y", way, [y_copy(turn, way, part) for part in parts])
        for part in parts:
            low, high = spans[part]
            for way, edge in enumerate((TOP, TOP + NY - 1)):
                dst[:, low:high, edge:edge + 1] -= y_halo[turn, way, :, low - 1:high - 1]

    def take_z(dst, turn, part):
        for way in both:
            arrive("z", way, [z_copy(turn, way, part)])
        source = (inner_r, face_r)[part]
        for t, pieces in enumerate(tiles[part]):
            low = jnp.broadcast_to(source[turn, 0, t:t + 1], (NZ // 2, NZ))
            high = jnp.broadcast_to(source[turn, 1, t:t + 1], (NZ // 2, NZ))
            tile = jnp.concatenate([low, high], axis=0).T.reshape(4, NY, NZ)
            at = 0
            for f, a, b in pieces:
                dst[f, a:b, ROWS] -= jnp.where(edges, tile[at:at + b - a], 0.0)
                at += b - a

    def moment(left, right, low, high, sums):
        def step(x, sums):
            for t in range(NY // 8):
                rows = slice(TOP + 8 * t, TOP + 8 * t + 8)
                u = left[:, x, rows]
                v = u if right is left else right[:, x, rows]
                sums = tuple(sums[i] + u[i:i + 1] * v[i:] for i in range(F))
            return sums

        return lax.fori_loop(low, high, step, sums)

    def faces(left, right, sums):
        def step(k, sums):
            x = 1 + (NX - 1) * k
            for t in range(NY // 8):
                rows = slice(TOP + 8 * t, TOP + 8 * t + 8)
                u = left[:, x, rows]
                v = u if right is left else right[:, x, rows]
                sums = tuple(sums[i] + u[i:i + 1] * v[i:] for i in range(F))
            return sums

        return lax.fori_loop(0, 2, step, sums)

    none = tuple(jnp.zeros((F - i,) + TILE, jnp.float32) for i in range(F))

    sub = lax.broadcasted_iota(jnp.int32, TILE, 0)
    cell = lax.broadcasted_iota(jnp.int32, TILE, 1)

    def fold(parts):
        width = 1
        while len(parts) > 1:
            odd = (sub & width) != 0
            merged = []
            for i in range(0, len(parts), 2):
                a, b = parts[i], parts[i + 1]
                kept = jnp.where(odd, b, a)
                moved = jnp.where(odd, a, b)
                moved = jnp.where(odd, pltpu.roll(moved, width, 0), pltpu.roll(moved, 8 - width, 0))
                merged.append(kept + moved)
            parts = merged
            width *= 2
        return parts[0]

    place = lax.rem(cell, 2 * F)
    own = sub == lax.rem(F - lax.div(cell, 2 * F), F)

    def gather(k, sums, total):
        for c in range(F):
            line = fold([sums[min(i, c)][max(i, c) - min(i, c)] for i in range(F)])
            total = jnp.where(place == k * F + c, jnp.sum(line, axis=1, keepdims=True), total)
        return total

    def as_row(total):
        return jnp.sum(jnp.where(own, total, 0.0), axis=0, keepdims=True)

    def copy_part(stage, src, dst, device):
        return pltpu.make_async_remote_copy(
            src_ref=src, dst_ref=dst,
            send_sem=g_send.at[stage], recv_sem=g_recv.at[stage],
            device_id=device, device_id_type=MESH)

    def spread(stage, parts, mine, devices, rows):
        for k, value in enumerate(rows):
            parts[mine, k:k + 1] = value
        for device in devices:
            copy_part(stage, parts.at[mine], parts.at[mine], device).start()
        count = len(devices)
        return copy_part(stage, parts.at[0:count], parts.at[0:count], devices[0])

    def added(parts, count):
        sums = [parts[k] for k in range(count)]
        while len(sums) > 1:
            sums = [sums[k] + sums[k + 1] for k in range(0, len(sums), 2)]
        return sums[0]

    loads[0].wait()
    loads[1].wait()
    pl.semaphore_wait(barrier, len(near))
    for way in both:
        start("x", way, [x_copy(0, way, group) for group in range(GROUPS)])
    tell(0, near)
    loads[2].wait()
    for way in both:
        start("y", way, [y_copy(0, way, part) for part in range(3)])
    for part in both:
        pack_z(0, part)
    for way in both:
        start("z", way, [z_copy(0, way, part) for part in both])
    loads[3].wait()
    diag[...] = 6.0 + diag[...]
    inside(buf_p, buf_q)
    zeroth = moment(buf_p, buf_p, 1, NX + 1, none)
    blank = jnp.zeros(TILE, jnp.float32)
    row_zero = as_row(gather(0, zeroth, blank))
    pl.semaphore_wait(heard.at[0], len(near))
    tell(1, second)
    take_y(buf_q, 0, range(3))
    for part in both:
        take_z(buf_q, 0, part)

    def forward(group):
        take_x(buf_p, buf_q, 0, group)
        for way in both:
            start("x", way, [x_copy(1, way, group)])

    forward(0)
    for way in both:
        start("y", way, [y_copy(1, way, 0)])
    pack_z(1, 0)
    for way in both:
        start("z", way, [z_copy(1, way, 0)])
    forward(1)
    first_sums = moment(buf_p, buf_q, 2, NX, none)
    forward(2)
    second_sums = moment(buf_q, buf_q, 2, NX, none)
    for group in range(3, GROUPS):
        forward(group)
    for way in both:
        start("y", way, [y_copy(1, way, part) for part in (1, 2)])
    pack_z(1, 1)
    for way in both:
        start("z", way, [z_copy(1, way, 1)])

    if second:
        pl.semaphore_wait(heard.at[1], len(second))
    tell(2, [(ix, across, iz)])

    inside(buf_q, buf_r)
    total = gather(0, faces(buf_p, buf_q, first_sums), blank)
    total = gather(1, faces(buf_q, buf_q, second_sums), total)
    row_one = as_row(total)
    pl.semaphore_wait(heard.at[2], 1)
    in_line = 2 * iz + core
    early_done = spread(0, part_e, in_line, line, (row_zero, row_one))
    take_y(buf_r, 1, (0,))
    take_z(buf_r, 1, 0)
    third = moment(buf_q, buf_r, 2, NX, none)
    fourth = moment(buf_r, buf_r, 2, NX, none)
    take_y(buf_r, 1, (1, 2))
    take_z(buf_r, 1, 1)
    for group in range(GROUPS):
        take_x(buf_q, buf_r, 1, group)
    third = faces(buf_q, buf_r, third)
    fourth = faces(buf_r, buf_r, fourth)
    row_two = as_row(gather(1, fourth, gather(0, third, blank)))

    late_done = spread(1, part_l, in_line, line, (row_two,))
    early_done.wait_recv()
    early = added(part_e, len(line) + 1)
    late_done.wait_recv()
    late = added(part_l, len(line) + 1)
    chip = ix * chips_y + lax.div(row, 2)
    planes_done = spread(2, part_p, chip, plane, (early[0:1], early[1:2], late))
    planes_done.wait_recv()
    gram_ref[...] = added(part_p, len(plane) + 1)

    early_done.wait_send()
    late_done.wait_send()
    planes_done.wait_send()
    for turn in both:
        for way in both:
            sent("x", way, [x_copy(turn, way, group) for group in range(GROUPS)])
            sent("y", way, [y_copy(turn, way, part) for part in range(3)])
            sent("z", way, [z_copy(turn, way, part) for part in both])


def combine_kernel(gram_ref, buf_b, buf_a, x_hbm, norm_ref, buf_x, coeff, out_sem):
    turned = [
        pltpu.roll(jnp.broadcast_to(gram_ref[k:k + 1], TILE), 0, 1, stride=2 * F, stride_axis=0) for k in range(3)
    ]
    sub = lax.broadcasted_iota(jnp.int32, TILE, 0)
    cell = lax.broadcasted_iota(jnp.int32, TILE, 1)

    def column(order, c):
        k, half = ((0, 0), (1, 0), (1, 1), (2, 0), (2, 1))[order]
        at = half * F + c
        return jnp.broadcast_to(turned[k][:, at:at + 1], TILE)

    def spread(value, row):
        return jnp.broadcast_to(value[row:row + 1], TILE)

    moments = [[column(order, c) for c in range(F)] for order in range(5)]
    columns = [[moments[2][c], moments[3][c]] for c in range(F)]
    columns += [[moments[3][c], moments[4][c]] for c in range(F)]
    rights = [[moments[1][c], moments[2][c]] for c in range(F)]
    for k in range(2 * F):
        half, row = k // F, k % F
        pivot = columns[k]
        inverse = 1.0 / spread(pivot[half], row)
        mine = sub == row
        for other in columns[k + 1:] + rights:
            r = spread(other[half], row) * inverse
            for h in range(2):
                value = other[h] - pivot[h] * r
                other[h] = jnp.where(mine, r, value) if h == half else value
    norms = jnp.zeros((1, 128), jnp.float32)
    for c in range(F):
        for h in range(2):
            coeff[c, h] = rights[c][h]
        fit = moments[1][c] * rights[c][0] + moments[2][c] * rights[c][1]
        left = jnp.where(sub == c, moments[0][c], 0.0) - fit
        norms = jnp.where(cell[0:1] == c, jnp.sum(left, axis=0, keepdims=True), norms)
    norm_ref[...] = jnp.sqrt(jnp.maximum(norms, 0.0))[:, :F]

    pair = 2
    outs = []
    for c0 in range(0, F, pair):
        weights = [[[spread(coeff[c, h], i) for i in range(F)] for h in range(2)] for c in range(c0, c0 + pair)]

        def step(x, _):
            for t in range(NY // 8):
                rows = slice(8 * t, 8 * t + 8)
                held = slice(TOP + 8 * t, TOP + 8 * t + 8)
                fields = [buf_b[:, x + 1, held], buf_a[:, x + 1, held]]
                for c in range(pair):
                    sums = [None, None]
                    for h in range(2):
                        for i in range(F):
                            term = weights[c][h][i] * fields[h][i]
                            sums[h] = term if sums[h] is None else sums[h] + term
                    buf_x[c0 + c, x, rows] = sums[0] + sums[1]
            return 0

        lax.fori_loop(0, NX, step, 0)
        out = pltpu.make_async_copy(buf_x.at[c0:c0 + pair], x_hbm.at[c0:c0 + pair], out_sem.at[c0 // pair])
        out.start()
        outs.append(out)
    for out in outs:
        out.wait()


def solution(mesh):
    gx, gy, gz = mesh.shape["gx"], mesh.shape["gy"], mesh.shape["gz"]
    f32 = jnp.float32
    dma = pltpu.SemaphoreType.DMA
    hbm = pl.BlockSpec(memory_space=pltpu.HBM)
    vmem = pl.BlockSpec(memory_space=pltpu.VMEM)
    block = (F, NX, NY, NZ)
    padded = (F, NX + 2, NY + 16, NZ)

    def body(right_side, shift):
        gram, fields, images = pl.pallas_call(
            functools.partial(exchange_kernel, gx, gy, gz),
            out_shape=(
                jax.ShapeDtypeStruct((3, NZ), f32),
                jax.ShapeDtypeStruct(padded, f32),
                jax.ShapeDtypeStruct(padded, f32),
            ),
            in_specs=[hbm, hbm],
            out_specs=(vmem, vmem, vmem),
            scratch_shapes=[
                pltpu.VMEM(padded, f32),
                pltpu.VMEM((NX, NY, NZ), f32),
                pltpu.VMEM((2, 2, F, NX, 1, NZ), f32),
                pltpu.VMEM((2, 2, INNER, NZ), f32),
                pltpu.VMEM((2, 2, INNER, NZ), f32),
                pltpu.VMEM((2, 2, FACE, NZ), f32),
                pltpu.VMEM((2, 2, FACE, NZ), f32),
                pltpu.VMEM((2 * gz, 2, NZ), f32),
                pltpu.VMEM((2 * gz, 1, NZ), f32),
                pltpu.VMEM((gx * gy // 2, 3, NZ), f32),
                dma((4,)),
                dma((2, 2, GROUPS)),
                dma((2, 2, GROUPS)),
                dma((2, 2, 3)),
                dma((2, 2, 3)),
                dma((2, 2, 2)),
                dma((2, 2, 2)),
                dma((3,)),
                dma((3,)),
                pltpu.SemaphoreType.REGULAR((3,)),
            ],
            compiler_params=pltpu.CompilerParams(
                collective_id=0, has_side_effects=True, vmem_limit_bytes=24 << 20
            ),
        )(*(pltpu.with_memory_space_constraint(a, pltpu.HBM) for a in (right_side, shift)))
        solved, norms = pl.pallas_call(
            combine_kernel,
            out_shape=(jax.ShapeDtypeStruct(block, f32), jax.ShapeDtypeStruct((1, F), f32)),
            in_specs=[vmem, vmem, vmem],
            out_specs=(hbm, vmem),
            scratch_shapes=[
                pltpu.VMEM(block, f32),
                pltpu.VMEM((F, 2) + TILE, f32),
                dma((F // 2,)),
            ],
            compiler_params=pltpu.CompilerParams(vmem_limit_bytes=16 << 20),
        )(gram, fields, images)
        return solved, norms.reshape(F)

    return jax.shard_map(
        body,
        mesh=mesh,
        in_specs=(P(None, "gx", "gy", "gz"), P("gx", "gy", "gz")),
        out_specs=(P(None, "gx", "gy", "gz"), P()),
        check_vma=False,
    )
```

```python
import functools

import jax
import jax.numpy as jnp
from jax import lax
from jax.experimental import pallas as pl
from jax.experimental.pallas import tpu as pltpu
from jax.sharding import PartitionSpec as P

MESH = pl.DeviceIdType.MESH
F, NX, NY, NZ = 8, 8, 32, 128
TOP = 8
ROWS = slice(TOP, TOP + NY)
GROUPS = 4
WIDE = F // GROUPS
INNER, FACE = 12, 4
TILE = (8, 128)


def exchange_kernel(gx, gy, gz, b_hbm, s_hbm, gram_ref, buf_p, buf_q,
                    buf_r, diag, y_halo, inner_s, inner_r, face_s, face_r, part_e, part_l, part_p,
                    load_sem, xs_sem, xr_sem, ys_sem, yr_sem, zs_sem, zr_sem, g_send, g_recv, heard):
    ix, iy, iz = lax.axis_index("gx"), lax.axis_index("gy"), lax.axis_index("gz")

    loads = [
        pltpu.make_async_copy(b_hbm.at[:, 0], buf_p.at[:, 1, ROWS], load_sem.at[0]),
        pltpu.make_async_copy(b_hbm.at[:, NX - 1], buf_p.at[:, NX, ROWS], load_sem.at[1]),
        pltpu.make_async_copy(b_hbm.at[:, 1:NX - 1], buf_p.at[:, 2:NX, ROWS], load_sem.at[2]),
        pltpu.make_async_copy(s_hbm, diag, load_sem.at[3]),
    ]
    for load in loads:
        load.start()

    chips_y = gy // 2
    core = lax.rem(iy, 2)
    row = iy - core
    xs = [ix] + [lax.rem(ix + k, gx) for k in range(1, gx)]
    ys = [iy] + [lax.rem(iy + 2 * k, gy) for k in range(1, chips_y)]
    zs = [iz] + [lax.rem(iz + k, gz) for k in range(1, gz)]
    across = row + 1 - core
    beyond = lax.rem(iy + gy - 1 + 2 * core, gy)
    def hops(k, n):
        return min(k, n - k)

    line = [(ix, y, zs[k]) for k in sorted(range(1, gz), key=lambda k: -hops(k, gz)) for y in (across, iy)]
    line += [(ix, across, iz)]
    steps = sorted(((a, b) for a in range(gx) for b in range(chips_y)), key=lambda p: -hops(p[0], gx) - hops(p[1], chips_y))
    plane = [(xs[a], ys[b], iz) for a, b in steps if a or b]
    step_y = [ys[k] for k in dict.fromkeys((1, chips_y - 1)) if k % chips_y]
    near = [(xs[k], iy, iz) for k in dict.fromkeys((1, gx - 1))] + [(ix, beyond, iz), (ix, across, iz)]
    near += [(ix, iy, zs[k]) for k in dict.fromkeys((1, gz - 1))] + [(ix, y, iz) for y in step_y]
    second = [(xs[2 % gx], iy, iz), (ix, ys[2 % chips_y], iz)] if gx > 2 and chips_y > 2 else []
    second += [(ix, iy, zs[k]) for k in dict.fromkeys((2, gz - 2))] if gz > 3 else []

    barrier = pltpu.get_barrier_semaphore()
    for device in near:
        pl.semaphore_signal(barrier, inc=1, device_id=device, device_id_type=MESH)

    def tell(stage, devices):
        for device in devices:
            pl.semaphore_signal(heard.at[stage], inc=1, device_id=device, device_id_type=MESH)

    zero_x = jnp.zeros((F, NY, NZ), jnp.float32)
    zero_y = jnp.zeros((F, NX, 1, NZ), jnp.float32)
    for turn, buf in enumerate((buf_p, buf_q)):
        buf[:, 1:NX + 1, TOP - 1:TOP] = zero_y
        buf[:, 1:NX + 1, TOP + NY:TOP + NY + 1] = zero_y
        for way in range(2):
            @pl.when(ix == way * (gx - 1))
            def _():
                buf[:, way * (NX + 1), ROWS] = zero_x

            @pl.when(iy == way * (gy - 1))
            def _():
                y_halo[turn, way] = zero_y

            @pl.when(iz == way * (gz - 1))
            def _():
                inner_r[turn, way] = jnp.zeros((INNER, NZ), jnp.float32)
                face_r[turn, way] = jnp.zeros((FACE, NZ), jnp.float32)

    bufs, both = (buf_p, buf_q), range(2)
    has = {
        "x": (ix > 0, ix < gx - 1),
        "y": (iy > 0, iy < gy - 1),
        "z": (iz > 0, iz < gz - 1),
    }

    def x_copy(turn, way, group):
        fields = slice(group * WIDE, (group + 1) * WIDE)
        buf = bufs[turn]
        return pltpu.make_async_remote_copy(
            src_ref=buf.at[fields, NX if way else 1, ROWS],
            dst_ref=buf.at[fields, 0 if way else NX + 1, ROWS],
            send_sem=xs_sem.at[turn, way, group],
            recv_sem=xr_sem.at[turn, way, group],
            device_id=(ix + 1 if way else ix - 1, iy, iz),
            device_id_type=MESH,
        )

    spans = ((2, NX), (1, 2), (NX, NX + 1))

    def y_copy(turn, way, part):
        buf, (low, high) = bufs[turn], spans[part]
        edge = TOP + NY - 1 if way else TOP
        return pltpu.make_async_remote_copy(
            src_ref=buf.at[:, low:high, edge:edge + 1],
            dst_ref=y_halo.at[turn, 1 - way, :, low - 1:high - 1],
            send_sem=ys_sem.at[turn, way, part],
            recv_sem=yr_sem.at[turn, way, part],
            device_id=(ix, iy + 1 if way else iy - 1, iz),
            device_id_type=MESH,
        )

    def z_copy(turn, way, part):
        source, target = ((inner_s, inner_r), (face_s, face_r))[part]
        return pltpu.make_async_remote_copy(
            src_ref=source.at[turn, way],
            dst_ref=target.at[turn, 0 if way else 1],
            send_sem=zs_sem.at[turn, way, part],
            recv_sem=zr_sem.at[turn, way, part],
            device_id=(ix, iy, iz + 1 if way else iz - 1),
            device_id_type=MESH,
        )

    def start(axis, way, copies):
        @pl.when(has[axis][way])
        def _():
            for copy in copies:
                copy.start()

    def arrive(axis, way, copies):
        @pl.when(has[axis][1 - way])
        def _():
            for copy in copies:
                copy.wait_recv()

    def sent(axis, way, copies):
        @pl.when(has[axis][way])
        def _():
            for copy in copies:
                copy.wait_send()

    tiles = ([], [])
    for f in range(0, F, 2):
        tiles[0].append([(f, 2, 6)])
        tiles[0].append([(f, 6, 8), (f + 1, 2, 4)])
        tiles[0].append([(f + 1, 4, 8)])
        tiles[1].append([(f, 1, 2), (f, 8, 9), (f + 1, 1, 2), (f + 1, 8, 9)])

    def pack_z(turn, part):
        buf, target = bufs[turn], (inner_s, face_s)[part]
        for t, pieces in enumerate(tiles[part]):
            tile = jnp.concatenate([buf[f, a:b, ROWS] for f, a, b in pieces], axis=0)
            tile = tile.reshape(NZ, NZ).T
            target[turn, 0, t:t + 1] = tile[0:1]
            target[turn, 1, t:t + 1] = tile[NZ - 1:NZ]

    lane = lax.broadcasted_iota(jnp.int32, (NY, NZ), 1)
    first, last = lane == 0, lane == NZ - 1
    edges = jnp.logical_or(first, last)

    def dots(left, right, x, sums):
        for t in range(NY // 8):
            rows = slice(TOP + 8 * t, TOP + 8 * t + 8)
            u = left[:, x, rows]
            v = u if right is left else right[:, x, rows]
            sums = tuple(sums[i] + u[i:i + 1] * v[i:] for i in range(F))
        return sums

    def inside(src, dst, left, right, sums):
        def step(x, sums):
            for f in range(F):
                c = src[f, x, ROWS]
                beside = src[f, x, TOP + 1:TOP + NY + 1] + src[f, x, TOP - 1:TOP + NY - 1]
                for other in (x - 1, x + 1):
                    if not isinstance(x, int) or 1 <= other <= NX:
                        beside = beside + src[f, other, ROWS]
                beside = beside + jnp.where(last, 0.0, pltpu.roll(c, NZ - 1, 1))
                beside = beside + jnp.where(first, 0.0, pltpu.roll(c, 1, 1))
                dst[f, x, ROWS] = diag[x - 1] * c - beside
            return dots(left, right, x, sums)

        sums = lax.fori_loop(2, NX, step, step(1, sums))
        return step(NX, sums)

    def take_x(src, dst, turn, group):
        for way in both:
            arrive("x", way, [x_copy(turn, way, group)])
        for f in range(group * WIDE, (group + 1) * WIDE):
            dst[f, 1, ROWS] -= src[f, 0, ROWS]
            dst[f, NX, ROWS] -= src[f, NX + 1, ROWS]

    def take_y(dst, turn, parts):
        for way in both:
            arrive("y", way, [y_copy(turn, way, part) for part in parts])
        for part in parts:
            low, high = spans[part]
            for way, edge in enumerate((TOP, TOP + NY - 1)):
                dst[:, low:high, edge:edge + 1] -= y_halo[turn, way, :, low - 1:high - 1]

    def take_z(dst, turn, part):
        for way in both:
            arrive("z", way, [z_copy(turn, way, part)])
        source = (inner_r, face_r)[part]
        for t, pieces in enumerate(tiles[part]):
            low = jnp.broadcast_to(source[turn, 0, t:t + 1], (NZ // 2, NZ))
            high = jnp.broadcast_to(source[turn, 1, t:t + 1], (NZ // 2, NZ))
            tile = jnp.concatenate([low, high], axis=0).T.reshape(4, NY, NZ)
            at = 0
            for f, a, b in pieces:
                dst[f, a:b, ROWS] -= jnp.where(edges, tile[at:at + b - a], 0.0)
                at += b - a

    def moment(left, right, low, high, sums):
        return lax.fori_loop(low, high, lambda x, sums: dots(left, right, x, sums), sums)

    def faces(left, right, sums):
        return lax.fori_loop(0, 2, lambda k, sums: dots(left, right, 1 + (NX - 1) * k, sums), sums)

    none = tuple(jnp.zeros((F - i,) + TILE, jnp.float32) for i in range(F))

    sub = lax.broadcasted_iota(jnp.int32, TILE, 0)
    cell = lax.broadcasted_iota(jnp.int32, TILE, 1)

    def fold(parts):
        width = 1
        while len(parts) > 1:
            odd = (sub & width) != 0
            merged = []
            for i in range(0, len(parts), 2):
                a, b = parts[i], parts[i + 1]
                kept = jnp.where(odd, b, a)
                moved = jnp.where(odd, a, b)
                moved = jnp.where(odd, pltpu.roll(moved, width, 0), pltpu.roll(moved, 8 - width, 0))
                merged.append(kept + moved)
            parts = merged
            width *= 2
        return parts[0]

    place = lax.rem(cell, 2 * F)
    own = sub == lax.rem(F - lax.div(cell, 2 * F), F)

    def gather(k, sums, total):
        for c in range(F):
            line = fold([sums[min(i, c)][max(i, c) - min(i, c)] for i in range(F)])
            total = jnp.where(place == k * F + c, jnp.sum(line, axis=1, keepdims=True), total)
        return total

    def as_row(total):
        return jnp.sum(jnp.where(own, total, 0.0), axis=0, keepdims=True)

    def copy_part(stage, src, dst, device):
        return pltpu.make_async_remote_copy(
            src_ref=src, dst_ref=dst,
            send_sem=g_send.at[stage], recv_sem=g_recv.at[stage],
            device_id=device, device_id_type=MESH)

    def spread(stage, parts, mine, devices, rows):
        for k, value in enumerate(rows):
            parts[mine, k:k + 1] = value
        for device in devices:
            copy_part(stage, parts.at[mine], parts.at[mine], device).start()
        count = len(devices)
        return copy_part(stage, parts.at[0:count], parts.at[0:count], devices[0])

    def added(parts, count):
        sums = [parts[k] for k in range(count)]
        while len(sums) > 1:
            sums = [sums[k] + sums[k + 1] for k in range(0, len(sums), 2)]
        return sums[0]

    loads[0].wait()
    loads[1].wait()
    pl.semaphore_wait(barrier, len(near))
    for way in both:
        start("x", way, [x_copy(0, way, group) for group in range(GROUPS)])
    tell(0, near)
    loads[2].wait()
    for way in both:
        start("y", way, [y_copy(0, way, part) for part in range(3)])
    for part in both:
        pack_z(0, part)
    for way in both:
        start("z", way, [z_copy(0, way, part) for part in both])
    loads[3].wait()
    diag[...] = 6.0 + diag[...]
    zeroth = inside(buf_p, buf_q, buf_p, buf_p, none)
    blank = jnp.zeros(TILE, jnp.float32)
    row_zero = as_row(gather(0, zeroth, blank))
    pl.semaphore_wait(heard.at[0], len(near))
    tell(1, second)
    take_y(buf_q, 0, range(3))
    for part in both:
        take_z(buf_q, 0, part)

    def forward(group):
        take_x(buf_p, buf_q, 0, group)
        for way in both:
            start("x", way, [x_copy(1, way, group)])

    forward(0)
    for way in both:
        start("y", way, [y_copy(1, way, 0)])
    pack_z(1, 0)
    for way in both:
        start("z", way, [z_copy(1, way, 0)])
    forward(1)
    second_sums = moment(buf_q, buf_q, 2, NX, none)
    forward(2)
    for group in range(3, GROUPS):
        forward(group)
    for way in both:
        start("y", way, [y_copy(1, way, part) for part in (1, 2)])
    pack_z(1, 1)
    for way in both:
        start("z", way, [z_copy(1, way, 1)])

    if second:
        pl.semaphore_wait(heard.at[1], len(second))
    tell(2, [(ix, across, iz)])

    total = gather(0, inside(buf_q, buf_r, buf_p, buf_q, none), blank)
    total = gather(1, faces(buf_q, buf_q, second_sums), total)
    row_one = as_row(total)
    pl.semaphore_wait(heard.at[2], 1)
    in_line = 2 * iz + core
    early_done = spread(0, part_e, in_line, line, (row_zero, row_one))
    take_y(buf_r, 1, (0,))
    take_z(buf_r, 1, 0)
    third = moment(buf_q, buf_r, 2, NX, none)
    fourth = moment(buf_r, buf_r, 2, NX, none)
    take_y(buf_r, 1, (1, 2))
    take_z(buf_r, 1, 1)
    for group in range(GROUPS):
        take_x(buf_q, buf_r, 1, group)
    third = faces(buf_q, buf_r, third)
    fourth = faces(buf_r, buf_r, fourth)
    row_two = as_row(gather(1, fourth, gather(0, third, blank)))

    late_done = spread(1, part_l, in_line, line, (row_two,))
    early_done.wait_recv()
    early = added(part_e, len(line) + 1)
    late_done.wait_recv()
    late = added(part_l, len(line) + 1)
    chip = ix * chips_y + lax.div(row, 2)
    planes_done = spread(2, part_p, chip, plane, (early[0:1], early[1:2], late))
    planes_done.wait_recv()
    gram_ref[...] = added(part_p, len(plane) + 1)

    early_done.wait_send()
    late_done.wait_send()
    planes_done.wait_send()
    for turn in both:
        for way in both:
            sent("x", way, [x_copy(turn, way, group) for group in range(GROUPS)])
            sent("y", way, [y_copy(turn, way, part) for part in range(3)])
            sent("z", way, [z_copy(turn, way, part) for part in both])


def combine_kernel(gram_ref, buf_b, buf_a, x_hbm, norm_ref, buf_x, coeff, out_sem):
    turned = [
        pltpu.roll(jnp.broadcast_to(gram_ref[k:k + 1], TILE), 0, 1, stride=2 * F, stride_axis=0) for k in range(3)
    ]
    sub = lax.broadcasted_iota(jnp.int32, TILE, 0)
    cell = lax.broadcasted_iota(jnp.int32, TILE, 1)

    def column(order, c):
        k, half = ((0, 0), (1, 0), (1, 1), (2, 0), (2, 1))[order]
        at = half * F + c
        return jnp.broadcast_to(turned[k][:, at:at + 1], TILE)

    def spread(value, row):
        return jnp.broadcast_to(value[row:row + 1], TILE)

    moments = [[column(order, c) for c in range(F)] for order in range(5)]
    columns = [[moments[2][c], moments[3][c]] for c in range(F)]
    columns += [[moments[3][c], moments[4][c]] for c in range(F)]
    rights = [[moments[1][c], moments[2][c]] for c in range(F)]
    for k in range(2 * F):
        half, row = k // F, k % F
        pivot = columns[k]
        inverse = 1.0 / spread(pivot[half], row)
        mine = sub == row
        for other in columns[k + 1:] + rights:
            r = spread(other[half], row) * inverse
            for h in range(2):
                value = other[h] - pivot[h] * r
                other[h] = jnp.where(mine, r, value) if h == half else value
    norms = jnp.zeros((1, 128), jnp.float32)
    for c in range(F):
        for h in range(2):
            coeff[c, h] = rights[c][h]
        fit = moments[1][c] * rights[c][0] + moments[2][c] * rights[c][1]
        left = jnp.where(sub == c, moments[0][c], 0.0) - fit
        norms = jnp.where(cell[0:1] == c, jnp.sum(left, axis=0, keepdims=True), norms)
    norm_ref[...] = jnp.sqrt(jnp.maximum(norms, 0.0))[:, :F]

    pair = 2
    outs = []
    for c0 in range(0, F, pair):
        weights = [[[spread(coeff[c, h], i) for i in range(F)] for h in range(2)] for c in range(c0, c0 + pair)]

        def step(x, _):
            for t in range(NY // 8):
                rows = slice(8 * t, 8 * t + 8)
                held = slice(TOP + 8 * t, TOP + 8 * t + 8)
                fields = [buf_b[:, x + 1, held], buf_a[:, x + 1, held]]
                for c in range(pair):
                    sums = [None, None]
                    for h in range(2):
                        for i in range(F):
                            term = weights[c][h][i] * fields[h][i]
                            sums[h] = term if sums[h] is None else sums[h] + term
                    buf_x[c0 + c, x, rows] = sums[0] + sums[1]
            return 0

        lax.fori_loop(0, NX, step, 0)
        out = pltpu.make_async_copy(buf_x.at[c0:c0 + pair], x_hbm.at[c0:c0 + pair], out_sem.at[c0 // pair])
        out.start()
        outs.append(out)
    for out in outs:
        out.wait()


def solution(mesh):
    gx, gy, gz = mesh.shape["gx"], mesh.shape["gy"], mesh.shape["gz"]
    f32 = jnp.float32
    dma = pltpu.SemaphoreType.DMA
    hbm = pl.BlockSpec(memory_space=pltpu.HBM)
    vmem = pl.BlockSpec(memory_space=pltpu.VMEM)
    block = (F, NX, NY, NZ)
    padded = (F, NX + 2, NY + 16, NZ)

    def body(right_side, shift):
        gram, fields, images = pl.pallas_call(
            functools.partial(exchange_kernel, gx, gy, gz),
            out_shape=(
                jax.ShapeDtypeStruct((3, NZ), f32),
                jax.ShapeDtypeStruct(padded, f32),
                jax.ShapeDtypeStruct(padded, f32),
            ),
            in_specs=[hbm, hbm],
            out_specs=(vmem, vmem, vmem),
            scratch_shapes=[
                pltpu.VMEM(padded, f32),
                pltpu.VMEM((NX, NY, NZ), f32),
                pltpu.VMEM((2, 2, F, NX, 1, NZ), f32),
                pltpu.VMEM((2, 2, INNER, NZ), f32),
                pltpu.VMEM((2, 2, INNER, NZ), f32),
                pltpu.VMEM((2, 2, FACE, NZ), f32),
                pltpu.VMEM((2, 2, FACE, NZ), f32),
                pltpu.VMEM((2 * gz, 2, NZ), f32),
                pltpu.VMEM((2 * gz, 1, NZ), f32),
                pltpu.VMEM((gx * gy // 2, 3, NZ), f32),
                dma((4,)),
                dma((2, 2, GROUPS)),
                dma((2, 2, GROUPS)),
                dma((2, 2, 3)),
                dma((2, 2, 3)),
                dma((2, 2, 2)),
                dma((2, 2, 2)),
                dma((3,)),
                dma((3,)),
                pltpu.SemaphoreType.REGULAR((3,)),
            ],
            compiler_params=pltpu.CompilerParams(
                collective_id=0, has_side_effects=True, vmem_limit_bytes=24 << 20
            ),
        )(*(pltpu.with_memory_space_constraint(a, pltpu.HBM) for a in (right_side, shift)))
        solved, norms = pl.pallas_call(
            combine_kernel,
            out_shape=(jax.ShapeDtypeStruct(block, f32), jax.ShapeDtypeStruct((1, F), f32)),
            in_specs=[vmem, vmem, vmem],
            out_specs=(hbm, vmem),
            scratch_shapes=[
                pltpu.VMEM(block, f32),
                pltpu.VMEM((F, 2) + TILE, f32),
                dma((F // 2,)),
            ],
            compiler_params=pltpu.CompilerParams(vmem_limit_bytes=16 << 20),
        )(gram, fields, images)
        return solved, norms.reshape(F)

    return jax.shard_map(
        body,
        mesh=mesh,
        in_specs=(P(None, "gx", "gy", "gz"), P("gx", "gy", "gz")),
        out_specs=(P(None, "gx", "gy", "gz"), P()),
        check_vma=False,
    )
```

```python
import functools

import jax
import jax.numpy as jnp
from jax import lax
from jax.experimental import pallas as pl
from jax.experimental.pallas import tpu as pltpu
from jax.sharding import PartitionSpec as P

MESH = pl.DeviceIdType.MESH
F, NX, NY, NZ = 8, 8, 32, 128
TOP = 8
ROWS = slice(TOP, TOP + NY)
GROUPS = 4
WIDE = F // GROUPS
INNER, FACE = 12, 4
TILE = (8, 128)


def exchange_kernel(gx, gy, gz, b_hbm, s_hbm, gram_ref, buf_p, buf_q,
                    buf_r, diag, y_halo, inner_s, inner_r, face_s, face_r, part_e, part_l, part_p,
                    load_sem, xs_sem, xr_sem, ys_sem, yr_sem, zs_sem, zr_sem, g_send, g_recv, heard):
    ix, iy, iz = lax.axis_index("gx"), lax.axis_index("gy"), lax.axis_index("gz")

    loads = [
        pltpu.make_async_copy(b_hbm.at[:, 0], buf_p.at[:, 1, ROWS], load_sem.at[0]),
        pltpu.make_async_copy(b_hbm.at[:, NX - 1], buf_p.at[:, NX, ROWS], load_sem.at[1]),
        pltpu.make_async_copy(b_hbm.at[:, 1:NX - 1], buf_p.at[:, 2:NX, ROWS], load_sem.at[2]),
        pltpu.make_async_copy(s_hbm, diag, load_sem.at[3]),
    ]
    for load in loads:
        load.start()

    chips_y = gy // 2
    core = lax.rem(iy, 2)
    row = iy - core
    xs = [ix] + [lax.rem(ix + k, gx) for k in range(1, gx)]
    ys = [iy] + [lax.rem(iy + 2 * k, gy) for k in range(1, chips_y)]
    zs = [iz] + [lax.rem(iz + k, gz) for k in range(1, gz)]
    across = row + 1 - core
    beyond = lax.rem(iy + gy - 1 + 2 * core, gy)
    def hops(k, n):
        return min(k, n - k)

    line = [(ix, y, zs[k]) for k in sorted(range(1, gz), key=lambda k: -hops(k, gz)) for y in (across, iy)]
    line += [(ix, across, iz)]
    steps = sorted(((a, b) for a in range(gx) for b in range(chips_y)), key=lambda p: -hops(p[0], gx) - hops(p[1], chips_y))
    plane = [(xs[a], ys[b], iz) for a, b in steps if a or b]
    step_y = [ys[k] for k in dict.fromkeys((1, chips_y - 1)) if k % chips_y]
    near = [(xs[k], iy, iz) for k in dict.fromkeys((1, gx - 1))] + [(ix, beyond, iz), (ix, across, iz)]
    near += [(ix, iy, zs[k]) for k in dict.fromkeys((1, gz - 1))] + [(ix, y, iz) for y in step_y]
    second = [(xs[2 % gx], iy, iz), (ix, ys[2 % chips_y], iz)] if gx > 2 and chips_y > 2 else []
    second += [(ix, iy, zs[k]) for k in dict.fromkeys((2, gz - 2))] if gz > 3 else []

    barrier = pltpu.get_barrier_semaphore()
    for device in near:
        pl.semaphore_signal(barrier, inc=1, device_id=device, device_id_type=MESH)

    def tell(stage, devices):
        for device in devices:
            pl.semaphore_signal(heard.at[stage], inc=1, device_id=device, device_id_type=MESH)

    zero_x = jnp.zeros((F, NY, NZ), jnp.float32)
    zero_y = jnp.zeros((F, NX, 1, NZ), jnp.float32)
    for turn, buf in enumerate((buf_p, buf_q)):
        buf[:, 1:NX + 1, TOP - 1:TOP] = zero_y
        buf[:, 1:NX + 1, TOP + NY:TOP + NY + 1] = zero_y
        for way in range(2):
            @pl.when(ix == way * (gx - 1))
            def _():
                buf[:, way * (NX + 1), ROWS] = zero_x

            @pl.when(iy == way * (gy - 1))
            def _():
                y_halo[turn, way] = zero_y

            @pl.when(iz == way * (gz - 1))
            def _():
                inner_r[turn, way] = jnp.zeros((INNER, NZ), jnp.float32)
                face_r[turn, way] = jnp.zeros((FACE, NZ), jnp.float32)

    bufs, both = (buf_p, buf_q), range(2)
    has = {
        "x": (ix > 0, ix < gx - 1),
        "y": (iy > 0, iy < gy - 1),
        "z": (iz > 0, iz < gz - 1),
    }

    def x_copy(turn, way, group):
        fields = slice(group * WIDE, (group + 1) * WIDE)
        buf = bufs[turn]
        return pltpu.make_async_remote_copy(
            src_ref=buf.at[fields, NX if way else 1, ROWS],
            dst_ref=buf.at[fields, 0 if way else NX + 1, ROWS],
            send_sem=xs_sem.at[turn, way, group],
            recv_sem=xr_sem.at[turn, way, group],
            device_id=(ix + 1 if way else ix - 1, iy, iz),
            device_id_type=MESH,
        )

    spans = ((2, NX), (1, 2), (NX, NX + 1))

    def y_copy(turn, way, part):
        buf, (low, high) = bufs[turn], spans[part]
        edge = TOP + NY - 1 if way else TOP
        return pltpu.make_async_remote_copy(
            src_ref=buf.at[:, low:high, edge:edge + 1],
            dst_ref=y_halo.at[turn, 1 - way, :, low - 1:high - 1],
            send_sem=ys_sem.at[turn, way, part],
            recv_sem=yr_sem.at[turn, way, part],
            device_id=(ix, iy + 1 if way else iy - 1, iz),
            device_id_type=MESH,
        )

    def z_copy(turn, way, part):
        source, target = ((inner_s, inner_r), (face_s, face_r))[part]
        return pltpu.make_async_remote_copy(
            src_ref=source.at[turn, way],
            dst_ref=target.at[turn, 0 if way else 1],
            send_sem=zs_sem.at[turn, way, part],
            recv_sem=zr_sem.at[turn, way, part],
            device_id=(ix, iy, iz + 1 if way else iz - 1),
            device_id_type=MESH,
        )

    def start(axis, way, copies):
        @pl.when(has[axis][way])
        def _():
            for copy in copies:
                copy.start()

    def arrive(axis, way, copies):
        @pl.when(has[axis][1 - way])
        def _():
            for copy in copies:
                copy.wait_recv()

    def sent(axis, way, copies):
        @pl.when(has[axis][way])
        def _():
            for copy in copies:
                copy.wait_send()

    tiles = ([], [])
    for f in range(0, F, 2):
        tiles[0].append([(f, 2, 6)])
        tiles[0].append([(f, 6, 8), (f + 1, 2, 4)])
        tiles[0].append([(f + 1, 4, 8)])
        tiles[1].append([(f, 1, 2), (f, 8, 9), (f + 1, 1, 2), (f + 1, 8, 9)])

    def pack_z(turn, part):
        buf, target = bufs[turn], (inner_s, face_s)[part]
        for t, pieces in enumerate(tiles[part]):
            tile = jnp.concatenate([buf[f, a:b, ROWS] for f, a, b in pieces], axis=0)
            tile = tile.reshape(NZ, NZ).T
            target[turn, 0, t:t + 1] = tile[0:1]
            target[turn, 1, t:t + 1] = tile[NZ - 1:NZ]

    lane = lax.broadcasted_iota(jnp.int32, (NY, NZ), 1)
    first, last = lane == 0, lane == NZ - 1
    edges = jnp.logical_or(first, last)

    def dots(left, right, x, sums):
        for t in range(NY // 8):
            rows = slice(TOP + 8 * t, TOP + 8 * t + 8)
            u = left[:, x, rows]
            v = u if right is left else right[:, x, rows]
            sums = tuple(sums[i] + u[i:i + 1] * v[i:] for i in range(F))
        return sums

    def inside(src, dst, left, right, sums):
        def step(x, sums):
            for f in range(F):
                c = src[f, x, ROWS]
                beside = src[f, x, TOP + 1:TOP + NY + 1] + src[f, x, TOP - 1:TOP + NY - 1]
                for other in (x - 1, x + 1):
                    if not isinstance(x, int) or 1 <= other <= NX:
                        beside = beside + src[f, other, ROWS]
                beside = beside + jnp.where(last, 0.0, pltpu.roll(c, NZ - 1, 1))
                beside = beside + jnp.where(first, 0.0, pltpu.roll(c, 1, 1))
                dst[f, x, ROWS] = diag[x - 1] * c - beside
            return dots(left, right, x, sums)

        sums = lax.fori_loop(2, NX, step, step(1, sums))
        return step(NX, sums)

    def take_x(src, dst, turn, group):
        for way in both:
            arrive("x", way, [x_copy(turn, way, group)])
        for f in range(group * WIDE, (group + 1) * WIDE):
            dst[f, 1, ROWS] -= src[f, 0, ROWS]
            dst[f, NX, ROWS] -= src[f, NX + 1, ROWS]

    def take_y(dst, turn, parts):
        for way in both:
            arrive("y", way, [y_copy(turn, way, part) for part in parts])
        for part in parts:
            low, high = spans[part]
            for way, edge in enumerate((TOP, TOP + NY - 1)):
                dst[:, low:high, edge:edge + 1] -= y_halo[turn, way, :, low - 1:high - 1]

    def take_z(dst, turn, part):
        for way in both:
            arrive("z", way, [z_copy(turn, way, part)])
        source = (inner_r, face_r)[part]
        for t, pieces in enumerate(tiles[part]):
            low = jnp.broadcast_to(source[turn, 0, t:t + 1], (NZ // 2, NZ))
            high = jnp.broadcast_to(source[turn, 1, t:t + 1], (NZ // 2, NZ))
            tile = jnp.concatenate([low, high], axis=0).T.reshape(4, NY, NZ)
            at = 0
            for f, a, b in pieces:
                dst[f, a:b, ROWS] -= jnp.where(edges, tile[at:at + b - a], 0.0)
                at += b - a

    def moment(left, right, low, high, sums):
        return lax.fori_loop(low, high, lambda x, sums: dots(left, right, x, sums), sums)

    def faces(left, right, sums):
        return lax.fori_loop(0, 2, lambda k, sums: dots(left, right, 1 + (NX - 1) * k, sums), sums)

    none = tuple(jnp.zeros((F - i,) + TILE, jnp.float32) for i in range(F))

    sub = lax.broadcasted_iota(jnp.int32, TILE, 0)
    cell = lax.broadcasted_iota(jnp.int32, TILE, 1)

    def fold(parts):
        width = 1
        while len(parts) > 1:
            odd = (sub & width) != 0
            merged = []
            for i in range(0, len(parts), 2):
                a, b = parts[i], parts[i + 1]
                kept = jnp.where(odd, b, a)
                moved = jnp.where(odd, a, b)
                moved = jnp.where(odd, pltpu.roll(moved, width, 0), pltpu.roll(moved, 8 - width, 0))
                merged.append(kept + moved)
            parts = merged
            width *= 2
        return parts[0]

    place = lax.rem(cell, 2 * F)
    own = sub == lax.rem(F - lax.div(cell, 2 * F), F)

    def gather(k, sums, total):
        for c in range(F):
            line = fold([sums[min(i, c)][max(i, c) - min(i, c)] for i in range(F)])
            total = jnp.where(place == k * F + c, jnp.sum(line, axis=1, keepdims=True), total)
        return total

    def as_row(total):
        return jnp.sum(jnp.where(own, total, 0.0), axis=0, keepdims=True)

    def copy_part(stage, src, dst, device):
        return pltpu.make_async_remote_copy(
            src_ref=src, dst_ref=dst,
            send_sem=g_send.at[stage], recv_sem=g_recv.at[stage],
            device_id=device, device_id_type=MESH)

    def spread(stage, parts, mine, devices, rows):
        for k, value in enumerate(rows):
            parts[mine, k:k + 1] = value
        for device in devices:
            copy_part(stage, parts.at[mine], parts.at[mine], device).start()
        count = len(devices)
        return copy_part(stage, parts.at[0:count], parts.at[0:count], devices[0])

    def added(parts, count):
        sums = [parts[k] for k in range(count)]
        while len(sums) > 1:
            sums = [sums[k] + sums[k + 1] for k in range(0, len(sums), 2)]
        return sums[0]

    loads[0].wait()
    loads[1].wait()
    pl.semaphore_wait(barrier, len(near))
    for way in both:
        start("x", way, [x_copy(0, way, group) for group in range(GROUPS)])
    tell(0, near)
    loads[2].wait()
    for way in both:
        start("y", way, [y_copy(0, way, part) for part in range(3)])
    for part in both:
        pack_z(0, part)
    for way in both:
        start("z", way, [z_copy(0, way, part) for part in both])
    loads[3].wait()
    diag[...] = 6.0 + diag[...]
    zeroth = inside(buf_p, buf_q, buf_p, buf_p, none)
    blank = jnp.zeros(TILE, jnp.float32)
    row_zero = as_row(gather(0, zeroth, blank))
    pl.semaphore_wait(heard.at[0], len(near))
    tell(1, second)
    take_y(buf_q, 0, range(3))
    for part in both:
        take_z(buf_q, 0, part)

    def forward(group):
        take_x(buf_p, buf_q, 0, group)
        for way in both:
            start("x", way, [x_copy(1, way, group)])

    forward(0)
    for way in both:
        start("y", way, [y_copy(1, way, 0)])
    pack_z(1, 0)
    for way in both:
        start("z", way, [z_copy(1, way, 0)])
    forward(1)
    second_sums = moment(buf_q, buf_q, 2, NX, none)
    forward(2)
    for group in range(3, GROUPS):
        forward(group)
    for way in both:
        start("y", way, [y_copy(1, way, part) for part in (1, 2)])
    pack_z(1, 1)
    for way in both:
        start("z", way, [z_copy(1, way, 1)])

    if second:
        pl.semaphore_wait(heard.at[1], len(second))
    tell(2, [(ix, across, iz)])

    total = gather(0, inside(buf_q, buf_r, buf_p, buf_q, none), blank)
    total = gather(1, faces(buf_q, buf_q, second_sums), total)
    row_one = as_row(total)
    pl.semaphore_wait(heard.at[2], 1)
    in_line = 2 * iz + core
    early_done = spread(0, part_e, in_line, line, (row_zero, row_one))
    take_y(buf_r, 1, (0,))
    take_z(buf_r, 1, 0)
    third = moment(buf_q, buf_r, 2, NX, none)
    fourth = moment(buf_r, buf_r, 2, NX, none)
    take_y(buf_r, 1, (1, 2))
    take_z(buf_r, 1, 1)
    for group in range(GROUPS):
        take_x(buf_q, buf_r, 1, group)
    third = faces(buf_q, buf_r, third)
    fourth = faces(buf_r, buf_r, fourth)
    row_two = as_row(gather(1, fourth, gather(0, third, blank)))

    late_done = spread(1, part_l, in_line, line, (row_two,))
    early_done.wait_recv()
    early = added(part_e, len(line) + 1)
    late_done.wait_recv()
    late = added(part_l, len(line) + 1)
    chip = ix * chips_y + lax.div(row, 2)
    planes_done = spread(2, part_p, chip, plane, (early[0:1], early[1:2], late))
    planes_done.wait_recv()
    gram_ref[...] = added(part_p, len(plane) + 1)

    early_done.wait_send()
    late_done.wait_send()
    planes_done.wait_send()
    for turn in both:
        for way in both:
            sent("x", way, [x_copy(turn, way, group) for group in range(GROUPS)])
            sent("y", way, [y_copy(turn, way, part) for part in range(3)])
            sent("z", way, [z_copy(turn, way, part) for part in both])


def combine_kernel(gram_ref, buf_b, buf_a, x_hbm, norm_ref, buf_x, coeff, out_sem):
    turned = [
        pltpu.roll(jnp.broadcast_to(gram_ref[k:k + 1], TILE), 0, 1, stride=2 * F, stride_axis=0) for k in range(3)
    ]
    sub = lax.broadcasted_iota(jnp.int32, TILE, 0)
    cell = lax.broadcasted_iota(jnp.int32, TILE, 1)

    def column(order, c):
        k, half = ((0, 0), (1, 0), (1, 1), (2, 0), (2, 1))[order]
        at = half * F + c
        return jnp.broadcast_to(turned[k][:, at:at + 1], TILE)

    def spread(value, row):
        return jnp.broadcast_to(value[row:row + 1], TILE)

    moments = [[column(order, c) for c in range(F)] for order in range(5)]
    columns = [[moments[2][c], moments[3][c]] for c in range(F)]
    columns += [[moments[3][c], moments[4][c]] for c in range(F)]
    rights = [[moments[1][c], moments[2][c]] for c in range(F)]
    for k in range(2 * F):
        half, row = k // F, k % F
        pivot = columns[k]
        inverse = 1.0 / spread(pivot[half], row)
        mine = sub == row
        for other in columns[k + 1:] + rights:
            r = spread(other[half], row) * inverse
            for h in range(2):
                value = other[h] - pivot[h] * r
                other[h] = jnp.where(mine, r, value) if h == half else value
    norms = jnp.zeros((1, 128), jnp.float32)
    for c in range(F):
        for h in range(2):
            coeff[c, h] = rights[c][h]
        fit = moments[1][c] * rights[c][0] + moments[2][c] * rights[c][1]
        left = jnp.where(sub == c, moments[0][c], 0.0) - fit
        norms = jnp.where(cell[0:1] == c, jnp.sum(left, axis=0, keepdims=True), norms)
    norm_ref[...] = jnp.sqrt(jnp.maximum(norms, 0.0))[:, :F]

    def out(x):
        return pltpu.make_async_copy(buf_x.at[:, x], x_hbm.at[:, x], out_sem.at[x])

    def step(x, _):
        for t in range(NY // 8):
            rows = slice(8 * t, 8 * t + 8)
            held = slice(TOP + 8 * t, TOP + 8 * t + 8)
            fields = [buf_b[:, x + 1, held], buf_a[:, x + 1, held]]
            for c in range(F):
                sums = [None, None]
                for h in range(2):
                    for i in range(F):
                        term = jnp.broadcast_to(coeff[c, h, i:i + 1], TILE) * fields[h][i]
                        sums[h] = term if sums[h] is None else sums[h] + term
                buf_x[c, x, rows] = sums[0] + sums[1]
        out(x).start()
        return 0

    lax.fori_loop(0, NX, step, 0)
    for x in range(NX):
        out(x).wait()


def solution(mesh):
    gx, gy, gz = mesh.shape["gx"], mesh.shape["gy"], mesh.shape["gz"]
    f32 = jnp.float32
    dma = pltpu.SemaphoreType.DMA
    hbm = pl.BlockSpec(memory_space=pltpu.HBM)
    vmem = pl.BlockSpec(memory_space=pltpu.VMEM)
    block = (F, NX, NY, NZ)
    padded = (F, NX + 2, NY + 16, NZ)

    def body(right_side, shift):
        gram, fields, images = pl.pallas_call(
            functools.partial(exchange_kernel, gx, gy, gz),
            out_shape=(
                jax.ShapeDtypeStruct((3, NZ), f32),
                jax.ShapeDtypeStruct(padded, f32),
                jax.ShapeDtypeStruct(padded, f32),
            ),
            in_specs=[hbm, hbm],
            out_specs=(vmem, vmem, vmem),
            scratch_shapes=[
                pltpu.VMEM(padded, f32),
                pltpu.VMEM((NX, NY, NZ), f32),
                pltpu.VMEM((2, 2, F, NX, 1, NZ), f32),
                pltpu.VMEM((2, 2, INNER, NZ), f32),
                pltpu.VMEM((2, 2, INNER, NZ), f32),
                pltpu.VMEM((2, 2, FACE, NZ), f32),
                pltpu.VMEM((2, 2, FACE, NZ), f32),
                pltpu.VMEM((2 * gz, 2, NZ), f32),
                pltpu.VMEM((2 * gz, 1, NZ), f32),
                pltpu.VMEM((gx * gy // 2, 3, NZ), f32),
                dma((4,)),
                dma((2, 2, GROUPS)),
                dma((2, 2, GROUPS)),
                dma((2, 2, 3)),
                dma((2, 2, 3)),
                dma((2, 2, 2)),
                dma((2, 2, 2)),
                dma((3,)),
                dma((3,)),
                pltpu.SemaphoreType.REGULAR((3,)),
            ],
            compiler_params=pltpu.CompilerParams(
                collective_id=0, has_side_effects=True, vmem_limit_bytes=24 << 20
            ),
        )(*(pltpu.with_memory_space_constraint(a, pltpu.HBM) for a in (right_side, shift)))
        solved, norms = pl.pallas_call(
            combine_kernel,
            out_shape=(jax.ShapeDtypeStruct(block, f32), jax.ShapeDtypeStruct((1, F), f32)),
            in_specs=[vmem, vmem, vmem],
            out_specs=(hbm, vmem),
            scratch_shapes=[
                pltpu.VMEM(block, f32),
                pltpu.VMEM((F, 2) + TILE, f32),
                dma((NX,)),
            ],
            compiler_params=pltpu.CompilerParams(vmem_limit_bytes=16 << 20),
        )(gram, fields, images)
        return solved, norms.reshape(F)

    return jax.shard_map(
        body,
        mesh=mesh,
        in_specs=(P(None, "gx", "gy", "gz"), P("gx", "gy", "gz")),
        out_specs=(P(None, "gx", "gy", "gz"), P()),
        check_vma=False,
    )
```

```python
import functools

import jax
import jax.numpy as jnp
from jax import lax
from jax.experimental import pallas as pl
from jax.experimental.pallas import tpu as pltpu
from jax.sharding import PartitionSpec as P

MESH = pl.DeviceIdType.MESH
F, NX, NY, NZ = 8, 8, 32, 128
TOP = 8
ROWS = slice(TOP, TOP + NY)
CUTS = (0, 4, 7, 8)
GROUPS = len(CUTS) - 1
INNER, FACE = 12, 4
TILE = (8, 128)


def exchange_kernel(gx, gy, gz, b_hbm, s_hbm, gram_ref, buf_p, buf_q,
                    buf_r, diag, y_halo, inner_s, inner_r, face_s, face_r, part_e, part_l, part_p,
                    load_sem, xs_sem, xr_sem, ys_sem, yr_sem, zs_sem, zr_sem, g_send, g_recv, heard):
    ix, iy, iz = lax.axis_index("gx"), lax.axis_index("gy"), lax.axis_index("gz")

    loads = [
        pltpu.make_async_copy(b_hbm.at[:, 0], buf_p.at[:, 1, ROWS], load_sem.at[0]),
        pltpu.make_async_copy(b_hbm.at[:, NX - 1], buf_p.at[:, NX, ROWS], load_sem.at[1]),
        pltpu.make_async_copy(b_hbm.at[:, 1:NX - 1], buf_p.at[:, 2:NX, ROWS], load_sem.at[2]),
        pltpu.make_async_copy(s_hbm, diag, load_sem.at[3]),
    ]
    for load in loads:
        load.start()

    chips_y = gy // 2
    core = lax.rem(iy, 2)
    row = iy - core
    xs = [ix] + [lax.rem(ix + k, gx) for k in range(1, gx)]
    ys = [iy] + [lax.rem(iy + 2 * k, gy) for k in range(1, chips_y)]
    zs = [iz] + [lax.rem(iz + k, gz) for k in range(1, gz)]
    across = row + 1 - core
    beyond = lax.rem(iy + gy - 1 + 2 * core, gy)
    def hops(k, n):
        return min(k, n - k)

    line = [(ix, y, zs[k]) for k in sorted(range(1, gz), key=lambda k: -hops(k, gz)) for y in (across, iy)]
    line += [(ix, across, iz)]
    steps = sorted(((a, b) for a in range(gx) for b in range(chips_y)), key=lambda p: -hops(p[0], gx) - hops(p[1], chips_y))
    plane = [(xs[a], ys[b], iz) for a, b in steps if a or b]
    step_y = [ys[k] for k in dict.fromkeys((1, chips_y - 1)) if k % chips_y]
    near = [(xs[k], iy, iz) for k in dict.fromkeys((1, gx - 1))] + [(ix, beyond, iz), (ix, across, iz)]
    near += [(ix, iy, zs[k]) for k in dict.fromkeys((1, gz - 1))] + [(ix, y, iz) for y in step_y]
    second = [(xs[2 % gx], iy, iz), (ix, ys[2 % chips_y], iz)] if gx > 2 and chips_y > 2 else []
    second += [(ix, iy, zs[k]) for k in dict.fromkeys((2, gz - 2))] if gz > 3 else []

    barrier = pltpu.get_barrier_semaphore()
    for device in near:
        pl.semaphore_signal(barrier, inc=1, device_id=device, device_id_type=MESH)

    def tell(stage, devices):
        for device in devices:
            pl.semaphore_signal(heard.at[stage], inc=1, device_id=device, device_id_type=MESH)

    zero_x = jnp.zeros((F, NY, NZ), jnp.float32)
    zero_y = jnp.zeros((F, NX, 1, NZ), jnp.float32)
    for turn, buf in enumerate((buf_p, buf_q)):
        buf[:, 1:NX + 1, TOP - 1:TOP] = zero_y
        buf[:, 1:NX + 1, TOP + NY:TOP + NY + 1] = zero_y
        for way in range(2):
            @pl.when(ix == way * (gx - 1))
            def _():
                buf[:, way * (NX + 1), ROWS] = zero_x

            @pl.when(iy == way * (gy - 1))
            def _():
                y_halo[turn, way] = zero_y

            @pl.when(iz == way * (gz - 1))
            def _():
                inner_r[turn, way] = jnp.zeros((INNER, NZ), jnp.float32)
                face_r[turn, way] = jnp.zeros((FACE, NZ), jnp.float32)

    bufs, both = (buf_p, buf_q), range(2)
    has = {
        "x": (ix > 0, ix < gx - 1),
        "y": (iy > 0, iy < gy - 1),
        "z": (iz > 0, iz < gz - 1),
    }

    def x_copy(turn, way, group):
        fields = slice(CUTS[group], CUTS[group + 1])
        buf = bufs[turn]
        return pltpu.make_async_remote_copy(
            src_ref=buf.at[fields, NX if way else 1, ROWS],
            dst_ref=buf.at[fields, 0 if way else NX + 1, ROWS],
            send_sem=xs_sem.at[turn, way, group],
            recv_sem=xr_sem.at[turn, way, group],
            device_id=(ix + 1 if way else ix - 1, iy, iz),
            device_id_type=MESH,
        )

    spans = ((2, NX), (1, 2), (NX, NX + 1), (1, NX + 1))
    y_parts = ((3,), (0, 1, 2))

    def y_copy(turn, way, part):
        buf, (low, high) = bufs[turn], spans[part]
        edge = TOP + NY - 1 if way else TOP
        return pltpu.make_async_remote_copy(
            src_ref=buf.at[:, low:high, edge:edge + 1],
            dst_ref=y_halo.at[turn, 1 - way, :, low - 1:high - 1],
            send_sem=ys_sem.at[turn, way, part],
            recv_sem=yr_sem.at[turn, way, part],
            device_id=(ix, iy + 1 if way else iy - 1, iz),
            device_id_type=MESH,
        )

    def z_copy(turn, way, part):
        source, target = ((inner_s, inner_r), (face_s, face_r))[part]
        return pltpu.make_async_remote_copy(
            src_ref=source.at[turn, way],
            dst_ref=target.at[turn, 0 if way else 1],
            send_sem=zs_sem.at[turn, way, part],
            recv_sem=zr_sem.at[turn, way, part],
            device_id=(ix, iy, iz + 1 if way else iz - 1),
            device_id_type=MESH,
        )

    def start(axis, way, copies):
        @pl.when(has[axis][way])
        def _():
            for copy in copies:
                copy.start()

    def arrive(axis, way, copies):
        @pl.when(has[axis][1 - way])
        def _():
            for copy in copies:
                copy.wait_recv()

    def sent(axis, way, copies):
        @pl.when(has[axis][way])
        def _():
            for copy in copies:
                copy.wait_send()

    tiles = ([], [])
    for f in range(0, F, 2):
        tiles[0].append([(f, 2, 6)])
        tiles[0].append([(f, 6, 8), (f + 1, 2, 4)])
        tiles[0].append([(f + 1, 4, 8)])
        tiles[1].append([(f, 1, 2), (f, 8, 9), (f + 1, 1, 2), (f + 1, 8, 9)])

    def pack_z(turn, part):
        buf, target = bufs[turn], (inner_s, face_s)[part]
        for t, pieces in enumerate(tiles[part]):
            tile = jnp.concatenate([buf[f, a:b, ROWS] for f, a, b in pieces], axis=0)
            tile = tile.reshape(NZ, NZ).T
            target[turn, 0, t:t + 1] = tile[0:1]
            target[turn, 1, t:t + 1] = tile[NZ - 1:NZ]

    lane = lax.broadcasted_iota(jnp.int32, (NY, NZ), 1)
    first, last = lane == 0, lane == NZ - 1
    edges = jnp.logical_or(first, last)

    def dots(left, right, x, sums):
        for t in range(NY // 8):
            rows = slice(TOP + 8 * t, TOP + 8 * t + 8)
            u = left[:, x, rows]
            v = u if right is left else right[:, x, rows]
            sums = tuple(sums[i] + u[i:i + 1] * v[i:] for i in range(F))
        return sums

    def inside(src, dst, left, right, sums):
        def step(x, sums):
            for f in range(F):
                c = src[f, x, ROWS]
                beside = src[f, x, TOP + 1:TOP + NY + 1] + src[f, x, TOP - 1:TOP + NY - 1]
                for other in (x - 1, x + 1):
                    if not isinstance(x, int) or 1 <= other <= NX:
                        beside = beside + src[f, other, ROWS]
                beside = beside + jnp.where(last, 0.0, pltpu.roll(c, NZ - 1, 1))
                beside = beside + jnp.where(first, 0.0, pltpu.roll(c, 1, 1))
                dst[f, x, ROWS] = diag[x - 1] * c - beside
            return dots(left, right, x, sums)

        sums = lax.fori_loop(2, NX, step, step(1, sums))
        return step(NX, sums)

    def alone(src, dst):
        def step(f, _):
            for x in range(1, NX + 1):
                c = src[f, x, ROWS]
                beside = src[f, x, TOP + 1:TOP + NY + 1] + src[f, x, TOP - 1:TOP + NY - 1]
                for other in (x - 1, x + 1):
                    if 1 <= other <= NX:
                        beside = beside + src[f, other, ROWS]
                beside = beside + jnp.where(last, 0.0, pltpu.roll(c, NZ - 1, 1))
                beside = beside + jnp.where(first, 0.0, pltpu.roll(c, 1, 1))
                dst[f, x, ROWS] = diag[x - 1] * c - beside
            return 0

        lax.fori_loop(0, F, step, 0)

    def take_x(src, dst, turn, group):
        for way in both:
            arrive("x", way, [x_copy(turn, way, group)])
        for f in range(CUTS[group], CUTS[group + 1]):
            dst[f, 1, ROWS] -= src[f, 0, ROWS]
            dst[f, NX, ROWS] -= src[f, NX + 1, ROWS]

    def take_y(dst, turn, parts):
        for way in both:
            arrive("y", way, [y_copy(turn, way, part) for part in parts])
        for part in parts:
            low, high = spans[part]
            for way, edge in enumerate((TOP, TOP + NY - 1)):
                dst[:, low:high, edge:edge + 1] -= y_halo[turn, way, :, low - 1:high - 1]

    def take_z(dst, turn, part):
        for way in both:
            arrive("z", way, [z_copy(turn, way, part)])
        source = (inner_r, face_r)[part]
        for t, pieces in enumerate(tiles[part]):
            low = jnp.broadcast_to(source[turn, 0, t:t + 1], (NZ // 2, NZ))
            high = jnp.broadcast_to(source[turn, 1, t:t + 1], (NZ // 2, NZ))
            tile = jnp.concatenate([low, high], axis=0).T.reshape(4, NY, NZ)
            at = 0
            for f, a, b in pieces:
                dst[f, a:b, ROWS] -= jnp.where(edges, tile[at:at + b - a], 0.0)
                at += b - a

    def moment(left, right, low, high, sums):
        return lax.fori_loop(low, high, lambda x, sums: dots(left, right, x, sums), sums)

    def faces(left, right, sums):
        return lax.fori_loop(0, 2, lambda k, sums: dots(left, right, 1 + (NX - 1) * k, sums), sums)

    none = tuple(jnp.zeros((F - i,) + TILE, jnp.float32) for i in range(F))

    sub = lax.broadcasted_iota(jnp.int32, TILE, 0)
    cell = lax.broadcasted_iota(jnp.int32, TILE, 1)

    def fold(parts):
        width = 1
        while len(parts) > 1:
            odd = (sub & width) != 0
            merged = []
            for i in range(0, len(parts), 2):
                a, b = parts[i], parts[i + 1]
                kept = jnp.where(odd, b, a)
                moved = jnp.where(odd, a, b)
                moved = jnp.where(odd, pltpu.roll(moved, width, 0), pltpu.roll(moved, 8 - width, 0))
                merged.append(kept + moved)
            parts = merged
            width *= 2
        return parts[0]

    place = lax.rem(cell, 2 * F)
    own = sub == lax.rem(F - lax.div(cell, 2 * F), F)

    def gather(k, sums, total):
        for c in range(F):
            line = fold([sums[min(i, c)][max(i, c) - min(i, c)] for i in range(F)])
            total = jnp.where(place == k * F + c, jnp.sum(line, axis=1, keepdims=True), total)
        return total

    def as_row(total):
        return jnp.sum(jnp.where(own, total, 0.0), axis=0, keepdims=True)

    def copy_part(stage, src, dst, device):
        return pltpu.make_async_remote_copy(
            src_ref=src, dst_ref=dst,
            send_sem=g_send.at[stage], recv_sem=g_recv.at[stage],
            device_id=device, device_id_type=MESH)

    def spread(stage, parts, mine, devices, rows):
        for k, value in enumerate(rows):
            parts[mine, k:k + 1] = value
        for device in devices:
            copy_part(stage, parts.at[mine], parts.at[mine], device).start()
        count = len(devices)
        return copy_part(stage, parts.at[0:count], parts.at[0:count], devices[0])

    def added(parts, count):
        sums = [parts[k] for k in range(count)]
        while len(sums) > 1:
            sums = [sums[k] + sums[k + 1] for k in range(0, len(sums), 2)]
        return sums[0]

    loads[0].wait()
    loads[1].wait()
    pl.semaphore_wait(barrier, len(near))
    for way in both:
        start("x", way, [x_copy(0, way, group) for group in range(GROUPS)])
    tell(0, near)
    loads[2].wait()
    for way in both:
        start("y", way, [y_copy(0, way, part) for part in y_parts[0]])
    for part in both:
        pack_z(0, part)
    for way in both:
        start("z", way, [z_copy(0, way, part) for part in both])
    loads[3].wait()
    diag[...] = 6.0 + diag[...]
    zeroth = inside(buf_p, buf_q, buf_p, buf_p, none)
    blank = jnp.zeros(TILE, jnp.float32)
    row_zero = as_row(gather(0, zeroth, blank))
    pl.semaphore_wait(heard.at[0], len(near))
    tell(1, second)
    take_y(buf_q, 0, y_parts[0])
    for part in both:
        take_z(buf_q, 0, part)

    def forward(group):
        take_x(buf_p, buf_q, 0, group)
        for way in both:
            start("x", way, [x_copy(1, way, group)])

    forward(0)
    for way in both:
        start("y", way, [y_copy(1, way, 0)])
    pack_z(1, 0)
    for way in both:
        start("z", way, [z_copy(1, way, 0)])
    forward(1)
    second_sums = moment(buf_q, buf_q, 2, NX, none)
    forward(2)
    for group in range(3, GROUPS):
        forward(group)
    for way in both:
        start("y", way, [y_copy(1, way, part) for part in (1, 2)])
    pack_z(1, 1)
    for way in both:
        start("z", way, [z_copy(1, way, 1)])

    if second:
        pl.semaphore_wait(heard.at[1], len(second))
    tell(2, [(ix, across, iz)])

    alone(buf_q, buf_r)
    total = gather(0, moment(buf_p, buf_q, 1, NX + 1, none), blank)
    total = gather(1, faces(buf_q, buf_q, second_sums), total)
    row_one = as_row(total)
    pl.semaphore_wait(heard.at[2], 1)
    in_line = 2 * iz + core
    early_done = spread(0, part_e, in_line, line, (row_zero, row_one))
    take_y(buf_r, 1, (0,))
    take_z(buf_r, 1, 0)
    third = moment(buf_q, buf_r, 2, NX, none)
    fourth = moment(buf_r, buf_r, 2, NX, none)
    take_y(buf_r, 1, (1, 2))
    take_z(buf_r, 1, 1)
    for group in range(GROUPS):
        take_x(buf_q, buf_r, 1, group)
    third = faces(buf_q, buf_r, third)
    fourth = faces(buf_r, buf_r, fourth)
    row_two = as_row(gather(1, fourth, gather(0, third, blank)))

    late_done = spread(1, part_l, in_line, line, (row_two,))
    early_done.wait_recv()
    early = added(part_e, len(line) + 1)
    late_done.wait_recv()
    late = added(part_l, len(line) + 1)
    chip = ix * chips_y + lax.div(row, 2)
    planes_done = spread(2, part_p, chip, plane, (early[0:1], early[1:2], late))
    planes_done.wait_recv()
    gram_ref[...] = added(part_p, len(plane) + 1)

    early_done.wait_send()
    late_done.wait_send()
    planes_done.wait_send()
    for turn in both:
        for way in both:
            sent("x", way, [x_copy(turn, way, group) for group in range(GROUPS)])
            sent("y", way, [y_copy(turn, way, part) for part in y_parts[turn]])
            sent("z", way, [z_copy(turn, way, part) for part in both])


def combine_kernel(gram_ref, buf_b, buf_a, x_hbm, norm_ref, buf_x, coeff, out_sem):
    turned = [
        pltpu.roll(jnp.broadcast_to(gram_ref[k:k + 1], TILE), 0, 1, stride=2 * F, stride_axis=0) for k in range(3)
    ]
    sub = lax.broadcasted_iota(jnp.int32, TILE, 0)
    cell = lax.broadcasted_iota(jnp.int32, TILE, 1)

    def column(order, c):
        k, half = ((0, 0), (1, 0), (1, 1), (2, 0), (2, 1))[order]
        at = half * F + c
        return jnp.broadcast_to(turned[k][:, at:at + 1], TILE)

    def spread(value, row):
        return jnp.broadcast_to(value[row:row + 1], TILE)

    moments = [[column(order, c) for c in range(F)] for order in range(5)]
    columns = [[moments[2][c], moments[3][c]] for c in range(F)]
    columns += [[moments[3][c], moments[4][c]] for c in range(F)]
    rights = [[moments[1][c], moments[2][c]] for c in range(F)]
    for k in range(2 * F):
        half, row = k // F, k % F
        pivot = columns[k]
        inverse = 1.0 / spread(pivot[half], row)
        mine = sub == row
        for other in columns[k + 1:] + rights:
            r = spread(other[half], row) * inverse
            for h in range(2):
                value = other[h] - pivot[h] * r
                other[h] = jnp.where(mine, r, value) if h == half else value
    norms = jnp.zeros((1, 128), jnp.float32)
    for c in range(F):
        for h in range(2):
            coeff[c, h] = rights[c][h]
        fit = moments[1][c] * rights[c][0] + moments[2][c] * rights[c][1]
        left = jnp.where(sub == c, moments[0][c], 0.0) - fit
        norms = jnp.where(cell[0:1] == c, jnp.sum(left, axis=0, keepdims=True), norms)
    norm_ref[...] = jnp.sqrt(jnp.maximum(norms, 0.0))[:, :F]

    def out(x):
        return pltpu.make_async_copy(buf_x.at[:, x], x_hbm.at[:, x], out_sem.at[x])

    def step(x, _):
        for t in range(NY // 8):
            rows = slice(8 * t, 8 * t + 8)
            held = slice(TOP + 8 * t, TOP + 8 * t + 8)
            fields = [buf_b[:, x + 1, held], buf_a[:, x + 1, held]]
            for c in range(F):
                sums = [None, None]
                for h in range(2):
                    for i in range(F):
                        term = jnp.broadcast_to(coeff[c, h, i:i + 1], TILE) * fields[h][i]
                        sums[h] = term if sums[h] is None else sums[h] + term
                buf_x[c, x, rows] = sums[0] + sums[1]
        out(x).start()
        return 0

    lax.fori_loop(0, NX, step, 0)
    for x in range(NX):
        out(x).wait()


def solution(mesh):
    gx, gy, gz = mesh.shape["gx"], mesh.shape["gy"], mesh.shape["gz"]
    f32 = jnp.float32
    dma = pltpu.SemaphoreType.DMA
    hbm = pl.BlockSpec(memory_space=pltpu.HBM)
    vmem = pl.BlockSpec(memory_space=pltpu.VMEM)
    block = (F, NX, NY, NZ)
    padded = (F, NX + 2, NY + 16, NZ)

    def body(right_side, shift):
        gram, fields, images = pl.pallas_call(
            functools.partial(exchange_kernel, gx, gy, gz),
            out_shape=(
                jax.ShapeDtypeStruct((3, NZ), f32),
                jax.ShapeDtypeStruct(padded, f32),
                jax.ShapeDtypeStruct(padded, f32),
            ),
            in_specs=[hbm, hbm],
            out_specs=(vmem, vmem, vmem),
            scratch_shapes=[
                pltpu.VMEM(padded, f32),
                pltpu.VMEM((NX, NY, NZ), f32),
                pltpu.VMEM((2, 2, F, NX, 1, NZ), f32),
                pltpu.VMEM((2, 2, INNER, NZ), f32),
                pltpu.VMEM((2, 2, INNER, NZ), f32),
                pltpu.VMEM((2, 2, FACE, NZ), f32),
                pltpu.VMEM((2, 2, FACE, NZ), f32),
                pltpu.VMEM((2 * gz, 2, NZ), f32),
                pltpu.VMEM((2 * gz, 1, NZ), f32),
                pltpu.VMEM((gx * gy // 2, 3, NZ), f32),
                dma((4,)),
                dma((2, 2, GROUPS)),
                dma((2, 2, GROUPS)),
                dma((2, 2, 4)),
                dma((2, 2, 4)),
                dma((2, 2, 2)),
                dma((2, 2, 2)),
                dma((3,)),
                dma((3,)),
                pltpu.SemaphoreType.REGULAR((3,)),
            ],
            compiler_params=pltpu.CompilerParams(
                collective_id=0, has_side_effects=True, vmem_limit_bytes=24 << 20
            ),
        )(*(pltpu.with_memory_space_constraint(a, pltpu.HBM) for a in (right_side, shift)))
        solved, norms = pl.pallas_call(
            combine_kernel,
            out_shape=(jax.ShapeDtypeStruct(block, f32), jax.ShapeDtypeStruct((1, F), f32)),
            in_specs=[vmem, vmem, vmem],
            out_specs=(hbm, vmem),
            scratch_shapes=[
                pltpu.VMEM(block, f32),
                pltpu.VMEM((F, 2) + TILE, f32),
                dma((NX,)),
            ],
            compiler_params=pltpu.CompilerParams(vmem_limit_bytes=16 << 20),
        )(gram, fields, images)
        return solved, norms.reshape(F)

    return jax.shard_map(
        body,
        mesh=mesh,
        in_specs=(P(None, "gx", "gy", "gz"), P("gx", "gy", "gz")),
        out_specs=(P(None, "gx", "gy", "gz"), P()),
        check_vma=False,
    )
```

```python
import functools

import jax
import jax.numpy as jnp
from jax import lax
from jax.experimental import pallas as pl
from jax.experimental.pallas import tpu as pltpu
from jax.sharding import PartitionSpec as P

MESH = pl.DeviceIdType.MESH
F, NX, NY, NZ = 8, 8, 32, 128
TOP = 8
ROWS = slice(TOP, TOP + NY)
CUTS = (0, 4, 7, 8)
GROUPS = len(CUTS) - 1
INNER, FACE = 12, 4
TILE = (8, 128)


def exchange_kernel(gx, gy, gz, b_hbm, s_hbm, gram_ref, buf_p, buf_q,
                    buf_r, diag, y_halo, inner_s, inner_r, face_s, face_r, part_e, part_l, part_p,
                    load_sem, xs_sem, xr_sem, ys_sem, yr_sem, zs_sem, zr_sem, g_send, g_recv, heard):
    ix, iy, iz = lax.axis_index("gx"), lax.axis_index("gy"), lax.axis_index("gz")

    loads = [
        pltpu.make_async_copy(b_hbm.at[:, 0], buf_p.at[:, 1, ROWS], load_sem.at[0]),
        pltpu.make_async_copy(b_hbm.at[:, NX - 1], buf_p.at[:, NX, ROWS], load_sem.at[1]),
        pltpu.make_async_copy(b_hbm.at[:, 1:NX - 1], buf_p.at[:, 2:NX, ROWS], load_sem.at[2]),
        pltpu.make_async_copy(s_hbm, diag, load_sem.at[3]),
    ]
    for load in loads:
        load.start()

    chips_y = gy // 2
    core = lax.rem(iy, 2)
    row = iy - core
    xs = [ix] + [lax.rem(ix + k, gx) for k in range(1, gx)]
    ys = [iy] + [lax.rem(iy + 2 * k, gy) for k in range(1, chips_y)]
    zs = [iz] + [lax.rem(iz + k, gz) for k in range(1, gz)]
    across = row + 1 - core
    beyond = lax.rem(iy + gy - 1 + 2 * core, gy)
    def hops(k, n):
        return min(k, n - k)

    line = [(ix, y, zs[k]) for k in sorted(range(1, gz), key=lambda k: -hops(k, gz)) for y in (across, iy)]
    line += [(ix, across, iz)]
    steps = sorted(((a, b) for a in range(gx) for b in range(chips_y)), key=lambda p: -hops(p[0], gx) - hops(p[1], chips_y))
    plane = [(xs[a], ys[b], iz) for a, b in steps if a or b]
    step_y = [ys[k] for k in dict.fromkeys((1, chips_y - 1)) if k % chips_y]
    near = [(xs[k], iy, iz) for k in dict.fromkeys((1, gx - 1))] + [(ix, beyond, iz), (ix, across, iz)]
    near += [(ix, iy, zs[k]) for k in dict.fromkeys((1, gz - 1))] + [(ix, y, iz) for y in step_y]
    second = [(xs[2 % gx], iy, iz), (ix, ys[2 % chips_y], iz)] if gx > 2 and chips_y > 2 else []
    second += [(ix, iy, zs[k]) for k in dict.fromkeys((2, gz - 2))] if gz > 3 else []

    barrier = pltpu.get_barrier_semaphore()
    for device in near:
        pl.semaphore_signal(barrier, inc=1, device_id=device, device_id_type=MESH)

    def tell(stage, devices):
        for device in devices:
            pl.semaphore_signal(heard.at[stage], inc=1, device_id=device, device_id_type=MESH)

    zero_x = jnp.zeros((F, NY, NZ), jnp.float32)
    zero_y = jnp.zeros((F, NX, 1, NZ), jnp.float32)
    for turn, buf in enumerate((buf_p, buf_q)):
        buf[:, 1:NX + 1, TOP - 1:TOP] = zero_y
        buf[:, 1:NX + 1, TOP + NY:TOP + NY + 1] = zero_y
        for way in range(2):
            @pl.when(ix == way * (gx - 1))
            def _():
                buf[:, way * (NX + 1), ROWS] = zero_x

            @pl.when(iy == way * (gy - 1))
            def _():
                y_halo[turn, way] = zero_y

            @pl.when(iz == way * (gz - 1))
            def _():
                inner_r[turn, way] = jnp.zeros((INNER, NZ), jnp.float32)
                face_r[turn, way] = jnp.zeros((FACE, NZ), jnp.float32)

    bufs, both = (buf_p, buf_q), range(2)
    has = {
        "x": (ix > 0, ix < gx - 1),
        "y": (iy > 0, iy < gy - 1),
        "z": (iz > 0, iz < gz - 1),
    }

    def x_copy(turn, way, group):
        fields = slice(CUTS[group], CUTS[group + 1])
        buf = bufs[turn]
        return pltpu.make_async_remote_copy(
            src_ref=buf.at[fields, NX if way else 1, ROWS],
            dst_ref=buf.at[fields, 0 if way else NX + 1, ROWS],
            send_sem=xs_sem.at[turn, way, group],
            recv_sem=xr_sem.at[turn, way, group],
            device_id=(ix + 1 if way else ix - 1, iy, iz),
            device_id_type=MESH,
        )

    spans = ((2, NX), (1, 2), (NX, NX + 1), (1, NX + 1))
    y_parts = ((3,), (0, 1, 2))

    def y_copy(turn, way, part):
        buf, (low, high) = bufs[turn], spans[part]
        edge = TOP + NY - 1 if way else TOP
        return pltpu.make_async_remote_copy(
            src_ref=buf.at[:, low:high, edge:edge + 1],
            dst_ref=y_halo.at[turn, 1 - way, :, low - 1:high - 1],
            send_sem=ys_sem.at[turn, way, part],
            recv_sem=yr_sem.at[turn, way, part],
            device_id=(ix, iy + 1 if way else iy - 1, iz),
            device_id_type=MESH,
        )

    def z_copy(turn, way, part):
        source, target = ((inner_s, inner_r), (face_s, face_r))[part]
        return pltpu.make_async_remote_copy(
            src_ref=source.at[turn, way],
            dst_ref=target.at[turn, 0 if way else 1],
            send_sem=zs_sem.at[turn, way, part],
            recv_sem=zr_sem.at[turn, way, part],
            device_id=(ix, iy, iz + 1 if way else iz - 1),
            device_id_type=MESH,
        )

    def start(axis, way, copies):
        @pl.when(has[axis][way])
        def _():
            for copy in copies:
                copy.start()

    def arrive(axis, way, copies):
        @pl.when(has[axis][1 - way])
        def _():
            for copy in copies:
                copy.wait_recv()

    def sent(axis, way, copies):
        @pl.when(has[axis][way])
        def _():
            for copy in copies:
                copy.wait_send()

    tiles = ([], [])
    for f in range(0, F, 2):
        tiles[0].append([(f, 2, 6)])
        tiles[0].append([(f, 6, 8), (f + 1, 2, 4)])
        tiles[0].append([(f + 1, 4, 8)])
        tiles[1].append([(f, 1, 2), (f, 8, 9), (f + 1, 1, 2), (f + 1, 8, 9)])

    def pack_z(turn, part):
        buf, target = bufs[turn], (inner_s, face_s)[part]
        for t, pieces in enumerate(tiles[part]):
            tile = jnp.concatenate([buf[f, a:b, ROWS] for f, a, b in pieces], axis=0)
            tile = tile.reshape(NZ, NZ).T
            target[turn, 0, t:t + 1] = tile[0:1]
            target[turn, 1, t:t + 1] = tile[NZ - 1:NZ]

    lane = lax.broadcasted_iota(jnp.int32, (NY, NZ), 1)
    first, last = lane == 0, lane == NZ - 1
    edges = jnp.logical_or(first, last)

    def dots(left, right, x, sums):
        for t in range(NY // 8):
            rows = slice(TOP + 8 * t, TOP + 8 * t + 8)
            u = left[:, x, rows]
            v = u if right is left else right[:, x, rows]
            sums = tuple(sums[i] + u[i:i + 1] * v[i:] for i in range(F))
        return sums

    def inside(src, dst, left, right, sums):
        def step(x, sums):
            for f in range(F):
                c = src[f, x, ROWS]
                beside = src[f, x, TOP + 1:TOP + NY + 1] + src[f, x, TOP - 1:TOP + NY - 1]
                for other in (x - 1, x + 1):
                    if not isinstance(x, int) or 1 <= other <= NX:
                        beside = beside + src[f, other, ROWS]
                beside = beside + jnp.where(last, 0.0, pltpu.roll(c, NZ - 1, 1))
                beside = beside + jnp.where(first, 0.0, pltpu.roll(c, 1, 1))
                dst[f, x, ROWS] = diag[x - 1] * c - beside
            return dots(left, right, x, sums)

        sums = lax.fori_loop(2, NX, step, step(1, sums))
        return step(NX, sums)

    def alone(src, dst):
        def step(f, _):
            for x in range(1, NX + 1):
                c = src[f, x, ROWS]
                beside = src[f, x, TOP + 1:TOP + NY + 1] + src[f, x, TOP - 1:TOP + NY - 1]
                for other in (x - 1, x + 1):
                    if 1 <= other <= NX:
                        beside = beside + src[f, other, ROWS]
                beside = beside + jnp.where(last, 0.0, pltpu.roll(c, NZ - 1, 1))
                beside = beside + jnp.where(first, 0.0, pltpu.roll(c, 1, 1))
                dst[f, x, ROWS] = diag[x - 1] * c - beside
            return 0

        lax.fori_loop(0, F, step, 0)

    def take_x(src, dst, turn, group):
        for way in both:
            arrive("x", way, [x_copy(turn, way, group)])
        for f in range(CUTS[group], CUTS[group + 1]):
            dst[f, 1, ROWS] -= src[f, 0, ROWS]
            dst[f, NX, ROWS] -= src[f, NX + 1, ROWS]

    def take_y(dst, turn, parts):
        for way in both:
            arrive("y", way, [y_copy(turn, way, part) for part in parts])
        for part in parts:
            low, high = spans[part]
            for way, edge in enumerate((TOP, TOP + NY - 1)):
                dst[:, low:high, edge:edge + 1] -= y_halo[turn, way, :, low - 1:high - 1]

    def take_z(dst, turn, part):
        for way in both:
            arrive("z", way, [z_copy(turn, way, part)])
        source = (inner_r, face_r)[part]
        for t, pieces in enumerate(tiles[part]):
            low = jnp.broadcast_to(source[turn, 0, t:t + 1], (NZ // 2, NZ))
            high = jnp.broadcast_to(source[turn, 1, t:t + 1], (NZ // 2, NZ))
            tile = jnp.concatenate([low, high], axis=0).T.reshape(4, NY, NZ)
            at = 0
            for f, a, b in pieces:
                dst[f, a:b, ROWS] -= jnp.where(edges, tile[at:at + b - a], 0.0)
                at += b - a

    def moment(left, right, low, high, sums):
        return lax.fori_loop(low, high, lambda x, sums: dots(left, right, x, sums), sums)

    def faces(left, right, sums):
        return lax.fori_loop(0, 2, lambda k, sums: dots(left, right, 1 + (NX - 1) * k, sums), sums)

    none = tuple(jnp.zeros((F - i,) + TILE, jnp.float32) for i in range(F))

    sub = lax.broadcasted_iota(jnp.int32, TILE, 0)
    cell = lax.broadcasted_iota(jnp.int32, TILE, 1)

    def fold(parts):
        width = 1
        while len(parts) > 1:
            odd = (sub & width) != 0
            merged = []
            for i in range(0, len(parts), 2):
                a, b = parts[i], parts[i + 1]
                kept = jnp.where(odd, b, a)
                moved = jnp.where(odd, a, b)
                moved = jnp.where(odd, pltpu.roll(moved, width, 0), pltpu.roll(moved, 8 - width, 0))
                merged.append(kept + moved)
            parts = merged
            width *= 2
        return parts[0]

    place = lax.rem(cell, 2 * F)
    own = sub == lax.rem(F - lax.div(cell, 2 * F), F)

    def gather(k, sums, total):
        for c in range(F):
            line = fold([sums[min(i, c)][max(i, c) - min(i, c)] for i in range(F)])
            total = jnp.where(place == k * F + c, jnp.sum(line, axis=1, keepdims=True), total)
        return total

    def as_row(total):
        return jnp.sum(jnp.where(own, total, 0.0), axis=0, keepdims=True)

    def copy_part(stage, src, dst, device):
        return pltpu.make_async_remote_copy(
            src_ref=src, dst_ref=dst,
            send_sem=g_send.at[stage], recv_sem=g_recv.at[stage],
            device_id=device, device_id_type=MESH)

    def spread(stage, parts, mine, devices, rows):
        for k, value in enumerate(rows):
            parts[mine, k:k + 1] = value
        for device in devices:
            copy_part(stage, parts.at[mine], parts.at[mine], device).start()
        count = len(devices)
        return copy_part(stage, parts.at[0:count], parts.at[0:count], devices[0])

    def added(parts, count):
        sums = [parts[k] for k in range(count)]
        while len(sums) > 1:
            sums = [sums[k] + sums[k + 1] for k in range(0, len(sums), 2)]
        return sums[0]

    loads[0].wait()
    loads[1].wait()
    pl.semaphore_wait(barrier, len(near))
    for way in both:
        start("x", way, [x_copy(0, way, group) for group in range(GROUPS)])
    tell(0, near)
    loads[2].wait()
    for way in both:
        start("y", way, [y_copy(0, way, part) for part in y_parts[0]])
    for part in both:
        pack_z(0, part)
    for way in both:
        start("z", way, [z_copy(0, way, part) for part in both])
    loads[3].wait()
    diag[...] = 6.0 + diag[...]
    zeroth = inside(buf_p, buf_q, buf_p, buf_p, none)
    blank = jnp.zeros(TILE, jnp.float32)
    row_zero = as_row(gather(0, zeroth, blank))
    pl.semaphore_wait(heard.at[0], len(near))
    tell(1, second)
    take_y(buf_q, 0, y_parts[0])
    for part in both:
        take_z(buf_q, 0, part)

    def forward(group):
        take_x(buf_p, buf_q, 0, group)
        for way in both:
            start("x", way, [x_copy(1, way, group)])

    forward(0)
    for way in both:
        start("y", way, [y_copy(1, way, 0)])
    pack_z(1, 0)
    for way in both:
        start("z", way, [z_copy(1, way, 0)])
    forward(1)
    second_sums = moment(buf_q, buf_q, 2, NX, none)
    forward(2)
    for group in range(3, GROUPS):
        forward(group)
    for way in both:
        start("y", way, [y_copy(1, way, part) for part in (1, 2)])
    pack_z(1, 1)
    for way in both:
        start("z", way, [z_copy(1, way, 1)])

    if second:
        pl.semaphore_wait(heard.at[1], len(second))
    tell(2, [(ix, across, iz)])

    alone(buf_q, buf_r)
    total = gather(0, moment(buf_p, buf_q, 1, NX + 1, none), blank)
    total = gather(1, faces(buf_q, buf_q, second_sums), total)
    row_one = as_row(total)
    pl.semaphore_wait(heard.at[2], 1)
    in_line = 2 * iz + core
    early_done = spread(0, part_e, in_line, line, (row_zero, row_one))
    take_y(buf_r, 1, (0,))
    take_z(buf_r, 1, 0)
    third = moment(buf_q, buf_r, 2, NX, none)
    fourth = moment(buf_r, buf_r, 2, NX, none)
    take_y(buf_r, 1, (1, 2))
    take_z(buf_r, 1, 1)
    for group in range(GROUPS):
        take_x(buf_q, buf_r, 1, group)
    third = faces(buf_q, buf_r, third)
    fourth = faces(buf_r, buf_r, fourth)
    row_two = as_row(gather(1, fourth, gather(0, third, blank)))

    late_done = spread(1, part_l, in_line, line, (row_two,))
    for turn in both:
        for way in both:
            sent("x", way, [x_copy(turn, way, group) for group in range(GROUPS)])
            sent("y", way, [y_copy(turn, way, part) for part in y_parts[turn]])
            sent("z", way, [z_copy(turn, way, part) for part in both])
    early_done.wait_send()
    early_done.wait_recv()
    early = added(part_e, len(line) + 1)
    late_done.wait_recv()
    late = added(part_l, len(line) + 1)
    chip = ix * chips_y + lax.div(row, 2)
    planes_done = spread(2, part_p, chip, plane, (early[0:1], early[1:2], late))
    late_done.wait_send()
    planes_done.wait_recv()
    gram_ref[...] = added(part_p, len(plane) + 1)

    planes_done.wait_send()


def combine_kernel(gram_ref, buf_b, buf_a, x_hbm, norm_ref, buf_x, coeff, out_sem):
    turned = [
        pltpu.roll(jnp.broadcast_to(gram_ref[k:k + 1], TILE), 0, 1, stride=2 * F, stride_axis=0) for k in range(3)
    ]
    sub = lax.broadcasted_iota(jnp.int32, TILE, 0)
    cell = lax.broadcasted_iota(jnp.int32, TILE, 1)

    def column(order, c):
        k, half = ((0, 0), (1, 0), (1, 1), (2, 0), (2, 1))[order]
        at = half * F + c
        return jnp.broadcast_to(turned[k][:, at:at + 1], TILE)

    def spread(value, row):
        return jnp.broadcast_to(value[row:row + 1], TILE)

    moments = [[column(order, c) for c in range(F)] for order in range(5)]
    columns = [[moments[2][c], moments[3][c]] for c in range(F)]
    columns += [[moments[3][c], moments[4][c]] for c in range(F)]
    rights = [[moments[1][c], moments[2][c]] for c in range(F)]
    for k in range(2 * F):
        half, row = k // F, k % F
        pivot = columns[k]
        inverse = 1.0 / spread(pivot[half], row)
        mine = sub == row
        for other in columns[k + 1:] + rights:
            r = spread(other[half], row) * inverse
            for h in range(2):
                value = other[h] - pivot[h] * r
                other[h] = jnp.where(mine, r, value) if h == half else value
    norms = jnp.zeros((1, 128), jnp.float32)
    for c in range(F):
        for h in range(2):
            coeff[c, h] = rights[c][h]
        fit = moments[1][c] * rights[c][0] + moments[2][c] * rights[c][1]
        left = jnp.where(sub == c, moments[0][c], 0.0) - fit
        norms = jnp.where(cell[0:1] == c, jnp.sum(left, axis=0, keepdims=True), norms)
    norm_ref[...] = jnp.sqrt(jnp.maximum(norms, 0.0))[:, :F]

    def out(x):
        return pltpu.make_async_copy(buf_x.at[:, x], x_hbm.at[:, x], out_sem.at[x])

    def step(x, _):
        for t in range(NY // 8):
            rows = slice(8 * t, 8 * t + 8)
            held = slice(TOP + 8 * t, TOP + 8 * t + 8)
            fields = [buf_b[:, x + 1, held], buf_a[:, x + 1, held]]
            for c in range(F):
                sums = [None, None]
                for h in range(2):
                    for i in range(F):
                        term = jnp.broadcast_to(coeff[c, h, i:i + 1], TILE) * fields[h][i]
                        sums[h] = term if sums[h] is None else sums[h] + term
                buf_x[c, x, rows] = sums[0] + sums[1]
        out(x).start()
        return 0

    lax.fori_loop(0, NX, step, 0)
    for x in range(NX):
        out(x).wait()


def solution(mesh):
    gx, gy, gz = mesh.shape["gx"], mesh.shape["gy"], mesh.shape["gz"]
    f32 = jnp.float32
    dma = pltpu.SemaphoreType.DMA
    hbm = pl.BlockSpec(memory_space=pltpu.HBM)
    vmem = pl.BlockSpec(memory_space=pltpu.VMEM)
    block = (F, NX, NY, NZ)
    padded = (F, NX + 2, NY + 16, NZ)

    def body(right_side, shift):
        gram, fields, images = pl.pallas_call(
            functools.partial(exchange_kernel, gx, gy, gz),
            out_shape=(
                jax.ShapeDtypeStruct((3, NZ), f32),
                jax.ShapeDtypeStruct(padded, f32),
                jax.ShapeDtypeStruct(padded, f32),
            ),
            in_specs=[hbm, hbm],
            out_specs=(vmem, vmem, vmem),
            scratch_shapes=[
                pltpu.VMEM(padded, f32),
                pltpu.VMEM((NX, NY, NZ), f32),
                pltpu.VMEM((2, 2, F, NX, 1, NZ), f32),
                pltpu.VMEM((2, 2, INNER, NZ), f32),
                pltpu.VMEM((2, 2, INNER, NZ), f32),
                pltpu.VMEM((2, 2, FACE, NZ), f32),
                pltpu.VMEM((2, 2, FACE, NZ), f32),
                pltpu.VMEM((2 * gz, 2, NZ), f32),
                pltpu.VMEM((2 * gz, 1, NZ), f32),
                pltpu.VMEM((gx * gy // 2, 3, NZ), f32),
                dma((4,)),
                dma((2, 2, GROUPS)),
                dma((2, 2, GROUPS)),
                dma((2, 2, 4)),
                dma((2, 2, 4)),
                dma((2, 2, 2)),
                dma((2, 2, 2)),
                dma((3,)),
                dma((3,)),
                pltpu.SemaphoreType.REGULAR((3,)),
            ],
            compiler_params=pltpu.CompilerParams(
                collective_id=0, has_side_effects=True, vmem_limit_bytes=24 << 20
            ),
        )(*(pltpu.with_memory_space_constraint(a, pltpu.HBM) for a in (right_side, shift)))
        solved, norms = pl.pallas_call(
            combine_kernel,
            out_shape=(jax.ShapeDtypeStruct(block, f32), jax.ShapeDtypeStruct((1, F), f32)),
            in_specs=[vmem, vmem, vmem],
            out_specs=(hbm, vmem),
            scratch_shapes=[
                pltpu.VMEM(block, f32),
                pltpu.VMEM((F, 2) + TILE, f32),
                dma((NX,)),
            ],
            compiler_params=pltpu.CompilerParams(vmem_limit_bytes=16 << 20),
        )(gram, fields, images)
        return solved, norms.reshape(F)

    return jax.shard_map(
        body,
        mesh=mesh,
        in_specs=(P(None, "gx", "gy", "gz"), P("gx", "gy", "gz")),
        out_specs=(P(None, "gx", "gy", "gz"), P()),
        check_vma=False,
    )
```

```python
import functools

import jax
import jax.numpy as jnp
from jax import lax
from jax.experimental import pallas as pl
from jax.experimental.pallas import tpu as pltpu
from jax.sharding import PartitionSpec as P

MESH = pl.DeviceIdType.MESH
F, NX, NY, NZ = 8, 8, 32, 128
TOP = 8
ROWS = slice(TOP, TOP + NY)
CUTS = (0, 4, 7, 8)
GROUPS = len(CUTS) - 1
INNER, FACE = 12, 4
TILE = (8, 128)


def exchange_kernel(gx, gy, gz, b_hbm, s_hbm, gram_ref, buf_p, buf_q,
                    buf_r, diag, y_halo, inner_s, inner_r, face_s, face_r, part_e, part_l, part_p,
                    load_sem, xs_sem, xr_sem, ys_sem, yr_sem, zs_sem, zr_sem, g_send, g_recv, heard):
    ix, iy, iz = lax.axis_index("gx"), lax.axis_index("gy"), lax.axis_index("gz")

    loads = [
        pltpu.make_async_copy(b_hbm.at[:, 0], buf_p.at[:, 1, ROWS], load_sem.at[0]),
        pltpu.make_async_copy(b_hbm.at[:, NX - 1], buf_p.at[:, NX, ROWS], load_sem.at[1]),
        pltpu.make_async_copy(b_hbm.at[:, 1:NX - 1], buf_p.at[:, 2:NX, ROWS], load_sem.at[2]),
        pltpu.make_async_copy(s_hbm, diag, load_sem.at[3]),
    ]
    for load in loads:
        load.start()

    chips_y = gy // 2
    core = lax.rem(iy, 2)
    row = iy - core
    xs = [ix] + [lax.rem(ix + k, gx) for k in range(1, gx)]
    ys = [iy] + [lax.rem(iy + 2 * k, gy) for k in range(1, chips_y)]
    zs = [iz] + [lax.rem(iz + k, gz) for k in range(1, gz)]
    across = row + 1 - core
    beyond = lax.rem(iy + gy - 1 + 2 * core, gy)
    def hops(k, n):
        return min(k, n - k)

    line = [(ix, y, zs[k]) for k in sorted(range(1, gz), key=lambda k: -hops(k, gz)) for y in (across, iy)]
    line += [(ix, across, iz)]
    steps = sorted(((a, b) for a in range(gx) for b in range(chips_y)), key=lambda p: -hops(p[0], gx) - hops(p[1], chips_y))
    plane = [(xs[a], ys[b], iz) for a, b in steps if a or b]
    step_y = [ys[k] for k in dict.fromkeys((1, chips_y - 1)) if k % chips_y]
    near = [(xs[k], iy, iz) for k in dict.fromkeys((1, gx - 1))] + [(ix, beyond, iz), (ix, across, iz)]
    near += [(ix, iy, zs[k]) for k in dict.fromkeys((1, gz - 1))] + [(ix, y, iz) for y in step_y]
    second = [(xs[2 % gx], iy, iz), (ix, ys[2 % chips_y], iz)] if gx > 2 and chips_y > 2 else []
    second += [(ix, iy, zs[k]) for k in dict.fromkeys((2, gz - 2))] if gz > 3 else []

    barrier = pltpu.get_barrier_semaphore()
    for device in near:
        pl.semaphore_signal(barrier, inc=1, device_id=device, device_id_type=MESH)

    def tell(stage, devices):
        for device in devices:
            pl.semaphore_signal(heard.at[stage], inc=1, device_id=device, device_id_type=MESH)

    zero_x = jnp.zeros((F, NY, NZ), jnp.float32)
    zero_y = jnp.zeros((F, NX, 1, NZ), jnp.float32)
    for turn, buf in enumerate((buf_p, buf_q)):
        buf[:, 1:NX + 1, TOP - 1:TOP] = zero_y
        buf[:, 1:NX + 1, TOP + NY:TOP + NY + 1] = zero_y
        for way in range(2):
            @pl.when(ix == way * (gx - 1))
            def _():
                buf[:, way * (NX + 1), ROWS] = zero_x

            @pl.when(iy == way * (gy - 1))
            def _():
                y_halo[turn, way] = zero_y

            @pl.when(iz == way * (gz - 1))
            def _():
                inner_r[turn, way] = jnp.zeros((INNER, NZ), jnp.float32)
                face_r[turn, way] = jnp.zeros((FACE, NZ), jnp.float32)

    bufs, both = (buf_p, buf_q), range(2)
    has = {
        "x": (ix > 0, ix < gx - 1),
        "y": (iy > 0, iy < gy - 1),
        "z": (iz > 0, iz < gz - 1),
    }

    def x_copy(turn, way, group):
        fields = slice(CUTS[group], CUTS[group + 1])
        buf = bufs[turn]
        return pltpu.make_async_remote_copy(
            src_ref=buf.at[fields, NX if way else 1, ROWS],
            dst_ref=buf.at[fields, 0 if way else NX + 1, ROWS],
            send_sem=xs_sem.at[turn, way, group],
            recv_sem=xr_sem.at[turn, way, group],
            device_id=(ix + 1 if way else ix - 1, iy, iz),
            device_id_type=MESH,
        )

    spans = ((2, NX), (1, 2), (NX, NX + 1))

    def y_copy(turn, way, part):
        buf, (low, high) = bufs[turn], spans[part]
        edge = TOP + NY - 1 if way else TOP
        return pltpu.make_async_remote_copy(
            src_ref=buf.at[:, low:high, edge:edge + 1],
            dst_ref=y_halo.at[turn, 1 - way, :, low - 1:high - 1],
            send_sem=ys_sem.at[turn, way, part],
            recv_sem=yr_sem.at[turn, way, part],
            device_id=(ix, iy + 1 if way else iy - 1, iz),
            device_id_type=MESH,
        )

    def z_copy(turn, way, part):
        source, target = ((inner_s, inner_r), (face_s, face_r))[part]
        return pltpu.make_async_remote_copy(
            src_ref=source.at[turn, way],
            dst_ref=target.at[turn, 0 if way else 1],
            send_sem=zs_sem.at[turn, way, part],
            recv_sem=zr_sem.at[turn, way, part],
            device_id=(ix, iy, iz + 1 if way else iz - 1),
            device_id_type=MESH,
        )

    def start(axis, way, copies):
        @pl.when(has[axis][way])
        def _():
            for copy in copies:
                copy.start()

    def arrive(axis, way, copies):
        @pl.when(has[axis][1 - way])
        def _():
            for copy in copies:
                copy.wait_recv()

    def sent(axis, way, copies):
        @pl.when(has[axis][way])
        def _():
            for copy in copies:
                copy.wait_send()

    tiles = ([], [])
    for f in range(0, F, 2):
        tiles[0].append([(f, 2, 6)])
        tiles[0].append([(f, 6, 8), (f + 1, 2, 4)])
        tiles[0].append([(f + 1, 4, 8)])
        tiles[1].append([(f, 1, 2), (f, 8, 9), (f + 1, 1, 2), (f + 1, 8, 9)])

    def pack_z(turn, part):
        buf, target = bufs[turn], (inner_s, face_s)[part]
        for t, pieces in enumerate(tiles[part]):
            tile = jnp.concatenate([buf[f, a:b, ROWS] for f, a, b in pieces], axis=0)
            tile = tile.reshape(NZ, NZ).T
            target[turn, 0, t:t + 1] = tile[0:1]
            target[turn, 1, t:t + 1] = tile[NZ - 1:NZ]

    lane = lax.broadcasted_iota(jnp.int32, (NY, NZ), 1)
    first, last = lane == 0, lane == NZ - 1
    edges = jnp.logical_or(first, last)

    def dots(left, right, x, sums):
        for t in range(NY // 8):
            rows = slice(TOP + 8 * t, TOP + 8 * t + 8)
            u = left[:, x, rows]
            v = u if right is left else right[:, x, rows]
            sums = tuple(sums[i] + u[i:i + 1] * v[i:] for i in range(F))
        return sums

    def inside(src, dst, left, right, sums):
        def step(x, sums):
            for f in range(F):
                c = src[f, x, ROWS]
                beside = src[f, x, TOP + 1:TOP + NY + 1] + src[f, x, TOP - 1:TOP + NY - 1]
                for other in (x - 1, x + 1):
                    if not isinstance(x, int) or 1 <= other <= NX:
                        beside = beside + src[f, other, ROWS]
                beside = beside + jnp.where(last, 0.0, pltpu.roll(c, NZ - 1, 1))
                beside = beside + jnp.where(first, 0.0, pltpu.roll(c, 1, 1))
                dst[f, x, ROWS] = diag[x - 1] * c - beside
            return dots(left, right, x, sums)

        sums = lax.fori_loop(2, NX, step, step(1, sums))
        return step(NX, sums)

    def alone(src, dst):
        def step(f, _):
            for x in range(1, NX + 1):
                c = src[f, x, ROWS]
                beside = src[f, x, TOP + 1:TOP + NY + 1] + src[f, x, TOP - 1:TOP + NY - 1]
                for other in (x - 1, x + 1):
                    if 1 <= other <= NX:
                        beside = beside + src[f, other, ROWS]
                beside = beside + jnp.where(last, 0.0, pltpu.roll(c, NZ - 1, 1))
                beside = beside + jnp.where(first, 0.0, pltpu.roll(c, 1, 1))
                dst[f, x, ROWS] = diag[x - 1] * c - beside
            return 0

        lax.fori_loop(0, F, step, 0)

    def take_x(src, dst, turn, group):
        for way in both:
            arrive("x", way, [x_copy(turn, way, group)])
        for f in range(CUTS[group], CUTS[group + 1]):
            dst[f, 1, ROWS] -= src[f, 0, ROWS]
            dst[f, NX, ROWS] -= src[f, NX + 1, ROWS]

    def take_y(dst, turn, parts):
        for way in both:
            arrive("y", way, [y_copy(turn, way, part) for part in parts])
        for part in parts:
            low, high = spans[part]
            for way, edge in enumerate((TOP, TOP + NY - 1)):
                dst[:, low:high, edge:edge + 1] -= y_halo[turn, way, :, low - 1:high - 1]

    def take_z(dst, turn, part):
        for way in both:
            arrive("z", way, [z_copy(turn, way, part)])
        source = (inner_r, face_r)[part]
        for t, pieces in enumerate(tiles[part]):
            low = jnp.broadcast_to(source[turn, 0, t:t + 1], (NZ // 2, NZ))
            high = jnp.broadcast_to(source[turn, 1, t:t + 1], (NZ // 2, NZ))
            tile = jnp.concatenate([low, high], axis=0).T.reshape(4, NY, NZ)
            at = 0
            for f, a, b in pieces:
                dst[f, a:b, ROWS] -= jnp.where(edges, tile[at:at + b - a], 0.0)
                at += b - a

    def moment(left, right, low, high, sums):
        return lax.fori_loop(low, high, lambda x, sums: dots(left, right, x, sums), sums)

    def faces(left, right, sums):
        return lax.fori_loop(0, 2, lambda k, sums: dots(left, right, 1 + (NX - 1) * k, sums), sums)

    none = tuple(jnp.zeros((F - i,) + TILE, jnp.float32) for i in range(F))

    sub = lax.broadcasted_iota(jnp.int32, TILE, 0)
    cell = lax.broadcasted_iota(jnp.int32, TILE, 1)

    def fold(parts):
        width = 1
        while len(parts) > 1:
            odd = (sub & width) != 0
            merged = []
            for i in range(0, len(parts), 2):
                a, b = parts[i], parts[i + 1]
                kept = jnp.where(odd, b, a)
                moved = jnp.where(odd, a, b)
                moved = jnp.where(odd, pltpu.roll(moved, width, 0), pltpu.roll(moved, 8 - width, 0))
                merged.append(kept + moved)
            parts = merged
            width *= 2
        return parts[0]

    place = lax.rem(cell, 2 * F)
    own = sub == lax.rem(F - lax.div(cell, 2 * F), F)

    def gather(k, sums, total):
        for c in range(F):
            line = fold([sums[min(i, c)][max(i, c) - min(i, c)] for i in range(F)])
            total = jnp.where(place == k * F + c, jnp.sum(line, axis=1, keepdims=True), total)
        return total

    def as_row(total):
        return jnp.sum(jnp.where(own, total, 0.0), axis=0, keepdims=True)

    def copy_part(stage, src, dst, device):
        return pltpu.make_async_remote_copy(
            src_ref=src, dst_ref=dst,
            send_sem=g_send.at[stage], recv_sem=g_recv.at[stage],
            device_id=device, device_id_type=MESH)

    def spread(stage, parts, mine, devices, rows):
        for k, value in enumerate(rows):
            parts[mine, k:k + 1] = value
        for device in devices:
            copy_part(stage, parts.at[mine], parts.at[mine], device).start()
        count = len(devices)
        return copy_part(stage, parts.at[0:count], parts.at[0:count], devices[0])

    def added(parts, count):
        sums = [parts[k] for k in range(count)]
        while len(sums) > 1:
            sums = [sums[k] + sums[k + 1] for k in range(0, len(sums), 2)]
        return sums[0]

    loads[0].wait()
    loads[1].wait()
    pl.semaphore_wait(barrier, len(near))
    for way in both:
        start("x", way, [x_copy(0, way, group) for group in range(GROUPS)])
    tell(0, near)
    loads[2].wait()
    for way in both:
        start("y", way, [y_copy(0, way, part) for part in range(3)])
    for part in both:
        pack_z(0, part)
    for way in both:
        start("z", way, [z_copy(0, way, part) for part in both])
    loads[3].wait()
    diag[...] = 6.0 + diag[...]
    zeroth = inside(buf_p, buf_q, buf_p, buf_p, none)
    blank = jnp.zeros(TILE, jnp.float32)
    row_zero = as_row(gather(0, zeroth, blank))
    pl.semaphore_wait(heard.at[0], len(near))
    tell(1, second)
    take_y(buf_q, 0, range(3))
    for part in both:
        take_z(buf_q, 0, part)

    def forward(group):
        take_x(buf_p, buf_q, 0, group)
        for way in both:
            start("x", way, [x_copy(1, way, group)])

    forward(0)
    for way in both:
        start("y", way, [y_copy(1, way, 0)])
    pack_z(1, 0)
    for way in both:
        start("z", way, [z_copy(1, way, 0)])
    forward(1)
    second_sums = moment(buf_q, buf_q, 2, NX, none)
    forward(2)
    for group in range(3, GROUPS):
        forward(group)
    for way in both:
        start("y", way, [y_copy(1, way, part) for part in (1, 2)])
    pack_z(1, 1)
    for way in both:
        start("z", way, [z_copy(1, way, 1)])

    if second:
        pl.semaphore_wait(heard.at[1], len(second))
    tell(2, [(ix, across, iz)])

    alone(buf_q, buf_r)
    total = gather(0, moment(buf_p, buf_q, 1, NX + 1, none), blank)
    total = gather(1, faces(buf_q, buf_q, second_sums), total)
    row_one = as_row(total)
    pl.semaphore_wait(heard.at[2], 1)
    in_line = 2 * iz + core
    early_done = spread(0, part_e, in_line, line, (row_zero, row_one))
    take_y(buf_r, 1, (0,))
    take_z(buf_r, 1, 0)
    third = moment(buf_q, buf_r, 2, NX, none)
    fourth = moment(buf_r, buf_r, 2, NX, none)
    take_y(buf_r, 1, (1, 2))
    take_z(buf_r, 1, 1)
    for group in range(GROUPS):
        take_x(buf_q, buf_r, 1, group)
    third = faces(buf_q, buf_r, third)
    fourth = faces(buf_r, buf_r, fourth)
    row_two = as_row(gather(1, fourth, gather(0, third, blank)))

    late_done = spread(1, part_l, in_line, line, (row_two,))
    early_done.wait_recv()
    early = added(part_e, len(line) + 1)
    late_done.wait_recv()
    late = added(part_l, len(line) + 1)
    chip = ix * chips_y + lax.div(row, 2)
    planes_done = spread(2, part_p, chip, plane, (early[0:1], early[1:2], late))
    planes_done.wait_recv()
    gram_ref[...] = added(part_p, len(plane) + 1)

    early_done.wait_send()
    late_done.wait_send()
    planes_done.wait_send()
    for turn in both:
        for way in both:
            sent("x", way, [x_copy(turn, way, group) for group in range(GROUPS)])
            sent("y", way, [y_copy(turn, way, part) for part in range(3)])
            sent("z", way, [z_copy(turn, way, part) for part in both])


def combine_kernel(gram_ref, buf_b, buf_a, x_hbm, norm_ref, buf_x, coeff, out_sem):
    turned = [
        pltpu.roll(jnp.broadcast_to(gram_ref[k:k + 1], TILE), 0, 1, stride=2 * F, stride_axis=0) for k in range(3)
    ]
    sub = lax.broadcasted_iota(jnp.int32, TILE, 0)
    cell = lax.broadcasted_iota(jnp.int32, TILE, 1)

    def column(order, c):
        k, half = ((0, 0), (1, 0), (1, 1), (2, 0), (2, 1))[order]
        at = half * F + c
        return jnp.broadcast_to(turned[k][:, at:at + 1], TILE)

    def spread(value, row):
        return jnp.broadcast_to(value[row:row + 1], TILE)

    moments = [[column(order, c) for c in range(F)] for order in range(5)]
    columns = [[moments[2][c], moments[3][c]] for c in range(F)]
    columns += [[moments[3][c], moments[4][c]] for c in range(F)]
    rights = [[moments[1][c], moments[2][c]] for c in range(F)]
    for k in range(2 * F):
        half, row = k // F, k % F
        pivot = columns[k]
        inverse = 1.0 / spread(pivot[half], row)
        mine = sub == row
        for other in columns[k + 1:] + rights:
            r = spread(other[half], row) * inverse
            for h in range(2):
                value = other[h] - pivot[h] * r
                other[h] = jnp.where(mine, r, value) if h == half else value
    norms = jnp.zeros((1, 128), jnp.float32)
    for c in range(F):
        for h in range(2):
            coeff[c, h] = rights[c][h]
        fit = moments[1][c] * rights[c][0] + moments[2][c] * rights[c][1]
        left = jnp.where(sub == c, moments[0][c], 0.0) - fit
        norms = jnp.where(cell[0:1] == c, jnp.sum(left, axis=0, keepdims=True), norms)
    norm_ref[...] = jnp.sqrt(jnp.maximum(norms, 0.0))[:, :F]

    def out(x):
        return pltpu.make_async_copy(buf_x.at[:, x], x_hbm.at[:, x], out_sem.at[x])

    def step(x, _):
        for t in range(NY // 8):
            rows = slice(8 * t, 8 * t + 8)
            held = slice(TOP + 8 * t, TOP + 8 * t + 8)
            fields = [buf_b[:, x + 1, held], buf_a[:, x + 1, held]]
            for c in range(F):
                sums = [None, None]
                for h in range(2):
                    for i in range(F):
                        term = jnp.broadcast_to(coeff[c, h, i:i + 1], TILE) * fields[h][i]
                        sums[h] = term if sums[h] is None else sums[h] + term
                buf_x[c, x, rows] = sums[0] + sums[1]
        out(x).start()
        return 0

    lax.fori_loop(0, NX, step, 0)
    for x in range(NX):
        out(x).wait()


def solution(mesh):
    gx, gy, gz = mesh.shape["gx"], mesh.shape["gy"], mesh.shape["gz"]
    f32 = jnp.float32
    dma = pltpu.SemaphoreType.DMA
    hbm = pl.BlockSpec(memory_space=pltpu.HBM)
    vmem = pl.BlockSpec(memory_space=pltpu.VMEM)
    block = (F, NX, NY, NZ)
    padded = (F, NX + 2, NY + 16, NZ)

    def body(right_side, shift):
        gram, fields, images = pl.pallas_call(
            functools.partial(exchange_kernel, gx, gy, gz),
            out_shape=(
                jax.ShapeDtypeStruct((3, NZ), f32),
                jax.ShapeDtypeStruct(padded, f32),
                jax.ShapeDtypeStruct(padded, f32),
            ),
            in_specs=[hbm, hbm],
            out_specs=(vmem, vmem, vmem),
            scratch_shapes=[
                pltpu.VMEM(padded, f32),
                pltpu.VMEM((NX, NY, NZ), f32),
                pltpu.VMEM((2, 2, F, NX, 1, NZ), f32),
                pltpu.VMEM((2, 2, INNER, NZ), f32),
                pltpu.VMEM((2, 2, INNER, NZ), f32),
                pltpu.VMEM((2, 2, FACE, NZ), f32),
                pltpu.VMEM((2, 2, FACE, NZ), f32),
                pltpu.VMEM((2 * gz, 2, NZ), f32),
                pltpu.VMEM((2 * gz, 1, NZ), f32),
                pltpu.VMEM((gx * gy // 2, 3, NZ), f32),
                dma((4,)),
                dma((2, 2, GROUPS)),
                dma((2, 2, GROUPS)),
                dma((2, 2, 3)),
                dma((2, 2, 3)),
                dma((2, 2, 2)),
                dma((2, 2, 2)),
                dma((3,)),
                dma((3,)),
                pltpu.SemaphoreType.REGULAR((3,)),
            ],
            compiler_params=pltpu.CompilerParams(
                collective_id=0, has_side_effects=True, vmem_limit_bytes=24 << 20
            ),
        )(*(pltpu.with_memory_space_constraint(a, pltpu.HBM) for a in (right_side, shift)))
        solved, norms = pl.pallas_call(
            combine_kernel,
            out_shape=(jax.ShapeDtypeStruct(block, f32), jax.ShapeDtypeStruct((1, F), f32)),
            in_specs=[vmem, vmem, vmem],
            out_specs=(hbm, vmem),
            scratch_shapes=[
                pltpu.VMEM(block, f32),
                pltpu.VMEM((F, 2) + TILE, f32),
                dma((NX,)),
            ],
            compiler_params=pltpu.CompilerParams(vmem_limit_bytes=16 << 20),
        )(gram, fields, images)
        return solved, norms.reshape(F)

    return jax.shard_map(
        body,
        mesh=mesh,
        in_specs=(P(None, "gx", "gy", "gz"), P("gx", "gy", "gz")),
        out_specs=(P(None, "gx", "gy", "gz"), P()),
        check_vma=False,
    )
```
